32 devices in a mesh: blk: 16 (over z, x, core), rep: 2 (over y).
Axes of the slice: x: 2, y: 2, z: 4, core: 2. Of those that a mesh axis runs over, the one named last changes fastest.
Arguments:
- measured: float32 [3, 16, 8, 1536], P(None, 'blk', None, 'rep'), may hold values from -4 to 4
- rot_vector: float32 [3, 16, 8, 1536], P(None, 'blk', None, 'rep'), may hold values from -6 to 6
- confidence: float32 [3, 16, 8, 1536], P(None, 'blk', None, 'rep'), may hold values from 0.5 to 2
- first_local: int32 [16, 8, 1536], P('blk', None, 'rep'), may hold values from 0 to 2047
- second_local: int32 [16, 8, 1536], P('blk', None, 'rep'), may hold values from 0 to 2047
- edge_counts: int32 [16, 8, 2], P('blk', None, 'rep'), may hold values from 256 to 768, as said below
- start_angles: float32 [3, 32768], P(None, 'blk'), may hold values from -4 to 4
- anchor: float32 [32768], P('blk'), may hold values from 0.05 to 0.5
Outputs:
- estimate: float32 [3, 32768], P(None, 'blk')
- weights: float32 [16, 8, 1536], P('blk', None, 'rep')
The draws below stay inside these ranges and needn't reach their ends.
Inputs may be any that keep to these rules, and one draw needn't show every extreme that they name: `edge_counts`: live edges of a tile pair on one device fill its first slots; in every tile some pair holds 768 live edges on one device.
All inputs are finite; a program needn't handle non-finite values.
Results may differ from the reference program's by a relative error of at most 0.0001.
Values sent between devices are 32-bit elements; how exact they have to be, the bound alone decides.
No kernel may reach another device: no remote copies, remote signals or barrier semaphores. Data moves between devices by JAX's collectives and lax.ppermute only.
A program may use at most 128 MiB of HBM per device.

```python
import math
import jax
import jax.numpy as jnp
from jax import lax

CT = 2048
EH = 768
OFFS = 8
PASSES = 2
ITERS = 2
NCAM = 32768
EPT = 1536
N_BLK = 16


def draw_edge_counts(key, part):
    tile_total = NCAM // CT
    halves = EPT // EH
    base_key, pair_key, half_key = jax.random.split(jax.random.fold_in(key, 11), 3)
    base = jax.random.randint(base_key, (tile_total, OFFS, halves), EH // 3, EH + 1, dtype=jnp.int32)
    pick_pair = jax.random.randint(pair_key, (tile_total, 1, 1), 0, OFFS, dtype=jnp.int32)
    pick_half = jax.random.randint(half_key, (tile_total, 1, 1), 0, halves, dtype=jnp.int32)
    chosen = (jnp.arange(OFFS, dtype=jnp.int32)[None, :, None] == pick_pair) & (jnp.arange(halves, dtype=jnp.int32)[None, None, :] == pick_half)
    return jnp.where(chosen, EH, base).astype(jnp.int32)


def draw_measured(key, part):
    tile_total = NCAM // CT
    shape = (3, tile_total, OFFS, EPT)
    rising = 1.0 + 2.0 * jnp.arange(tile_total, dtype=jnp.float32) / max(tile_total - 1, 1)
    rising = rising[None, :, None, None]
    value_key = jax.random.fold_in(jax.random.fold_in(key, 23), 0)
    return jnp.clip(0.3 * rising * jax.random.normal(value_key, shape, jnp.float32), -4.0, 4.0)


def with_ends(values, key, smallest, largest):
    longest = values.shape.index(max(values.shape))
    spots = []
    for shift in (0, 1):
        where = [jax.random.randint(jax.random.fold_in(key, axis), (), 0, length) for axis, length in enumerate(values.shape)]
        where[longest] = (where[longest] + shift) % values.shape[longest]
        spots.append(tuple(where))
    return values.at[spots[0]].set(smallest).at[spots[1]].set(largest)


def block_scale(own_key, dims, cuts, low, largest):
    level = 1.0
    for axis_at, blocks in cuts:
        draws = jax.random.uniform(jax.random.fold_in(jax.random.fold_in(own_key, 6), axis_at), (blocks,), jnp.float32, low / len(cuts), largest / len(cuts))
        level = level * jnp.repeat(jnp.exp(draws), dims[axis_at] // blocks).reshape((-1,) + (1,) * (len(dims) - 1 - axis_at))
    return level


def gaussian(key, shape, scale, limit, cuts=(), held_as=jnp.bfloat16):
    array = jax.random.normal(key, shape, jnp.float32) * scale
    if len(cuts) > 0:
        array = block_scale(key, shape, cuts, -0.22, 0.18) * array
    return jnp.clip(array, min=-limit, max=limit).astype(held_as)


def setup_inputs(seed: int = 0) -> dict:
    key_of = jax.random.split(jax.random.key(seed), 9)
    return {
        "measured": draw_measured(jax.random.fold_in(key_of[8], 71), 0),
        "rot_vector": gaussian(key_of[1], (3, N_BLK, OFFS, EPT), 1.0, 6.0, ((1, 16), (3, 2)), jnp.float32),
        "confidence": jnp.clip(jnp.exp(math.log(2.0) - 1.3862944 * jax.random.uniform(key_of[2], (3, N_BLK, OFFS, EPT), jnp.float32) ** block_scale(key_of[2], (3, N_BLK, OFFS, EPT), ((1, 16), (3, 2)), -0.2, 0.2)), 0.5, 2.0),
        "first_local": with_ends(jax.random.randint(key_of[3], (N_BLK, OFFS, EPT), 0, CT), jax.random.fold_in(key_of[3], 1), 0, CT - 1).astype(jnp.int32),
        "second_local": with_ends(jax.random.randint(key_of[4], (N_BLK, OFFS, EPT), 0, CT), jax.random.fold_in(key_of[4], 1), 0, CT - 1).astype(jnp.int32),
        "edge_counts": draw_edge_counts(jax.random.fold_in(key_of[8], 71), 0),
        "start_angles": gaussian(key_of[6], (3, NCAM), 0.3, 4.0, ((1, 16),), jnp.float32),
        "anchor": jnp.clip(jnp.exp(math.log(0.5) - 2.3025851 * jax.random.uniform(key_of[7], (NCAM,), jnp.float32) ** block_scale(key_of[7], (NCAM,), ((0, 16),), -0.2, 0.2)), 0.05, 0.5),
    }


PAIRS = ((0, 0), (0, 1), (0, 2), (1, 1), (1, 2), (2, 2))
LOOKUP = ((0, 1, 2), (1, 3, 4), (2, 4, 5))
SOFTEN = 0.05

def rotations(vector):
    squared = vector[0] * vector[0] + vector[1] * vector[1] + vector[2] * vector[2]
    factor = 2.0 / (1.0 + squared)
    zeros = jnp.zeros_like(squared)
    skewed = ((zeros, -vector[2], vector[1]), (vector[2], zeros, -vector[0]), (-vector[1], vector[0], zeros))
    matrix_rows = []
    for first in range(3):
        entries = []
        for second in range(3):
            term = skewed[first][second] + vector[first] * vector[second]
            if first == second:
                entries.append(1.0 + factor * (term - squared))
            else:
                entries.append(factor * term)
        matrix_rows.append(jnp.stack(entries))
    return jnp.stack(matrix_rows)

def rotate(rotation, vector):
    return lax.optimization_barrier(jnp.sum(rotation * vector[None], axis=1))

def rotate_back(rotation, vector):
    return lax.optimization_barrier(jnp.sum(rotation * vector[:, None], axis=0))

def block_parts(weighted, rotation):
    far_list = []
    near_list = []
    for first, second in PAIRS:
        near_list.append(lax.optimization_barrier(jnp.sum(rotation[:, first] * weighted * rotation[:, second], axis=0)))
        if first == second:
            far_list.append(weighted[first])
        else:
            far_list.append(jnp.zeros_like(weighted[0]))
    return (jnp.stack(far_list), jnp.stack(near_list))

def inverse_apply(blocks, vector):
    adjugate = jnp.stack([blocks[3] * blocks[5] - blocks[4] * blocks[4], blocks[2] * blocks[4] - blocks[1] * blocks[5], blocks[1] * blocks[4] - blocks[2] * blocks[3], blocks[0] * blocks[5] - blocks[2] * blocks[2], blocks[1] * blocks[2] - blocks[0] * blocks[4], blocks[0] * blocks[3] - blocks[1] * blocks[1]])
    determinant = blocks[0] * adjugate[0] + blocks[1] * adjugate[1] + blocks[2] * adjugate[2]
    result = []
    for first in range(3):
        total = adjugate[LOOKUP[first][0]] * vector[0] + adjugate[LOOKUP[first][1]] * vector[1] + adjugate[LOOKUP[first][2]] * vector[2]
        result.append(total / determinant)
    return jnp.stack(result)

def spread(terms, index, total):
    return jax.vmap(lambda values: jax.ops.segment_sum(values, index, num_segments=total))(terms)

def reference(measured, rot_vector, confidence, first_local, second_local, edge_counts, start_angles, anchor):
    tile_ids = jnp.arange(N_BLK, dtype=jnp.int32)[:, None, None]
    pair_ids = jnp.arange(OFFS, dtype=jnp.int32)[None, :, None]
    first = (tile_ids * CT + first_local).reshape(-1).astype(jnp.int32)
    second = ((tile_ids + pair_ids) % N_BLK * CT + second_local).reshape(-1).astype(jnp.int32)
    slots = jnp.arange(EPT, dtype=jnp.int32) % EH
    live = (slots[None, None, :] < jnp.repeat(edge_counts, EH, axis=2)).astype(jnp.float32).reshape(-1)
    measured = measured.reshape(3, -1)
    confidence = confidence.reshape(3, -1)
    rotation = rotations(rot_vector.reshape(3, -1))
    cameras = N_BLK * CT
    diagonal = jnp.stack([anchor if first_c == second_c else jnp.zeros_like(anchor) for first_c, second_c in PAIRS])

    def gather_back(terms):
        return spread(terms, second, cameras) - spread(rotate_back(rotation, terms), first, cameras)
    estimate = start_angles
    weights = live
    for sweep_index in range(PASSES):
        misfit = measured - (estimate[:, second] - rotate(rotation, estimate[:, first]))
        weights = live / jnp.sqrt(lax.optimization_barrier(jnp.sum(confidence * misfit * misfit, axis=0)) + SOFTEN * SOFTEN)
        weighted = weights * confidence
        residual = gather_back(weighted * misfit) - anchor * estimate
        far_part, near_part = block_parts(weighted, rotation)
        blocks = spread(far_part, second, cameras) + spread(near_part, first, cameras) + diagonal
        scaled = inverse_apply(blocks, residual)
        direction = scaled
        norm_now = jnp.sum(residual * scaled)
        for inner_index in range(ITERS):
            changed = direction[:, second] - rotate(rotation, direction[:, first])
            image = gather_back(weighted * changed) + anchor * direction
            step_size = norm_now / jnp.sum(direction * image)
            estimate = estimate + step_size * direction
            residual = residual - step_size * image
            if inner_index + 1 < ITERS:
                scaled = inverse_apply(blocks, residual)
                norm_next = jnp.sum(residual * scaled)
                direction = scaled + norm_next / norm_now * direction
                norm_now = norm_next
    return (estimate, weights.reshape(N_BLK, OFFS, EPT))
```

```python
import functools

import jax
import jax.numpy as jnp
from jax import lax
from jax.experimental import pallas as pl
from jax.experimental.pallas import tpu as pltpu
from jax.sharding import PartitionSpec as P

PASSES = 2
SOFTEN = 0.05
LANES = 128
SUB = 8
SPLITS = 2
BLOCK_ENTRIES = ((0, 0), (1, 1), (2, 2), (0, 1), (0, 2), (1, 2))
F32 = jnp.float32
BF16 = jnp.bfloat16


def rotation_entries(v):
    squared = v[0] * v[0] + v[1] * v[1] + v[2] * v[2]
    factor = 2.0 / (1.0 + squared)
    skewed = ((None, -v[2], v[1]), (v[2], None, -v[0]), (-v[1], v[0], None))
    rows = []
    for a in range(3):
        row = []
        for b in range(3):
            if a == b:
                row.append(1.0 + factor * (v[a] * v[a] - squared))
            else:
                row.append(factor * (skewed[a][b] + v[a] * v[b]))
        rows.append(row)
    return rows


def rotate(rows, y):
    return [rows[a][0] * y[0] + rows[a][1] * y[1] + rows[a][2] * y[2] for a in range(3)]


def rotate_back(rows, y):
    return [rows[0][a] * y[0] + rows[1][a] * y[1] + rows[2][a] * y[2] for a in range(3)]


class Sizes:
    def __init__(self, n_blk, n_rep, pairs, slots, cams):
        self.n_blk, self.n_rep = n_blk, n_rep
        self.pairs, self.slots, self.cams = pairs, slots, cams
        self.hi = cams // LANES
        self.tile_rows = 3 * self.hi
        self.chunks = slots // LANES
        assert pairs == SUB and slots % LANES == 0 and cams % (LANES * SUB) == 0 and n_blk % 2 == 0


def block_at(sz, row, c):
    return pl.ds((row * sz.chunks + c) * SUB, SUB)


def chunk(sz, ref, row, c):
    return ref[block_at(sz, row, c), :]


def gather3(sz, source, index):
    hi = lax.shift_right_logical(index, 7)
    lo = lax.bitwise_and(index, LANES - 1)
    out = [None] * 3
    for r in range(sz.hi):
        mask = hi == r
        for c in range(3):
            got = jnp.take_along_axis(source(c, r), lo, axis=1, mode="promise_in_bounds")
            out[c] = got if r == 0 else jnp.where(mask, got, out[c])
    return out


def far_source(sz, far):
    return lambda c, r: far[pl.ds((c * sz.hi + r) * SUB, SUB), :]


def own_source(sz, own):
    return lambda c, r: jnp.broadcast_to(own[pl.ds(c * sz.hi + r, 1), :], (SUB, LANES))


def build_far(sz, far, tile_at, b, sign):
    for k in range(sz.pairs):
        t = lax.rem(b + (sign * k + sz.n_blk), sz.n_blk)
        far[pl.ds(k, sz.tile_rows, stride=SUB), :] = tile_at(k % 2, lax.div(t, 2))


def store_split(sz, vals, ch, c, value):
    high = value.astype(BF16).astype(F32)
    vals[block_at(sz, 2 * ch, c), :] = high
    vals[block_at(sz, 2 * ch + 1, c), :] = value - high


def scatter(sz, channels, vals, index_ref, index_row, lhs, rhs):
    lane_iota = lax.broadcasted_iota(jnp.int32, (LANES, LANES), 0)
    row_iota = lax.broadcasted_iota(jnp.int32, (sz.hi, LANES), 0)
    for c in range(sz.chunks):
        for k in range(sz.pairs):
            one = lambda ref, row: ref[pl.ds((row * sz.chunks + c) * SUB + k, 1), :]
            columns = pl.ds((c * sz.pairs + k) * LANES, LANES)
            index = one(index_ref, index_row).astype(jnp.int32)
            lo = lax.bitwise_and(index, LANES - 1)
            mask = row_iota == lax.shift_right_logical(index, 7)
            rhs[:, columns] = jnp.where(lane_iota == lo, 1.0, 0.0).astype(BF16)
            for part in range(SPLITS):
                for ch in range(channels):
                    block = jnp.where(mask, one(vals, 2 * ch + part), 0.0).astype(BF16)
                    lhs[pl.ds((part * channels + ch) * sz.hi, sz.hi), columns] = block
    rows = SPLITS * channels * sz.hi
    out = lax.dot_general(
        lhs[pl.ds(0, rows), :], rhs[...], (((1,), (1,)), ((), ())), preferred_element_type=F32
    )
    half = channels * sz.hi
    return out[:half] + out[half:]


MEAS, ROT, CONF, FIRST, SECOND = 0, 3, 6, 9, 10
CHANNELS = 11


def pack_kernel(sz, meas, rot, conf, first, second, counts, start, anchor, table, est, est_copies, anchor_out, *sends):
    for c in range(sz.chunks):
        lanes = pl.ds(c * LANES, LANES)
        slot = lax.broadcasted_iota(jnp.int32, (sz.pairs, LANES), 1) + c * LANES
        live = slot < counts[...]
        for i in range(3):
            table[block_at(sz, MEAS + i, c), :] = meas[i, :, lanes]
            table[block_at(sz, ROT + i, c), :] = rot[i, :, lanes]
            table[block_at(sz, CONF + i, c), :] = jnp.where(live, conf[i, :, lanes], 0.0)
        table[block_at(sz, FIRST, c), :] = first[:, lanes].astype(F32)
        table[block_at(sz, SECOND, c), :] = second[:, lanes].astype(F32)
    count = CHANNELS * sz.chunks
    for k in range(1, sz.pairs):
        sends[k - 1][...] = table[pl.ds(k, count, stride=SUB), :]
    for c in range(3):
        for r in range(sz.hi):
            est[pl.ds(c * sz.hi + r, 1), :] = start[pl.ds(c, 1), pl.ds(r * LANES, LANES)]
    for r in range(sz.hi):
        anchor_out[pl.ds(r, 1), :] = anchor[:, pl.ds(r * LANES, LANES)]
    for i in range(sz.n_blk // 2):
        est_copies[i] = est[...]


def step_factors(scal, n):
    total = scal[0]
    for i in range(1, n):
        total = total + scal[i]
    s = [jnp.sum(total[i : i + 1, :], axis=1, keepdims=True) for i in range(4)]
    alpha0 = s[0] / s[1]
    rz1 = alpha0 * alpha0 * s[2] - s[0]
    onward = 1.0 + rz1 / s[0]
    curve = onward * onward * s[1] - 2.0 * onward * alpha0 * s[2] + alpha0 * alpha0 * s[3]
    alpha1 = rz1 / curve
    return alpha0 + alpha1 * onward, -alpha1 * alpha0


def misfit_kernel(sz, first_pass, b_ref, *refs):
    refs = list(refs)
    take = lambda count: [refs.pop(0) for _ in range(count)]
    (table,) = take(1)
    recvs = take(sz.pairs - 1) if first_pass else take(1)
    est_a, est_b, own = take(3)
    if not first_pass:
        z_a, z_b, u_a, u_b, z, u, scal = take(7)
    if first_pass:
        (table_in,) = take(1)
    wc_out, wc_in, sums = take(3)
    if not first_pass:
        weights_ref, own_new = take(2)
    far, vals, lhs, rhs = refs
    b = b_ref[0]
    if first_pass:
        count = CHANNELS * sz.chunks
        table_in[pl.ds(0, count, stride=SUB), :] = table[pl.ds(0, count, stride=SUB), :]
        for k in range(1, sz.pairs):
            table_in[pl.ds(k, count, stride=SUB), :] = recvs[k - 1][...]
        est_ref = own

        def tile_at(parity, q):
            return (est_b if parity else est_a)[q]
    else:
        table_in = recvs[0]
        along_z, along_u = step_factors(scal, sz.n_blk * sz.n_rep)
        own_new[...] = own[...] + along_z * z[...] + along_u * u[...]
        est_ref = own_new

        def tile_at(parity, q):
            e, zz, uu = (est_b, z_b, u_b) if parity else (est_a, z_a, u_a)
            return e[q] + along_z * zz[q] + along_u * uu[q]

    total = None
    for incoming in (False, True):
        edges = table_in if incoming else table
        wc_ref = wc_in if incoming else wc_out
        build_far(sz, far, tile_at, b, -1 if incoming else 1)
        for c in range(sz.chunks):
            first = chunk(sz, edges, FIRST, c).astype(jnp.int32)
            second = chunk(sz, edges, SECOND, c).astype(jnp.int32)
            rows = rotation_entries([chunk(sz, edges, ROT + i, c) for i in range(3)])
            if incoming:
                at_first = gather3(sz, far_source(sz, far), first)
                at_second = gather3(sz, own_source(sz, est_ref), second)
            else:
                at_first = gather3(sz, own_source(sz, est_ref), first)
                at_second = gather3(sz, far_source(sz, far), second)
            turned = rotate(rows, at_first)
            misfit = [chunk(sz, edges, MEAS + i, c) - (at_second[i] - turned[i]) for i in range(3)]
            conf = [chunk(sz, edges, CONF + i, c) for i in range(3)]
            energy = conf[0] * misfit[0] * misfit[0] + conf[1] * misfit[1] * misfit[1] + conf[2] * misfit[2] * misfit[2]
            weight = 1.0 / jnp.sqrt(energy + SOFTEN * SOFTEN)
            if not first_pass and not incoming:
                weights_ref[:, pl.ds(c * LANES, LANES)] = jnp.where(conf[0] > 0.0, weight, 0.0)
            wc = [weight * conf[i] for i in range(3)]
            for i in range(3):
                wc_ref[block_at(sz, i, c), :] = wc[i]
            push = [wc[i] * misfit[i] for i in range(3)]
            if incoming:
                for i in range(3):
                    store_split(sz, vals, i, c, push[i])
                    store_split(sz, vals, 3 + i, c, wc[i])
            else:
                back = rotate_back(rows, push)
                for i in range(3):
                    store_split(sz, vals, i, c, -back[i])
                for n, (p, q) in enumerate(BLOCK_ENTRIES):
                    entry = sum(rows[i][p] * wc[i] * rows[i][q] for i in range(3))
                    store_split(sz, vals, 3 + n, c, entry)
        channels = 6 if incoming else 9
        part = scatter(sz, channels, vals, edges, SECOND if incoming else FIRST, lhs, rhs)
        if incoming:
            cut = 6 * sz.hi
            sums[pl.ds(0, cut), :] = sums[pl.ds(0, cut), :] + part
        else:
            sums[...] = part


def apply_inverse(sz, inv, v):
    a00, a11, a22, a01, a02, a12 = inv
    return [
        a00 * v[0] + a01 * v[1] + a02 * v[2],
        a01 * v[0] + a11 * v[1] + a12 * v[2],
        a02 * v[0] + a12 * v[1] + a22 * v[2],
    ]


def comp(sz, ref, i):
    return ref[pl.ds(i * sz.hi, sz.hi), :]


def precond_kernel(sz, mine, other, est, anchor, residual, inverse, z, z_copies):
    total = mine[...] + other[...]
    part = lambda i: total[i * sz.hi : (i + 1) * sz.hi]
    anc = anchor[...]
    res = [part(i) - anc * comp(sz, est, i) for i in range(3)]
    p00, p11, p22 = [part(3 + i) + anc for i in range(3)]
    p01, p02, p12 = [part(6 + i) for i in range(3)]
    adj00 = p11 * p22 - p12 * p12
    adj01 = p02 * p12 - p01 * p22
    adj02 = p01 * p12 - p02 * p11
    adj11 = p00 * p22 - p02 * p02
    adj12 = p01 * p02 - p00 * p12
    adj22 = p00 * p11 - p01 * p01
    det = p00 * adj00 + p01 * adj01 + p02 * adj02
    inv = [a / det for a in (adj00, adj11, adj22, adj01, adj02, adj12)]
    scaled = apply_inverse(sz, inv, res)
    for i in range(3):
        residual[pl.ds(i * sz.hi, sz.hi), :] = res[i]
        z[pl.ds(i * sz.hi, sz.hi), :] = scaled[i]
    for i in range(6):
        inverse[pl.ds(i * sz.hi, sz.hi), :] = inv[i]
    for i in range(sz.n_blk // 2):
        z_copies[i] = z[...]


def image_kernel(sz, b_ref, table, table_in, wc_out, wc_in, z_a, z_b, z, sums, far, vals, lhs, rhs):
    b = b_ref[0]

    def tile_at(parity, q):
        return (z_b if parity else z_a)[q]

    for incoming in (False, True):
        edges = table_in if incoming else table
        wc_ref = wc_in if incoming else wc_out
        build_far(sz, far, tile_at, b, -1 if incoming else 1)
        for c in range(sz.chunks):
            first = chunk(sz, edges, FIRST, c).astype(jnp.int32)
            second = chunk(sz, edges, SECOND, c).astype(jnp.int32)
            rows = rotation_entries([chunk(sz, edges, ROT + i, c) for i in range(3)])
            if incoming:
                at_first = gather3(sz, far_source(sz, far), first)
                at_second = gather3(sz, own_source(sz, z), second)
            else:
                at_first = gather3(sz, own_source(sz, z), first)
                at_second = gather3(sz, far_source(sz, far), second)
            turned = rotate(rows, at_first)
            push = [chunk(sz, wc_ref, i, c) * (at_second[i] - turned[i]) for i in range(3)]
            if incoming:
                for i in range(3):
                    store_split(sz, vals, i, c, push[i])
            else:
                back = rotate_back(rows, push)
                for i in range(3):
                    store_split(sz, vals, i, c, -back[i])
        part = scatter(sz, 3, vals, edges, SECOND if incoming else FIRST, lhs, rhs)
        if incoming:
            sums[...] = sums[...] + part
        else:
            sums[...] = part


def second_precond_kernel(sz, mine, other, z, anchor, inverse, w, u, u_copies):
    total = mine[...] + other[...]
    anc = anchor[...]
    image = [total[i * sz.hi : (i + 1) * sz.hi] + anc * comp(sz, z, i) for i in range(3)]
    scaled = apply_inverse(sz, [comp(sz, inverse, i) for i in range(6)], image)
    for i in range(3):
        w[pl.ds(i * sz.hi, sz.hi), :] = image[i]
        u[pl.ds(i * sz.hi, sz.hi), :] = scaled[i]
    for i in range(sz.n_blk // 2):
        u_copies[i] = u[...]


def fold(value):
    rows = value.shape[0]
    out = value[:SUB]
    for i in range(1, rows // SUB):
        out = out + value[i * SUB : (i + 1) * SUB]
    return out


def products_kernel(sz, b_ref, table, wc_out, u_a, u_b, residual, z, w, u, anchor, scal, far):
    b = b_ref[0]

    def tile_at(parity, q):
        return (u_b if parity else u_a)[q]

    build_far(sz, far, tile_at, b, 1)
    acc = jnp.zeros((SUB, LANES), F32)
    for c in range(sz.chunks):
        first = chunk(sz, table, FIRST, c).astype(jnp.int32)
        second = chunk(sz, table, SECOND, c).astype(jnp.int32)
        rows = rotation_entries([chunk(sz, table, ROT + i, c) for i in range(3)])
        at_first = gather3(sz, own_source(sz, u), first)
        at_second = gather3(sz, far_source(sz, far), second)
        turned = rotate(rows, at_first)
        for i in range(3):
            gap = at_second[i] - turned[i]
            acc = acc + chunk(sz, wc_out, i, c) * gap * gap
    share = 1.0 / sz.n_rep
    res, zz, ww, uu = residual[...], z[...], w[...], u[...]
    s1 = fold(res * zz) * share
    s2 = fold(zz * ww) * share
    s3 = fold(ww * uu) * share
    anc = anchor[...]
    s4 = acc + share * fold(anc * (comp(sz, u, 0) * comp(sz, u, 0) + comp(sz, u, 1) * comp(sz, u, 1) + comp(sz, u, 2) * comp(sz, u, 2)))
    block = [jnp.sum(s, axis=0, keepdims=True) for s in (s1, s2, s3, s4)]
    block = jnp.concatenate(block + [jnp.zeros((SUB - 4, LANES), F32)], axis=0)
    for i in range(sz.n_blk * sz.n_rep):
        scal[i] = block


def final_kernel(sz, est, z, u, scal, out):
    along_z, along_u = step_factors(scal, sz.n_blk * sz.n_rep)
    new = est[...] + along_z * z[...] + along_u * u[...]
    for c in range(3):
        for r in range(sz.hi):
            row = c * sz.hi + r
            out[pl.ds(c, 1), pl.ds(r * LANES, LANES)] = new[row : row + 1]


def on_device(measured, rot_vector, confidence, first_local, second_local, edge_counts, start_angles, anchor):
    n_blk, n_rep = lax.axis_size("blk"), lax.axis_size("rep")
    sz = Sizes(n_blk, n_rep, first_local.shape[1], first_local.shape[2], start_angles.shape[1])
    half = n_blk // 2
    tile = (sz.tile_rows, LANES)
    f32 = lambda *shape: jax.ShapeDtypeStruct(shape, F32)
    b = lax.axis_index("blk").astype(jnp.int32).reshape(1)
    smem = pl.BlockSpec(memory_space=pltpu.SMEM)
    vmem = pl.BlockSpec(memory_space=pltpu.VMEM)
    wide = sz.pairs * sz.slots
    rows = sz.chunks * SUB

    def scratch(channels):
        return [
            pltpu.VMEM((sz.tile_rows * SUB, LANES), F32),
            pltpu.VMEM((channels * 2 * rows, LANES), F32),
            pltpu.VMEM((SPLITS * channels * sz.hi, wide), BF16),
            pltpu.VMEM((LANES, wide), BF16),
        ]

    def call(kernel, name, outs, args, scalars=0, scratch_shapes=()):
        return pl.pallas_call(
            kernel,
            name=name,
            out_shape=outs,
            in_specs=[smem] * scalars + [vmem] * (len(args) - scalars),
            out_specs=[vmem] * len(outs),
            scratch_shapes=list(scratch_shapes),
            compiler_params=pltpu.CompilerParams(vmem_limit_bytes=48 * 1024 * 1024),
        )(*args)

    groups = [[core + 2 * i for i in range(half)] for core in range(2)]
    swap = [(i, i ^ 1) for i in range(n_blk)]

    def all_tiles(copies):
        same = lax.all_to_all(copies, "blk", 0, 0, axis_index_groups=groups)
        return same, lax.ppermute(same, "blk", swap)

    def other_half(value):
        if n_rep == 2:
            return lax.ppermute(value, "rep", [(0, 1), (1, 0)])
        return lax.psum(value, "rep") - value

    def all_products(scal):
        return lax.all_to_all(scal, ("blk", "rep"), 0, 0)

    packed = call(
        functools.partial(pack_kernel, sz),
        "pack",
        [f32(CHANNELS * rows, LANES), f32(*tile), f32(half, *tile), f32(sz.hi, LANES)]
        + [f32(CHANNELS * sz.chunks, LANES)] * (sz.pairs - 1),
        [measured[:, 0], rot_vector[:, 0], confidence[:, 0], first_local[0], second_local[0], edge_counts[0], start_angles, anchor.reshape(1, -1)],
    )
    table, est, est_copies, anchor_rows = packed[:4]
    recvs = [
        lax.ppermute(packed[4 + k - 1], "blk", [(i, (i + k) % n_blk) for i in range(n_blk)])
        for k in range(1, sz.pairs)
    ]
    est_a, est_b = all_tiles(est_copies)

    wc_shape = f32(3 * rows, LANES)
    sums_shape = f32(9 * sz.hi, LANES)
    for sweep in range(PASSES):
        if sweep == 0:
            table_in, wc_out, wc_in, sums = call(
                functools.partial(misfit_kernel, sz, True),
                "misfit_first",
                [f32(CHANNELS * rows, LANES), wc_shape, wc_shape, sums_shape],
                [b, table, *recvs, est_a, est_b, est],
                1,
                scratch(9),
            )
        else:
            wc_out, wc_in, sums, weights, est = call(
                functools.partial(misfit_kernel, sz, False),
                "misfit_next",
                [wc_shape, wc_shape, sums_shape, f32(sz.pairs, sz.slots), f32(*tile)],
                [b, table, table_in, est_a, est_b, est, z_a, z_b, u_a, u_b, z, u, scal],
                1,
                scratch(9),
            )
        residual, inverse, z, z_copies = call(
            functools.partial(precond_kernel, sz),
            "precond",
            [f32(*tile), f32(6 * sz.hi, LANES), f32(*tile), f32(half, *tile)],
            [sums, other_half(sums), est, anchor_rows],
        )
        z_a, z_b = all_tiles(z_copies)
        (sums,) = call(
            functools.partial(image_kernel, sz),
            "image",
            [f32(*tile)],
            [b, table, table_in, wc_out, wc_in, z_a, z_b, z],
            1,
            scratch(3),
        )
        w, u, u_copies = call(
            functools.partial(second_precond_kernel, sz),
            "second_precond",
            [f32(*tile), f32(*tile), f32(half, *tile)],
            [sums, other_half(sums), z, anchor_rows, inverse],
        )
        u_a, u_b = all_tiles(u_copies)
        (scal,) = call(
            functools.partial(products_kernel, sz),
            "products",
            [f32(n_blk * n_rep, SUB, LANES)],
            [b, table, wc_out, u_a, u_b, residual, z, w, u, anchor_rows],
            1,
            [pltpu.VMEM((sz.tile_rows * SUB, LANES), F32)],
        )
        scal = all_products(scal)
    (estimate,) = call(functools.partial(final_kernel, sz), "final", [f32(3, sz.cams)], [est, z, u, scal])
    return (estimate, weights[None])


def solution(mesh):
    return jax.shard_map(
        on_device,
        mesh=mesh,
        in_specs=(
            P(None, "blk", None, "rep"),
            P(None, "blk", None, "rep"),
            P(None, "blk", None, "rep"),
            P("blk", None, "rep"),
            P("blk", None, "rep"),
            P("blk", None, "rep"),
            P(None, "blk"),
            P("blk"),
        ),
        out_specs=(P(None, "blk"), P("blk", None, "rep")),
        check_vma=False,
    )
```

```python
import functools

import jax
import jax.numpy as jnp
from jax import lax
from jax.experimental import pallas as pl
from jax.experimental.pallas import tpu as pltpu
from jax.sharding import PartitionSpec as P

PASSES = 2
SOFTEN = 0.05
LANES = 128
SUB = 8
SPLITS = 2
BLOCK_ENTRIES = ((0, 0), (1, 1), (2, 2), (0, 1), (0, 2), (1, 2))
MEAS, ROT, CONF, FIRST, SECOND = 0, 3, 6, 9, 10
CHANNELS = 11
F32 = jnp.float32
BF16 = jnp.bfloat16


def rotation_entries(v):
    squared = v[0] * v[0] + v[1] * v[1] + v[2] * v[2]
    factor = 2.0 / (1.0 + squared)
    skewed = ((None, -v[2], v[1]), (v[2], None, -v[0]), (-v[1], v[0], None))
    rows = []
    for a in range(3):
        row = []
        for b in range(3):
            if a == b:
                row.append(1.0 + factor * (v[a] * v[a] - squared))
            else:
                row.append(factor * (skewed[a][b] + v[a] * v[b]))
        rows.append(row)
    return rows


def rotate(rows, y):
    return [rows[a][0] * y[0] + rows[a][1] * y[1] + rows[a][2] * y[2] for a in range(3)]


def rotate_back(rows, y):
    return [rows[0][a] * y[0] + rows[1][a] * y[1] + rows[2][a] * y[2] for a in range(3)]


class Sizes:
    def __init__(self, n_blk, n_rep, pairs, slots, cams):
        self.n_blk, self.n_rep = n_blk, n_rep
        self.pairs, self.slots, self.cams = pairs, slots, cams
        self.hi = cams // LANES
        self.tile_rows = 3 * self.hi
        self.chunks = slots // LANES
        self.edge_rows = CHANNELS * self.chunks
        assert pairs == SUB and slots % LANES == 0 and cams % (LANES * SUB) == 0 and n_blk % 2 == 0


def block_at(sz, row, c):
    return pl.ds((row * sz.chunks + c) * SUB, SUB)


def chunk(sz, ref, row, c):
    return ref[block_at(sz, row, c), :]


def gather3(sz, source, index):
    hi = lax.shift_right_logical(index, 7)
    lo = lax.bitwise_and(index, LANES - 1)
    out = [None] * 3
    for r in range(sz.hi):
        mask = hi == r
        for c in range(3):
            got = jnp.take_along_axis(source(c, r), lo, axis=1, mode="promise_in_bounds")
            out[c] = got if r == 0 else jnp.where(mask, got, out[c])
    return out


def far_source(sz, far):
    return lambda c, r: far[pl.ds((c * sz.hi + r) * SUB, SUB), :]


def own_source(sz, own):
    return lambda c, r: jnp.broadcast_to(own[pl.ds(c * sz.hi + r, 1), :], (SUB, LANES))


def build_far(sz, far, tile_at, b, sign):
    for k in range(sz.pairs):
        t = lax.rem(b + (sign * k + sz.n_blk), sz.n_blk)
        far[pl.ds(k, sz.tile_rows, stride=SUB), :] = tile_at(k % 2, lax.div(t, 2))


def store_split(sz, vals, ch, c, value):
    high = value.astype(BF16).astype(F32)
    vals[block_at(sz, 2 * ch, c), :] = high
    vals[block_at(sz, 2 * ch + 1, c), :] = value - high


def scatter(sz, channels, vals, index_ref, index_row, lhs, rhs):
    lane_iota = lax.broadcasted_iota(jnp.int32, (LANES, LANES), 0).astype(F32).astype(BF16)
    row_iota = lax.broadcasted_iota(jnp.int32, (sz.hi, LANES), 0).astype(F32).astype(BF16)
    one, zero = jnp.ones((), BF16), jnp.zeros((), BF16)
    for c in range(sz.chunks):
        index = chunk(sz, index_ref, index_row, c).astype(jnp.int32)
        lows = lax.bitwise_and(index, LANES - 1).astype(F32)
        highs = lax.shift_right_logical(index, 7).astype(F32)
        for k in range(sz.pairs):
            columns = pl.ds((c * sz.pairs + k) * LANES, LANES)
            lo = jnp.broadcast_to(lows[k : k + 1], (sz.hi, LANES)).astype(BF16)
            hi = jnp.broadcast_to(highs[k : k + 1], (sz.hi, LANES)).astype(BF16)
            for n in range(LANES // sz.hi):
                at = pl.ds(n * sz.hi, sz.hi)
                rhs[at, columns] = jnp.where(lane_iota[n * sz.hi : (n + 1) * sz.hi] == lo, one, zero)
            mask = row_iota == hi
            for part in range(SPLITS):
                for ch in range(channels):
                    row = vals[pl.ds(((2 * ch + part) * sz.chunks + c) * SUB + k, 1), :]
                    block = jnp.where(mask, jnp.broadcast_to(row, (sz.hi, LANES)).astype(BF16), zero)
                    lhs[pl.ds((part * channels + ch) * sz.hi, sz.hi), columns] = block
    rows = SPLITS * channels * sz.hi
    out = lax.dot_general(
        lhs[pl.ds(0, rows), :], rhs[...], (((1,), (1,)), ((), ())), preferred_element_type=F32
    )
    half = channels * sz.hi
    return out[:half] + out[half:]


def pack_kernel(sz, *refs):
    hbm, (table, est, anchor_out, send), local, sems = refs[:8], refs[8:12], refs[12:20], refs[20]
    copies = [pltpu.make_async_copy(src, dst, sems.at[i]) for i, (src, dst) in enumerate(zip(hbm, local))]
    for copy in copies:
        copy.start()
    for copy in copies:
        copy.wait()
    meas, rot, conf, first, second, counts, start, anchor = local
    b = lax.axis_index("blk")
    for c in range(sz.chunks):
        lanes = pl.ds(c * LANES, LANES)
        slot = lax.broadcasted_iota(jnp.int32, (sz.pairs, LANES), 1) + c * LANES
        live = slot < counts[...]
        for i in range(3):
            table[block_at(sz, MEAS + i, c), :] = meas[i, :, lanes]
            table[block_at(sz, ROT + i, c), :] = rot[i, :, lanes]
            table[block_at(sz, CONF + i, c), :] = jnp.where(live, conf[i, :, lanes], 0.0)
        table[block_at(sz, FIRST, c), :] = first[:, lanes].astype(F32)
        table[block_at(sz, SECOND, c), :] = second[:, lanes].astype(F32)
    for c in range(3):
        for r in range(sz.hi):
            est[pl.ds(c * sz.hi + r, 1), :] = start[pl.ds(c, 1), pl.ds(r * LANES, LANES)]
    for r in range(sz.hi):
        anchor_out[pl.ds(r, 1), :] = anchor[:, pl.ds(r * LANES, LANES)]
    parity = lax.rem(b, 2)
    count = sz.edge_rows
    for q in range(sz.n_blk // 2):
        for other in range(2):
            core = (1 - parity) if other else parity
            k = jnp.minimum(lax.rem(2 * q + core - b + sz.n_blk, sz.n_blk), sz.pairs - 1)
            at = count + sz.tile_rows if other else 0
            send[q, pl.ds(at, count), :] = table[pl.ds(k, count, stride=SUB), :]
        send[q, pl.ds(count, sz.tile_rows), :] = est[...]


def step_factors(scal, n):
    total = scal[0]
    for i in range(1, n):
        total = total + scal[i]
    s = [jnp.sum(total[i : i + 1, :], axis=1, keepdims=True) for i in range(4)]
    alpha0 = s[0] / s[1]
    rz1 = alpha0 * alpha0 * s[2] - s[0]
    onward = 1.0 + rz1 / s[0]
    curve = onward * onward * s[1] - 2.0 * onward * alpha0 * s[2] + alpha0 * alpha0 * s[3]
    alpha1 = rz1 / curve
    return alpha0 + alpha1 * onward, -alpha1 * alpha0


def gathered_change(sz, edges, far, own, incoming, c, rows):
    first = chunk(sz, edges, FIRST, c).astype(jnp.int32)
    second = chunk(sz, edges, SECOND, c).astype(jnp.int32)
    if incoming:
        at_first = gather3(sz, far_source(sz, far), first)
        at_second = gather3(sz, own_source(sz, own), second)
    else:
        at_first = gather3(sz, own_source(sz, own), first)
        at_second = gather3(sz, far_source(sz, far), second)
    turned = rotate(rows, at_first)
    return [at_second[i] - turned[i] for i in range(3)]


def edge_rotation(sz, edges, c):
    return rotation_entries([chunk(sz, edges, ROT + i, c) for i in range(3)])


def put3(sz, ref, c, values):
    for i in range(3):
        ref[block_at(sz, i, c), :] = values[i]


def get3(sz, ref, c):
    return [chunk(sz, ref, i, c) for i in range(3)]


def misfit_sums(sz, incoming, misfit_of, edges, wc_ref, weights_ref, sums, vals, lhs, rhs):
    for c in range(sz.chunks):
        rows = None
        if not incoming:
            rows = edge_rotation(sz, edges, c)
        misfit = misfit_of(c, rows)
        conf = [chunk(sz, edges, CONF + i, c) for i in range(3)]
        energy = conf[0] * misfit[0] * misfit[0] + conf[1] * misfit[1] * misfit[1] + conf[2] * misfit[2] * misfit[2]
        weight = 1.0 / jnp.sqrt(energy + SOFTEN * SOFTEN)
        if weights_ref is not None:
            weights_ref[:, pl.ds(c * LANES, LANES)] = jnp.where(conf[0] > 0.0, weight, 0.0)
        wc = [weight * conf[i] for i in range(3)]
        put3(sz, wc_ref, c, wc)
        push = [wc[i] * misfit[i] for i in range(3)]
        if incoming:
            for i in range(3):
                store_split(sz, vals, i, c, push[i])
                store_split(sz, vals, 3 + i, c, wc[i])
        else:
            back = rotate_back(rows, push)
            for i in range(3):
                store_split(sz, vals, i, c, -back[i])
            for n, (p, q) in enumerate(BLOCK_ENTRIES):
                entry = sum(rows[i][p] * wc[i] * rows[i][q] for i in range(3))
                store_split(sz, vals, 3 + n, c, entry)
    part = scatter(sz, 6 if incoming else 9, vals, edges, SECOND if incoming else FIRST, lhs, rhs)
    if incoming:
        cut = 6 * sz.hi
        sums[pl.ds(0, cut), :] = sums[pl.ds(0, cut), :] + part
    else:
        sums[...] = part


def first_misfit_kernel(sz, table, same, other, own, table_in, gap_out, gap_in, wc_out, wc_in, sums, far, vals, lhs, rhs):
    b = lax.axis_index("blk")
    count = sz.edge_rows
    table_in[pl.ds(0, count, stride=SUB), :] = table[pl.ds(0, count, stride=SUB), :]
    for k in range(1, sz.pairs):
        q = lax.div(lax.rem(b + (sz.n_blk - k), sz.n_blk), 2)
        if k % 2:
            block = other[q, pl.ds(count + sz.tile_rows, count), :]
        else:
            block = same[q, pl.ds(0, count), :]
        table_in[pl.ds(k, count, stride=SUB), :] = block

    def tile_at(parity, q):
        return (other if parity else same)[q, pl.ds(count, sz.tile_rows), :]

    for incoming in (False, True):
        edges, gap, wc_ref = (table_in, gap_in, wc_in) if incoming else (table, gap_out, wc_out)
        build_far(sz, far, tile_at, b, -1 if incoming else 1)

        def misfit_of(c, rows):
            rows = edge_rotation(sz, edges, c) if rows is None else rows
            change = gathered_change(sz, edges, far, own, incoming, c, rows)
            misfit = [chunk(sz, edges, MEAS + i, c) - change[i] for i in range(3)]
            put3(sz, gap, c, misfit)
            return misfit

        misfit_sums(sz, incoming, misfit_of, edges, wc_ref, None, sums, vals, lhs, rhs)


def next_misfit_kernel(
    sz, table, table_in, gap_out, gap_in, z_out, z_in, u_out, u_in, own, z, u, scal,
    wc_out, wc_in, sums, weights, own_new, vals, lhs, rhs,
):
    along_z, along_u = step_factors(scal, sz.n_blk * sz.n_rep)
    own_new[...] = own[...] + along_z * z[...] + along_u * u[...]
    for incoming in (False, True):
        edges, wc_ref = (table_in, wc_in) if incoming else (table, wc_out)
        old, by_z, by_u = (gap_in, z_in, u_in) if incoming else (gap_out, z_out, u_out)

        def misfit_of(c, rows):
            old3, z3, u3 = get3(sz, old, c), get3(sz, by_z, c), get3(sz, by_u, c)
            return [old3[i] - (along_z * z3[i] + along_u * u3[i]) for i in range(3)]

        misfit_sums(sz, incoming, misfit_of, edges, wc_ref, None if incoming else weights, sums, vals, lhs, rhs)


def apply_inverse(sz, inv, v):
    a00, a11, a22, a01, a02, a12 = inv
    return [
        a00 * v[0] + a01 * v[1] + a02 * v[2],
        a01 * v[0] + a11 * v[1] + a12 * v[2],
        a02 * v[0] + a12 * v[1] + a22 * v[2],
    ]


def comp(sz, ref, i):
    return ref[pl.ds(i * sz.hi, sz.hi), :]


def precond_kernel(sz, mine, other, est, anchor, residual, inverse, z, z_copies):
    total = mine[...] + other[...]
    part = lambda i: total[i * sz.hi : (i + 1) * sz.hi]
    anc = anchor[...]
    res = [part(i) - anc * comp(sz, est, i) for i in range(3)]
    p00, p11, p22 = [part(3 + i) + anc for i in range(3)]
    p01, p02, p12 = [part(6 + i) for i in range(3)]
    adj00 = p11 * p22 - p12 * p12
    adj01 = p02 * p12 - p01 * p22
    adj02 = p01 * p12 - p02 * p11
    adj11 = p00 * p22 - p02 * p02
    adj12 = p01 * p02 - p00 * p12
    adj22 = p00 * p11 - p01 * p01
    det = p00 * adj00 + p01 * adj01 + p02 * adj02
    inv = [a / det for a in (adj00, adj11, adj22, adj01, adj02, adj12)]
    scaled = apply_inverse(sz, inv, res)
    for i in range(3):
        residual[pl.ds(i * sz.hi, sz.hi), :] = res[i]
        z[pl.ds(i * sz.hi, sz.hi), :] = scaled[i]
    for i in range(6):
        inverse[pl.ds(i * sz.hi, sz.hi), :] = inv[i]
    for i in range(sz.n_blk // 2):
        z_copies[i] = z[...]


def image_kernel(sz, keep, table, table_in, wc_out, wc_in, z_a, z_b, z, sums, *refs):
    kept, (far, vals, lhs, rhs) = refs[:-4], refs[-4:]
    b = lax.axis_index("blk")

    def tile_at(parity, q):
        return (z_b if parity else z_a)[q]

    for incoming in (False, True):
        edges, wc_ref = (table_in, wc_in) if incoming else (table, wc_out)
        build_far(sz, far, tile_at, b, -1 if incoming else 1)
        for c in range(sz.chunks):
            rows = edge_rotation(sz, edges, c)
            change = gathered_change(sz, edges, far, z, incoming, c, rows)
            if keep:
                put3(sz, kept[int(incoming)], c, change)
            wc = get3(sz, wc_ref, c)
            push = [wc[i] * change[i] for i in range(3)]
            if incoming:
                for i in range(3):
                    store_split(sz, vals, i, c, push[i])
            else:
                back = rotate_back(rows, push)
                for i in range(3):
                    store_split(sz, vals, i, c, -back[i])
        part = scatter(sz, 3, vals, edges, SECOND if incoming else FIRST, lhs, rhs)
        if incoming:
            sums[...] = sums[...] + part
        else:
            sums[...] = part


def second_precond_kernel(sz, mine, other, z, anchor, inverse, w, u, u_copies):
    total = mine[...] + other[...]
    anc = anchor[...]
    image = [total[i * sz.hi : (i + 1) * sz.hi] + anc * comp(sz, z, i) for i in range(3)]
    scaled = apply_inverse(sz, [comp(sz, inverse, i) for i in range(6)], image)
    for i in range(3):
        w[pl.ds(i * sz.hi, sz.hi), :] = image[i]
        u[pl.ds(i * sz.hi, sz.hi), :] = scaled[i]
    for i in range(sz.n_blk // 2):
        u_copies[i] = u[...]


def fold(value):
    rows = value.shape[0]
    out = value[:SUB]
    for i in range(1, rows // SUB):
        out = out + value[i * SUB : (i + 1) * SUB]
    return out


def products_kernel(sz, keep, table, *refs):
    refs = list(refs)
    table_in = refs.pop(0) if keep else None
    wc_out, u_a, u_b, residual, z, w, u, anchor, scal = refs[:9]
    kept, far = refs[9:-1], refs[-1]
    b = lax.axis_index("blk")

    def tile_at(parity, q):
        return (u_b if parity else u_a)[q]

    acc = jnp.zeros((SUB, LANES), F32)
    for incoming in (False, True) if keep else (False,):
        edges = table_in if incoming else table
        build_far(sz, far, tile_at, b, -1 if incoming else 1)
        for c in range(sz.chunks):
            change = gathered_change(sz, edges, far, u, incoming, c, edge_rotation(sz, edges, c))
            if keep:
                put3(sz, kept[int(incoming)], c, change)
            if not incoming:
                wc = get3(sz, wc_out, c)
                for i in range(3):
                    acc = acc + wc[i] * change[i] * change[i]
    share = 1.0 / sz.n_rep
    res, zz, ww, uu = residual[...], z[...], w[...], u[...]
    s1 = fold(res * zz) * share
    s2 = fold(zz * ww) * share
    s3 = fold(ww * uu) * share
    anc = anchor[...]
    s4 = acc + share * fold(anc * (comp(sz, u, 0) * comp(sz, u, 0) + comp(sz, u, 1) * comp(sz, u, 1) + comp(sz, u, 2) * comp(sz, u, 2)))
    block = [jnp.sum(s, axis=0, keepdims=True) for s in (s1, s2, s3, s4)]
    block = jnp.concatenate(block + [jnp.zeros((SUB - 4, LANES), F32)], axis=0)
    for i in range(sz.n_blk * sz.n_rep):
        scal[i] = block


def final_kernel(sz, est, z, u, scal, out):
    along_z, along_u = step_factors(scal, sz.n_blk * sz.n_rep)
    new = est[...] + along_z * z[...] + along_u * u[...]
    for c in range(3):
        for r in range(sz.hi):
            row = c * sz.hi + r
            out[pl.ds(c, 1), pl.ds(r * LANES, LANES)] = new[row : row + 1]


def on_device(measured, rot_vector, confidence, first_local, second_local, edge_counts, start_angles, anchor):
    n_blk, n_rep = lax.axis_size("blk"), lax.axis_size("rep")
    sz = Sizes(n_blk, n_rep, first_local.shape[1], first_local.shape[2], start_angles.shape[1])
    half = n_blk // 2
    tile = (sz.tile_rows, LANES)
    f32 = lambda *shape: jax.ShapeDtypeStruct(shape, F32)
    vmem = pl.BlockSpec(memory_space=pltpu.VMEM)
    wide = sz.pairs * sz.slots
    rows = sz.chunks * SUB
    far_shape = pltpu.VMEM((sz.tile_rows * SUB, LANES), F32)

    def sums_scratch(channels):
        return [
            pltpu.VMEM((channels * 2 * rows, LANES), F32),
            pltpu.VMEM((SPLITS * channels * sz.hi, wide), BF16),
            pltpu.VMEM((LANES, wide), BF16),
        ]

    def call(kernel, name, outs, args, scratch_shapes=(), spec=vmem):
        return pl.pallas_call(
            kernel,
            name=name,
            out_shape=outs,
            in_specs=[spec] * len(args),
            out_specs=[vmem] * len(outs),
            scratch_shapes=list(scratch_shapes),
            compiler_params=pltpu.CompilerParams(vmem_limit_bytes=48 * 1024 * 1024),
        )(*args)

    groups = [[core + 2 * i for i in range(half)] for core in range(2)]
    swap = [(i, i ^ 1) for i in range(n_blk)]

    def all_tiles(copies):
        same = lax.all_to_all(copies, "blk", 0, 0, axis_index_groups=groups)
        return same, lax.ppermute(same, "blk", swap)

    def other_half(value):
        if n_rep == 2:
            return lax.ppermute(value, "rep", [(0, 1), (1, 0)])
        return lax.psum(value, "rep") - value

    def all_products(scal):
        return lax.all_to_all(scal, ("blk", "rep"), 0, 0)

    inputs = [
        measured[:, 0], rot_vector[:, 0], confidence[:, 0], first_local[0], second_local[0], edge_counts[0],
        start_angles, anchor.reshape(1, -1),
    ]
    table_shape = f32(CHANNELS * rows, LANES)
    table, est, anchor_rows, send = call(
        functools.partial(pack_kernel, sz),
        "pack",
        [table_shape, f32(*tile), f32(sz.hi, LANES), f32(half, 2 * sz.edge_rows + sz.tile_rows, LANES)],
        inputs,
        [pltpu.VMEM(x.shape, x.dtype) for x in inputs] + [pltpu.SemaphoreType.DMA((len(inputs),))],
        pl.BlockSpec(memory_space=pltpu.HBM),
    )
    same, other = all_tiles(send)

    per_edge = f32(3 * rows, LANES)
    sums_shape = f32(9 * sz.hi, LANES)
    for sweep in range(PASSES):
        last = sweep + 1 == PASSES
        if sweep == 0:
            table_in, gap_out, gap_in, wc_out, wc_in, sums = call(
                functools.partial(first_misfit_kernel, sz),
                "misfit_first",
                [table_shape, per_edge, per_edge, per_edge, per_edge, sums_shape],
                [table, same, other, est],
                [far_shape] + sums_scratch(9),
            )
        else:
            wc_out, wc_in, sums, weights, est = call(
                functools.partial(next_misfit_kernel, sz),
                "misfit_next",
                [per_edge, per_edge, sums_shape, f32(sz.pairs, sz.slots), f32(*tile)],
                [table, table_in, gap_out, gap_in, z_out, z_in, u_out, u_in, est, z, u, scal],
                sums_scratch(9),
            )
        residual, inverse, z, z_copies = call(
            functools.partial(precond_kernel, sz),
            "precond",
            [f32(*tile), f32(6 * sz.hi, LANES), f32(*tile), f32(half, *tile)],
            [sums, other_half(sums), est, anchor_rows],
        )
        z_a, z_b = all_tiles(z_copies)
        sums, *kept = call(
            functools.partial(image_kernel, sz, not last),
            "image",
            [f32(*tile)] + ([] if last else [per_edge, per_edge]),
            [table, table_in, wc_out, wc_in, z_a, z_b, z],
            [far_shape] + sums_scratch(3),
        )
        if not last:
            z_out, z_in = kept
        w, u, u_copies = call(
            functools.partial(second_precond_kernel, sz),
            "second_precond",
            [f32(*tile), f32(*tile), f32(half, *tile)],
            [sums, other_half(sums), z, anchor_rows, inverse],
        )
        u_a, u_b = all_tiles(u_copies)
        scal, *kept = call(
            functools.partial(products_kernel, sz, not last),
            "products",
            [f32(n_blk * n_rep, SUB, LANES)] + ([] if last else [per_edge, per_edge]),
            [table] + ([] if last else [table_in]) + [wc_out, u_a, u_b, residual, z, w, u, anchor_rows],
            [far_shape],
        )
        if not last:
            u_out, u_in = kept
        scal = all_products(scal)
    (estimate,) = call(functools.partial(final_kernel, sz), "final", [f32(3, sz.cams)], [est, z, u, scal])
    return (estimate, weights[None])


def solution(mesh):
    return jax.shard_map(
        on_device,
        mesh=mesh,
        in_specs=(
            P(None, "blk", None, "rep"),
            P(None, "blk", None, "rep"),
            P(None, "blk", None, "rep"),
            P("blk", None, "rep"),
            P("blk", None, "rep"),
            P("blk", None, "rep"),
            P(None, "blk"),
            P("blk"),
        ),
        out_specs=(P(None, "blk"), P("blk", None, "rep")),
        check_vma=False,
    )
```

```python
import functools

import jax
import jax.numpy as jnp
from jax import lax
from jax.experimental import pallas as pl
from jax.experimental.pallas import tpu as pltpu
from jax.sharding import PartitionSpec as P

PASSES = 2
SOFTEN = 0.05
LANES = 128
SUB = 8
SPLITS = 2
BLOCK_ENTRIES = ((0, 0), (1, 1), (2, 2), (0, 1), (0, 2), (1, 2))
MEAS, ROT, CONF, FIRST, SECOND = 0, 3, 6, 9, 10
CHANNELS = 11
F32 = jnp.float32
BF16 = jnp.bfloat16


def rotation_entries(v):
    squared = v[0] * v[0] + v[1] * v[1] + v[2] * v[2]
    factor = 2.0 / (1.0 + squared)
    skewed = ((None, -v[2], v[1]), (v[2], None, -v[0]), (-v[1], v[0], None))
    rows = []
    for a in range(3):
        row = []
        for b in range(3):
            if a == b:
                row.append(1.0 + factor * (v[a] * v[a] - squared))
            else:
                row.append(factor * (skewed[a][b] + v[a] * v[b]))
        rows.append(row)
    return rows


def rotate(rows, y):
    return [rows[a][0] * y[0] + rows[a][1] * y[1] + rows[a][2] * y[2] for a in range(3)]


def rotate_back(rows, y):
    return [rows[0][a] * y[0] + rows[1][a] * y[1] + rows[2][a] * y[2] for a in range(3)]


class Sizes:
    def __init__(self, n_blk, n_rep, pairs, slots, cams):
        self.n_blk, self.n_rep = n_blk, n_rep
        self.pairs, self.slots, self.cams = pairs, slots, cams
        self.hi = cams // LANES
        self.tile_rows = 3 * self.hi
        self.chunks = slots // LANES
        self.edge_rows = CHANNELS * self.chunks
        assert pairs == SUB and slots % LANES == 0 and cams % (LANES * SUB) == 0 and n_blk % 2 == 0


def block_at(sz, row, c):
    return pl.ds((row * sz.chunks + c) * SUB, SUB)


def chunk(sz, ref, row, c):
    return ref[block_at(sz, row, c), :]


def gather3(sz, source, index):
    hi = lax.shift_right_logical(index, 7)
    lo = lax.bitwise_and(index, LANES - 1)
    out = [None] * 3
    for r in range(sz.hi):
        mask = hi == r
        for c in range(3):
            got = jnp.take_along_axis(source(c, r), lo, axis=1, mode="promise_in_bounds")
            out[c] = got if r == 0 else jnp.where(mask, got, out[c])
    return out


def far_source(sz, far):
    return lambda c, r: far[pl.ds((c * sz.hi + r) * SUB, SUB), :]


def own_source(sz, own):
    return lambda c, r: jnp.broadcast_to(own[pl.ds(c * sz.hi + r, 1), :], (SUB, LANES))


def build_far(sz, far, tile_at, b, sign):
    for k in range(sz.pairs):
        t = lax.rem(b + (sign * k + sz.n_blk), sz.n_blk)
        far[pl.ds(k, sz.tile_rows, stride=SUB), :] = tile_at(k % 2, lax.div(t, 2))


def store_split(sz, vals, ch, c, value):
    high = value.astype(BF16).astype(F32)
    vals[block_at(sz, 2 * ch, c), :] = high
    vals[block_at(sz, 2 * ch + 1, c), :] = value - high


def scatter(sz, channels, vals, index_ref, index_row, lhs, rhs):
    lane_iota = lax.broadcasted_iota(jnp.int32, (LANES, LANES), 0).astype(F32).astype(BF16)
    row_iota = lax.broadcasted_iota(jnp.int32, (sz.hi, LANES), 0).astype(F32).astype(BF16)
    one, zero = jnp.ones((), BF16), jnp.zeros((), BF16)
    for c in range(sz.chunks):
        index = chunk(sz, index_ref, index_row, c).astype(jnp.int32)
        lows = lax.bitwise_and(index, LANES - 1).astype(F32)
        highs = lax.shift_right_logical(index, 7).astype(F32)
        for k in range(sz.pairs):
            columns = pl.ds((c * sz.pairs + k) * LANES, LANES)
            lo = jnp.broadcast_to(lows[k : k + 1], (sz.hi, LANES)).astype(BF16)
            hi = jnp.broadcast_to(highs[k : k + 1], (sz.hi, LANES)).astype(BF16)
            for n in range(LANES // sz.hi):
                at = pl.ds(n * sz.hi, sz.hi)
                rhs[at, columns] = jnp.where(lane_iota[n * sz.hi : (n + 1) * sz.hi] == lo, one, zero)
            mask = row_iota == hi
            for part in range(SPLITS):
                for ch in range(channels):
                    row = vals[pl.ds(((2 * ch + part) * sz.chunks + c) * SUB + k, 1), :]
                    block = jnp.where(mask, jnp.broadcast_to(row, (sz.hi, LANES)).astype(BF16), zero)
                    lhs[pl.ds((part * channels + ch) * sz.hi, sz.hi), columns] = block
    rows = SPLITS * channels * sz.hi
    out = lax.dot_general(
        lhs[pl.ds(0, rows), :], rhs[...], (((1,), (1,)), ((), ())), preferred_element_type=F32
    )
    half = channels * sz.hi
    return out[:half] + out[half:]


def tile_kernel(sz, start, est, est_copies):
    for c in range(3):
        for r in range(sz.hi):
            est[pl.ds(c * sz.hi + r, 1), :] = start[pl.ds(c, 1), pl.ds(r * LANES, LANES)]
    for i in range(sz.n_blk // 2):
        est_copies[i] = est[...]


def pack_kernel(sz, meas, rot, conf, first, second, counts, anchor, after, table, anchor_out, *sends):
    b = lax.axis_index("blk")
    for c in range(sz.chunks):
        lanes = pl.ds(c * LANES, LANES)
        slot = lax.broadcasted_iota(jnp.int32, (sz.pairs, LANES), 1) + c * LANES
        live = slot < counts[...]
        for i in range(3):
            table[block_at(sz, MEAS + i, c), :] = meas[i, :, lanes]
            table[block_at(sz, ROT + i, c), :] = rot[i, :, lanes]
            table[block_at(sz, CONF + i, c), :] = jnp.where(live, conf[i, :, lanes], 0.0)
        table[block_at(sz, FIRST, c), :] = first[:, lanes].astype(F32)
        table[block_at(sz, SECOND, c), :] = second[:, lanes].astype(F32)
    for r in range(sz.hi):
        anchor_out[pl.ds(r, 1), :] = anchor[:, pl.ds(r * LANES, LANES)]
    step = 1 - 2 * lax.rem(b, 2)
    count = sz.edge_rows
    for m in range(1, sz.pairs // 2):
        sends[m - 1][pl.ds(0, count), :] = table[pl.ds(2 * m, count, stride=SUB), :]
        sends[m - 1][pl.ds(count, count), :] = table[pl.ds(2 * m + step, count, stride=SUB), :]
    sends[-1][...] = table[pl.ds(sz.pairs - 1, count, stride=SUB), :]


def relay_kernel(sz, table, *refs):
    recvs, relay = refs[:-1], refs[-1]
    even_core = lax.rem(lax.axis_index("blk"), 2) == 0
    count = sz.edge_rows
    steps = sz.pairs // 2
    for j in range(steps):
        if j == 0:
            from_even = table[pl.ds(1, count, stride=SUB), :]
        else:
            from_even = recvs[j - 1][pl.ds(count, count), :]
        if j + 1 < steps:
            from_odd = recvs[j][pl.ds(count, count), :]
        else:
            from_odd = recvs[-1][...]
        relay[pl.ds(j * count, count), :] = jnp.where(even_core, from_even, from_odd)


def step_factors(scal, n):
    total = scal[0]
    for i in range(1, n):
        total = total + scal[i]
    s = [jnp.sum(total[i : i + 1, :], axis=1, keepdims=True) for i in range(4)]
    alpha0 = s[0] / s[1]
    rz1 = alpha0 * alpha0 * s[2] - s[0]
    onward = 1.0 + rz1 / s[0]
    curve = onward * onward * s[1] - 2.0 * onward * alpha0 * s[2] + alpha0 * alpha0 * s[3]
    alpha1 = rz1 / curve
    return alpha0 + alpha1 * onward, -alpha1 * alpha0


def gathered_change(sz, edges, far, own, incoming, c, rows):
    first = chunk(sz, edges, FIRST, c).astype(jnp.int32)
    second = chunk(sz, edges, SECOND, c).astype(jnp.int32)
    if incoming:
        at_first = gather3(sz, far_source(sz, far), first)
        at_second = gather3(sz, own_source(sz, own), second)
    else:
        at_first = gather3(sz, own_source(sz, own), first)
        at_second = gather3(sz, far_source(sz, far), second)
    turned = rotate(rows, at_first)
    return [at_second[i] - turned[i] for i in range(3)]


def edge_rotation(sz, edges, c):
    return rotation_entries([chunk(sz, edges, ROT + i, c) for i in range(3)])


def put3(sz, ref, c, values):
    for i in range(3):
        ref[block_at(sz, i, c), :] = values[i]


def get3(sz, ref, c):
    return [chunk(sz, ref, i, c) for i in range(3)]


def misfit_sums(sz, incoming, misfit_of, edges, wc_ref, weights_ref, sums, vals, lhs, rhs):
    for c in range(sz.chunks):
        rows = None
        if not incoming:
            rows = edge_rotation(sz, edges, c)
        misfit = misfit_of(c, rows)
        conf = [chunk(sz, edges, CONF + i, c) for i in range(3)]
        energy = conf[0] * misfit[0] * misfit[0] + conf[1] * misfit[1] * misfit[1] + conf[2] * misfit[2] * misfit[2]
        weight = 1.0 / jnp.sqrt(energy + SOFTEN * SOFTEN)
        if weights_ref is not None:
            weights_ref[:, pl.ds(c * LANES, LANES)] = jnp.where(conf[0] > 0.0, weight, 0.0)
        wc = [weight * conf[i] for i in range(3)]
        put3(sz, wc_ref, c, wc)
        push = [wc[i] * misfit[i] for i in range(3)]
        if incoming:
            for i in range(3):
                store_split(sz, vals, i, c, push[i])
                store_split(sz, vals, 3 + i, c, wc[i])
        else:
            back = rotate_back(rows, push)
            for i in range(3):
                store_split(sz, vals, i, c, -back[i])
            for n, (p, q) in enumerate(BLOCK_ENTRIES):
                entry = sum(rows[i][p] * wc[i] * rows[i][q] for i in range(3))
                store_split(sz, vals, 3 + n, c, entry)
    part = scatter(sz, 6 if incoming else 9, vals, edges, SECOND if incoming else FIRST, lhs, rhs)
    if incoming:
        cut = 6 * sz.hi
        sums[pl.ds(0, cut), :] = sums[pl.ds(0, cut), :] + part
    else:
        sums[...] = part


def first_misfit(sz, incoming, edges, tile_at, own, gap, wc_ref, sums, far, vals, lhs, rhs):
    build_far(sz, far, tile_at, lax.axis_index("blk"), -1 if incoming else 1)

    def misfit_of(c, rows):
        rows = edge_rotation(sz, edges, c) if rows is None else rows
        change = gathered_change(sz, edges, far, own, incoming, c, rows)
        misfit = [chunk(sz, edges, MEAS + i, c) - change[i] for i in range(3)]
        put3(sz, gap, c, misfit)
        return misfit

    misfit_sums(sz, incoming, misfit_of, edges, wc_ref, None, sums, vals, lhs, rhs)


def outgoing_misfit_kernel(sz, table, est_a, est_b, own, gap, wc, sums, *scratch):
    tile_at = lambda parity, q: (est_b if parity else est_a)[q]
    first_misfit(sz, False, table, tile_at, own, gap, wc, sums, *scratch)


def incoming_misfit_kernel(sz, table, relayed, *refs):
    steps = sz.pairs // 2
    recvs, (est_a, est_b, own, sums_out, table_in, gap, wc, sums), scratch = refs[: steps - 1], refs[steps - 1 : -4], refs[-4:]
    count = sz.edge_rows
    for k in range(sz.pairs):
        if k == 0:
            block = table[pl.ds(0, count, stride=SUB), :]
        elif k % 2:
            block = relayed[pl.ds((k // 2) * count, count), :]
        else:
            block = recvs[k // 2 - 1][pl.ds(0, count), :]
        table_in[pl.ds(k, count, stride=SUB), :] = block
    sums[...] = sums_out[...]
    tile_at = lambda parity, q: (est_b if parity else est_a)[q]
    first_misfit(sz, True, table_in, tile_at, own, gap, wc, sums, *scratch)


def next_misfit_kernel(
    sz, table, table_in, gap_out, gap_in, z_out, z_in, u_out, u_in, own, z, u, scal,
    wc_out, wc_in, sums, weights, own_new, vals, lhs, rhs,
):
    along_z, along_u = step_factors(scal, sz.n_blk * sz.n_rep)
    own_new[...] = own[...] + along_z * z[...] + along_u * u[...]
    for incoming in (False, True):
        edges, wc_ref = (table_in, wc_in) if incoming else (table, wc_out)
        old, by_z, by_u = (gap_in, z_in, u_in) if incoming else (gap_out, z_out, u_out)

        def misfit_of(c, rows):
            old3, z3, u3 = get3(sz, old, c), get3(sz, by_z, c), get3(sz, by_u, c)
            return [old3[i] - (along_z * z3[i] + along_u * u3[i]) for i in range(3)]

        misfit_sums(sz, incoming, misfit_of, edges, wc_ref, None if incoming else weights, sums, vals, lhs, rhs)


def apply_inverse(sz, inv, v):
    a00, a11, a22, a01, a02, a12 = inv
    return [
        a00 * v[0] + a01 * v[1] + a02 * v[2],
        a01 * v[0] + a11 * v[1] + a12 * v[2],
        a02 * v[0] + a12 * v[1] + a22 * v[2],
    ]


def comp(sz, ref, i):
    return ref[pl.ds(i * sz.hi, sz.hi), :]


def precond_kernel(sz, mine, other, est, anchor, residual, inverse, z, z_copies):
    total = mine[...] + other[...]
    part = lambda i: total[i * sz.hi : (i + 1) * sz.hi]
    anc = anchor[...]
    res = [part(i) - anc * comp(sz, est, i) for i in range(3)]
    p00, p11, p22 = [part(3 + i) + anc for i in range(3)]
    p01, p02, p12 = [part(6 + i) for i in range(3)]
    adj00 = p11 * p22 - p12 * p12
    adj01 = p02 * p12 - p01 * p22
    adj02 = p01 * p12 - p02 * p11
    adj11 = p00 * p22 - p02 * p02
    adj12 = p01 * p02 - p00 * p12
    adj22 = p00 * p11 - p01 * p01
    det = p00 * adj00 + p01 * adj01 + p02 * adj02
    inv = [a / det for a in (adj00, adj11, adj22, adj01, adj02, adj12)]
    scaled = apply_inverse(sz, inv, res)
    for i in range(3):
        residual[pl.ds(i * sz.hi, sz.hi), :] = res[i]
        z[pl.ds(i * sz.hi, sz.hi), :] = scaled[i]
    for i in range(6):
        inverse[pl.ds(i * sz.hi, sz.hi), :] = inv[i]
    for i in range(sz.n_blk // 2):
        z_copies[i] = z[...]


def image_kernel(sz, keep, table, table_in, wc_out, wc_in, z_a, z_b, z, sums, *refs):
    kept, (far, vals, lhs, rhs) = refs[:-4], refs[-4:]
    b = lax.axis_index("blk")

    def tile_at(parity, q):
        return (z_b if parity else z_a)[q]

    for incoming in (False, True):
        edges, wc_ref = (table_in, wc_in) if incoming else (table, wc_out)
        build_far(sz, far, tile_at, b, -1 if incoming else 1)
        for c in range(sz.chunks):
            rows = edge_rotation(sz, edges, c)
            change = gathered_change(sz, edges, far, z, incoming, c, rows)
            if keep:
                put3(sz, kept[int(incoming)], c, change)
            wc = get3(sz, wc_ref, c)
            push = [wc[i] * change[i] for i in range(3)]
            if incoming:
                for i in range(3):
                    store_split(sz, vals, i, c, push[i])
            else:
                back = rotate_back(rows, push)
                for i in range(3):
                    store_split(sz, vals, i, c, -back[i])
        part = scatter(sz, 3, vals, edges, SECOND if incoming else FIRST, lhs, rhs)
        if incoming:
            sums[...] = sums[...] + part
        else:
            sums[...] = part


def second_precond_kernel(sz, mine, other, z, anchor, inverse, w, u, u_copies):
    total = mine[...] + other[...]
    anc = anchor[...]
    image = [total[i * sz.hi : (i + 1) * sz.hi] + anc * comp(sz, z, i) for i in range(3)]
    scaled = apply_inverse(sz, [comp(sz, inverse, i) for i in range(6)], image)
    for i in range(3):
        w[pl.ds(i * sz.hi, sz.hi), :] = image[i]
        u[pl.ds(i * sz.hi, sz.hi), :] = scaled[i]
    for i in range(sz.n_blk // 2):
        u_copies[i] = u[...]


def fold(value):
    rows = value.shape[0]
    out = value[:SUB]
    for i in range(1, rows // SUB):
        out = out + value[i * SUB : (i + 1) * SUB]
    return out


def products_kernel(sz, keep, table, *refs):
    refs = list(refs)
    table_in = refs.pop(0) if keep else None
    wc_out, u_a, u_b, residual, z, w, u, anchor, scal = refs[:9]
    kept, far = refs[9:-1], refs[-1]
    b = lax.axis_index("blk")

    def tile_at(parity, q):
        return (u_b if parity else u_a)[q]

    acc = jnp.zeros((SUB, LANES), F32)
    for incoming in (False, True) if keep else (False,):
        edges = table_in if incoming else table
        build_far(sz, far, tile_at, b, -1 if incoming else 1)
        for c in range(sz.chunks):
            change = gathered_change(sz, edges, far, u, incoming, c, edge_rotation(sz, edges, c))
            if keep:
                put3(sz, kept[int(incoming)], c, change)
            if not incoming:
                wc = get3(sz, wc_out, c)
                for i in range(3):
                    acc = acc + wc[i] * change[i] * change[i]
    share = 1.0 / sz.n_rep
    res, zz, ww, uu = residual[...], z[...], w[...], u[...]
    s1 = fold(res * zz) * share
    s2 = fold(zz * ww) * share
    s3 = fold(ww * uu) * share
    anc = anchor[...]
    s4 = acc + share * fold(anc * (comp(sz, u, 0) * comp(sz, u, 0) + comp(sz, u, 1) * comp(sz, u, 1) + comp(sz, u, 2) * comp(sz, u, 2)))
    block = [jnp.sum(s, axis=0, keepdims=True) for s in (s1, s2, s3, s4)]
    block = jnp.concatenate(block + [jnp.zeros((SUB - 4, LANES), F32)], axis=0)
    for i in range(sz.n_blk * sz.n_rep):
        scal[i] = block


def final_kernel(sz, est, z, u, scal, out):
    along_z, along_u = step_factors(scal, sz.n_blk * sz.n_rep)
    new = est[...] + along_z * z[...] + along_u * u[...]
    for c in range(3):
        for r in range(sz.hi):
            row = c * sz.hi + r
            out[pl.ds(c, 1), pl.ds(r * LANES, LANES)] = new[row : row + 1]


def on_device(measured, rot_vector, confidence, first_local, second_local, edge_counts, start_angles, anchor):
    n_blk, n_rep = lax.axis_size("blk"), lax.axis_size("rep")
    sz = Sizes(n_blk, n_rep, first_local.shape[1], first_local.shape[2], start_angles.shape[1])
    half = n_blk // 2
    tile = (sz.tile_rows, LANES)
    f32 = lambda *shape: jax.ShapeDtypeStruct(shape, F32)
    vmem = pl.BlockSpec(memory_space=pltpu.VMEM)
    wide = sz.pairs * sz.slots
    rows = sz.chunks * SUB
    far_shape = pltpu.VMEM((sz.tile_rows * SUB, LANES), F32)

    def sums_scratch(channels):
        return [
            pltpu.VMEM((channels * 2 * rows, LANES), F32),
            pltpu.VMEM((SPLITS * channels * sz.hi, wide), BF16),
            pltpu.VMEM((LANES, wide), BF16),
        ]

    def call(kernel, name, outs, args, scratch_shapes=()):
        return pl.pallas_call(
            kernel,
            name=name,
            out_shape=outs,
            in_specs=[vmem] * len(args),
            out_specs=[vmem] * len(outs),
            scratch_shapes=list(scratch_shapes),
            cost_estimate=pl.CostEstimate(flops=20_000_000, bytes_accessed=1_000_000, transcendentals=0),
            compiler_params=pltpu.CompilerParams(vmem_limit_bytes=48 * 1024 * 1024),
        )(*args)

    groups = [[core + 2 * i for i in range(half)] for core in range(2)]
    swap = [(i, i ^ 1) for i in range(n_blk)]

    def all_tiles(copies):
        same = lax.all_to_all(copies, "blk", 0, 0, axis_index_groups=groups)
        return same, lax.ppermute(same, "blk", swap)

    def other_half(value):
        if n_rep == 2:
            return lax.ppermute(value, "rep", [(0, 1), (1, 0)])
        return lax.psum(value, "rep") - value

    def all_products(scal):
        return lax.all_to_all(scal, ("blk", "rep"), 0, 0)

    table_shape = f32(CHANNELS * rows, LANES)
    est, est_copies = call(functools.partial(tile_kernel, sz), "tile", [f32(*tile), f32(half, *tile)], [start_angles])
    est_a, est_b = all_tiles(est_copies)
    steps = sz.pairs // 2
    table, anchor_rows, *sends = call(
        functools.partial(pack_kernel, sz),
        "pack",
        [table_shape, f32(sz.hi, LANES)] + [f32(2 * sz.edge_rows, LANES)] * (steps - 1) + [f32(sz.edge_rows, LANES)],
        [
            measured[:, 0], rot_vector[:, 0], confidence[:, 0], first_local[0], second_local[0], edge_counts[0],
            anchor.reshape(1, -1), est_b,
        ],
    )
    recvs = [
        lax.ppermute(sends[m - 1], "blk", [(i, (i + 2 * m) % n_blk) for i in range(n_blk)]) for m in range(1, steps)
    ]
    recvs.append(lax.ppermute(sends[-1], "blk", [(i, (i + sz.pairs) % n_blk) for i in range(1, n_blk, 2)]))

    per_edge = f32(3 * rows, LANES)
    sums_shape = f32(9 * sz.hi, LANES)
    for sweep in range(PASSES):
        last = sweep + 1 == PASSES
        if sweep == 0:
            gap_out, wc_out, sums = call(
                functools.partial(outgoing_misfit_kernel, sz),
                "misfit_outgoing",
                [per_edge, per_edge, sums_shape],
                [table, est_a, est_b, est],
                [far_shape] + sums_scratch(9),
            )
            (relay,) = call(
                functools.partial(relay_kernel, sz), "relay", [f32(steps * sz.edge_rows, LANES)], [table, *recvs]
            )
            relayed = lax.ppermute(relay, "blk", swap)
            table_in, gap_in, wc_in, sums = call(
                functools.partial(incoming_misfit_kernel, sz),
                "misfit_incoming",
                [table_shape, per_edge, per_edge, sums_shape],
                [table, relayed, *recvs[:-1], est_a, est_b, est, sums],
                [far_shape] + sums_scratch(6),
            )
        else:
            wc_out, wc_in, sums, weights, est = call(
                functools.partial(next_misfit_kernel, sz),
                "misfit_next",
                [per_edge, per_edge, sums_shape, f32(sz.pairs, sz.slots), f32(*tile)],
                [table, table_in, gap_out, gap_in, z_out, z_in, u_out, u_in, est, z, u, scal],
                sums_scratch(9),
            )
        residual, inverse, z, z_copies = call(
            functools.partial(precond_kernel, sz),
            "precond",
            [f32(*tile), f32(6 * sz.hi, LANES), f32(*tile), f32(half, *tile)],
            [sums, other_half(sums), est, anchor_rows],
        )
        z_a, z_b = all_tiles(z_copies)
        sums, *kept = call(
            functools.partial(image_kernel, sz, not last),
            "image",
            [f32(*tile)] + ([] if last else [per_edge, per_edge]),
            [table, table_in, wc_out, wc_in, z_a, z_b, z],
            [far_shape] + sums_scratch(3),
        )
        if not last:
            z_out, z_in = kept
        w, u, u_copies = call(
            functools.partial(second_precond_kernel, sz),
            "second_precond",
            [f32(*tile), f32(*tile), f32(half, *tile)],
            [sums, other_half(sums), z, anchor_rows, inverse],
        )
        u_a, u_b = all_tiles(u_copies)
        scal, *kept = call(
            functools.partial(products_kernel, sz, not last),
            "products",
            [f32(n_blk * n_rep, SUB, LANES)] + ([] if last else [per_edge, per_edge]),
            [table] + ([] if last else [table_in]) + [wc_out, u_a, u_b, residual, z, w, u, anchor_rows],
            [far_shape],
        )
        if not last:
            u_out, u_in = kept
        scal = all_products(scal)
    (estimate,) = call(functools.partial(final_kernel, sz), "final", [f32(3, sz.cams)], [est, z, u, scal])
    return (estimate, weights[None])


def solution(mesh):
    return jax.shard_map(
        on_device,
        mesh=mesh,
        in_specs=(
            P(None, "blk", None, "rep"),
            P(None, "blk", None, "rep"),
            P(None, "blk", None, "rep"),
            P("blk", None, "rep"),
            P("blk", None, "rep"),
            P("blk", None, "rep"),
            P(None, "blk"),
            P("blk"),
        ),
        out_specs=(P(None, "blk"), P("blk", None, "rep")),
        check_vma=False,
    )
```

```python
import functools

import jax
import jax.numpy as jnp
from jax import lax
from jax.experimental import pallas as pl
from jax.experimental.pallas import tpu as pltpu
from jax.sharding import PartitionSpec as P

PASSES = 2
SOFTEN = 0.05
LANES = 128
SUB = 8
SPLITS = 2
BLOCK_ENTRIES = ((0, 0), (1, 1), (2, 2), (0, 1), (0, 2), (1, 2))
MEAS, ROT, CONF, FIRST, SECOND = 0, 3, 6, 9, 10
CHANNELS = 11
F32 = jnp.float32
BF16 = jnp.bfloat16


def rotation_entries(v):
    squared = v[0] * v[0] + v[1] * v[1] + v[2] * v[2]
    factor = 2.0 / (1.0 + squared)
    skewed = ((None, -v[2], v[1]), (v[2], None, -v[0]), (-v[1], v[0], None))
    rows = []
    for a in range(3):
        row = []
        for b in range(3):
            if a == b:
                row.append(1.0 + factor * (v[a] * v[a] - squared))
            else:
                row.append(factor * (skewed[a][b] + v[a] * v[b]))
        rows.append(row)
    return rows


def rotate(rows, y):
    return [rows[a][0] * y[0] + rows[a][1] * y[1] + rows[a][2] * y[2] for a in range(3)]


def rotate_back(rows, y):
    return [rows[0][a] * y[0] + rows[1][a] * y[1] + rows[2][a] * y[2] for a in range(3)]


class Sizes:
    def __init__(self, n_blk, n_rep, pairs, slots, cams):
        self.n_blk, self.n_rep = n_blk, n_rep
        self.pairs, self.slots, self.cams = pairs, slots, cams
        self.hi = cams // LANES
        self.tile_rows = 3 * self.hi
        self.chunks = slots // LANES
        self.edge_rows = CHANNELS * self.chunks
        assert pairs == SUB and slots % LANES == 0 and cams % (LANES * SUB) == 0 and n_blk % 2 == 0


def block_at(sz, row, c):
    return pl.ds((row * sz.chunks + c) * SUB, SUB)


def chunk(sz, ref, row, c):
    return ref[block_at(sz, row, c), :]


def gather3(sz, source, index):
    hi = lax.shift_right_logical(index, 7)
    lo = lax.bitwise_and(index, LANES - 1)
    out = [None] * 3
    for r in range(sz.hi):
        mask = hi == r
        for c in range(3):
            got = jnp.take_along_axis(source(c, r), lo, axis=1, mode="promise_in_bounds")
            out[c] = got if r == 0 else jnp.where(mask, got, out[c])
    return out


def far_source(sz, far):
    return lambda c, r: far[pl.ds((c * sz.hi + r) * SUB, SUB), :]


def own_source(sz, own):
    return lambda c, r: jnp.broadcast_to(own[pl.ds(c * sz.hi + r, 1), :], (SUB, LANES))


def build_far(sz, far, tile_at, b, sign):
    for k in range(sz.pairs):
        t = lax.rem(b + (sign * k + sz.n_blk), sz.n_blk)
        far[pl.ds(k, sz.tile_rows, stride=SUB), :] = tile_at(k % 2, lax.div(t, 2))


def store_split(sz, vals, ch, c, value):
    high = value.astype(BF16).astype(F32)
    vals[block_at(sz, 2 * ch, c), :] = high
    vals[block_at(sz, 2 * ch + 1, c), :] = value - high


def scatter(sz, channels, vals, index_ref, index_row, lhs, rhs):
    lane_iota = lax.broadcasted_iota(jnp.int32, (LANES, LANES), 0).astype(F32).astype(BF16)
    row_iota = lax.broadcasted_iota(jnp.int32, (sz.hi, LANES), 0).astype(F32).astype(BF16)
    one, zero = jnp.ones((), BF16), jnp.zeros((), BF16)
    for c in range(sz.chunks):
        index = chunk(sz, index_ref, index_row, c).astype(jnp.int32)
        lows = lax.bitwise_and(index, LANES - 1).astype(F32)
        highs = lax.shift_right_logical(index, 7).astype(F32)
        for k in range(sz.pairs):
            columns = pl.ds((c * sz.pairs + k) * LANES, LANES)
            lo = jnp.broadcast_to(lows[k : k + 1], (sz.hi, LANES)).astype(BF16)
            hi = jnp.broadcast_to(highs[k : k + 1], (sz.hi, LANES)).astype(BF16)
            for n in range(LANES // sz.hi):
                at = pl.ds(n * sz.hi, sz.hi)
                rhs[at, columns] = jnp.where(lane_iota[n * sz.hi : (n + 1) * sz.hi] == lo, one, zero)
            mask = row_iota == hi
            for part in range(SPLITS):
                for ch in range(channels):
                    row = vals[pl.ds(((2 * ch + part) * sz.chunks + c) * SUB + k, 1), :]
                    block = jnp.where(mask, jnp.broadcast_to(row, (sz.hi, LANES)).astype(BF16), zero)
                    lhs[pl.ds((part * channels + ch) * sz.hi, sz.hi), columns] = block
    rows = SPLITS * channels * sz.hi
    out = lax.dot_general(
        lhs[pl.ds(0, rows), :], rhs[...], (((1,), (1,)), ((), ())), preferred_element_type=F32
    )
    half = channels * sz.hi
    return out[:half] + out[half:]


def opening_kernel(opened):
    opened[...] = jnp.zeros_like(opened)


def pack_kernel(sz, meas, rot, conf, first, second, counts, start, anchor, opened, table, est, est_copies, anchor_out, *sends):
    b = lax.axis_index("blk")
    across = lax.broadcasted_iota(jnp.int32, (sz.pairs, sz.pairs), 0)
    along = lax.broadcasted_iota(jnp.int32, (sz.pairs, sz.pairs), 1)
    spread = jnp.broadcast_to(counts[...], (sz.pairs, sz.pairs))
    limit = jnp.sum(jnp.where(across == along, spread, 0), axis=1, keepdims=True)
    for c in range(sz.chunks):
        lanes = pl.ds(c * LANES, LANES)
        slot = lax.broadcasted_iota(jnp.int32, (sz.pairs, LANES), 1) + c * LANES
        live = slot < limit
        for i in range(3):
            table[block_at(sz, MEAS + i, c), :] = meas[i, :, lanes]
            table[block_at(sz, ROT + i, c), :] = rot[i, :, lanes]
            table[block_at(sz, CONF + i, c), :] = jnp.where(live, conf[i, :, lanes], 0.0)
        table[block_at(sz, FIRST, c), :] = first[:, lanes].astype(F32)
        table[block_at(sz, SECOND, c), :] = second[:, lanes].astype(F32)
    for c in range(3):
        for r in range(sz.hi):
            est[pl.ds(c * sz.hi + r, 1), :] = start[pl.ds(c, 1), pl.ds(r * LANES, LANES)]
    for i in range(sz.n_blk // 2):
        est_copies[i] = est[...]
    for r in range(sz.hi):
        anchor_out[pl.ds(r, 1), :] = anchor[:, pl.ds(r * LANES, LANES)]
    step = 1 - 2 * lax.rem(b, 2)
    count = sz.edge_rows
    for m in range(1, sz.pairs // 2):
        sends[m - 1][pl.ds(0, count), :] = table[pl.ds(2 * m, count, stride=SUB), :]
        sends[m - 1][pl.ds(count, count), :] = table[pl.ds(2 * m + step, count, stride=SUB), :]
    sends[-1][...] = table[pl.ds(sz.pairs - 1, count, stride=SUB), :]


def relay_kernel(sz, table, *refs):
    recvs, relay = refs[:-1], refs[-1]
    even_core = lax.rem(lax.axis_index("blk"), 2) == 0
    count = sz.edge_rows
    steps = sz.pairs // 2
    for j in range(steps):
        if j == 0:
            from_even = table[pl.ds(1, count, stride=SUB), :]
        else:
            from_even = recvs[j - 1][pl.ds(count, count), :]
        if j + 1 < steps:
            from_odd = recvs[j][pl.ds(count, count), :]
        else:
            from_odd = recvs[-1][...]
        relay[pl.ds(j * count, count), :] = jnp.where(even_core, from_even, from_odd)


def step_factors(scal, n):
    total = scal[0]
    for i in range(1, n):
        total = total + scal[i]
    s = [jnp.sum(total[i : i + 1, :], axis=1, keepdims=True) for i in range(4)]
    alpha0 = s[0] / s[1]
    rz1 = alpha0 * alpha0 * s[2] - s[0]
    onward = 1.0 + rz1 / s[0]
    curve = onward * onward * s[1] - 2.0 * onward * alpha0 * s[2] + alpha0 * alpha0 * s[3]
    alpha1 = rz1 / curve
    return alpha0 + alpha1 * onward, -alpha1 * alpha0


def gathered_change(sz, edges, far, own, incoming, c, rows):
    first = chunk(sz, edges, FIRST, c).astype(jnp.int32)
    second = chunk(sz, edges, SECOND, c).astype(jnp.int32)
    if incoming:
        at_first = gather3(sz, far_source(sz, far), first)
        at_second = gather3(sz, own_source(sz, own), second)
    else:
        at_first = gather3(sz, own_source(sz, own), first)
        at_second = gather3(sz, far_source(sz, far), second)
    turned = rotate(rows, at_first)
    return [at_second[i] - turned[i] for i in range(3)]


def edge_rotation(sz, edges, c):
    return rotation_entries([chunk(sz, edges, ROT + i, c) for i in range(3)])


def put3(sz, ref, c, values):
    for i in range(3):
        ref[block_at(sz, i, c), :] = values[i]


def get3(sz, ref, c):
    return [chunk(sz, ref, i, c) for i in range(3)]


def misfit_sums(sz, incoming, misfit_of, edges, wc_ref, weights_ref, sums, vals, lhs, rhs):
    for c in range(sz.chunks):
        rows = None
        if not incoming:
            rows = edge_rotation(sz, edges, c)
        misfit = misfit_of(c, rows)
        conf = [chunk(sz, edges, CONF + i, c) for i in range(3)]
        energy = conf[0] * misfit[0] * misfit[0] + conf[1] * misfit[1] * misfit[1] + conf[2] * misfit[2] * misfit[2]
        weight = 1.0 / jnp.sqrt(energy + SOFTEN * SOFTEN)
        if weights_ref is not None:
            weights_ref[:, pl.ds(c * LANES, LANES)] = jnp.where(conf[0] > 0.0, weight, 0.0)
        wc = [weight * conf[i] for i in range(3)]
        put3(sz, wc_ref, c, wc)
        push = [wc[i] * misfit[i] for i in range(3)]
        if incoming:
            for i in range(3):
                store_split(sz, vals, i, c, push[i])
                store_split(sz, vals, 3 + i, c, wc[i])
        else:
            back = rotate_back(rows, push)
            for i in range(3):
                store_split(sz, vals, i, c, -back[i])
            for n, (p, q) in enumerate(BLOCK_ENTRIES):
                entry = sum(rows[i][p] * wc[i] * rows[i][q] for i in range(3))
                store_split(sz, vals, 3 + n, c, entry)
    part = scatter(sz, 6 if incoming else 9, vals, edges, SECOND if incoming else FIRST, lhs, rhs)
    if incoming:
        cut = 6 * sz.hi
        sums[pl.ds(0, cut), :] = sums[pl.ds(0, cut), :] + part
    else:
        sums[...] = part


def first_misfit(sz, incoming, edges, tile_at, own, gap, wc_ref, sums, far, vals, lhs, rhs):
    build_far(sz, far, tile_at, lax.axis_index("blk"), -1 if incoming else 1)

    def misfit_of(c, rows):
        rows = edge_rotation(sz, edges, c) if rows is None else rows
        change = gathered_change(sz, edges, far, own, incoming, c, rows)
        misfit = [chunk(sz, edges, MEAS + i, c) - change[i] for i in range(3)]
        put3(sz, gap, c, misfit)
        return misfit

    misfit_sums(sz, incoming, misfit_of, edges, wc_ref, None, sums, vals, lhs, rhs)


def outgoing_misfit_kernel(sz, table, est_a, est_b, own, gap, wc, sums, *scratch):
    tile_at = lambda parity, q: (est_b if parity else est_a)[q]
    first_misfit(sz, False, table, tile_at, own, gap, wc, sums, *scratch)


def incoming_misfit_kernel(sz, table, relayed, *refs):
    steps = sz.pairs // 2
    recvs, (est_a, est_b, own, sums_out, table_in, gap, wc, sums), scratch = refs[: steps - 1], refs[steps - 1 : -4], refs[-4:]
    count = sz.edge_rows
    for k in range(sz.pairs):
        if k == 0:
            block = table[pl.ds(0, count, stride=SUB), :]
        elif k % 2:
            block = relayed[pl.ds((k // 2) * count, count), :]
        else:
            block = recvs[k // 2 - 1][pl.ds(0, count), :]
        table_in[pl.ds(k, count, stride=SUB), :] = block
    sums[...] = sums_out[...]
    tile_at = lambda parity, q: (est_b if parity else est_a)[q]
    first_misfit(sz, True, table_in, tile_at, own, gap, wc, sums, *scratch)


def next_misfit_kernel(
    sz, table, table_in, gap_out, gap_in, z_out, z_in, u_out, u_in, own, z, u, scal,
    wc_out, wc_in, sums, weights, own_new, vals, lhs, rhs,
):
    along_z, along_u = step_factors(scal, sz.n_blk * sz.n_rep)
    own_new[...] = own[...] + along_z * z[...] + along_u * u[...]
    for incoming in (False, True):
        edges, wc_ref = (table_in, wc_in) if incoming else (table, wc_out)
        old, by_z, by_u = (gap_in, z_in, u_in) if incoming else (gap_out, z_out, u_out)

        def misfit_of(c, rows):
            old3, z3, u3 = get3(sz, old, c), get3(sz, by_z, c), get3(sz, by_u, c)
            return [old3[i] - (along_z * z3[i] + along_u * u3[i]) for i in range(3)]

        misfit_sums(sz, incoming, misfit_of, edges, wc_ref, None if incoming else weights, sums, vals, lhs, rhs)


def apply_inverse(sz, inv, v):
    a00, a11, a22, a01, a02, a12 = inv
    return [
        a00 * v[0] + a01 * v[1] + a02 * v[2],
        a01 * v[0] + a11 * v[1] + a12 * v[2],
        a02 * v[0] + a12 * v[1] + a22 * v[2],
    ]


def comp(sz, ref, i):
    return ref[pl.ds(i * sz.hi, sz.hi), :]


def precond_kernel(sz, mine, other, est, anchor, residual, inverse, z, z_copies):
    total = mine[...] + other[...]
    part = lambda i: total[i * sz.hi : (i + 1) * sz.hi]
    anc = anchor[...]
    res = [part(i) - anc * comp(sz, est, i) for i in range(3)]
    p00, p11, p22 = [part(3 + i) + anc for i in range(3)]
    p01, p02, p12 = [part(6 + i) for i in range(3)]
    adj00 = p11 * p22 - p12 * p12
    adj01 = p02 * p12 - p01 * p22
    adj02 = p01 * p12 - p02 * p11
    adj11 = p00 * p22 - p02 * p02
    adj12 = p01 * p02 - p00 * p12
    adj22 = p00 * p11 - p01 * p01
    det = p00 * adj00 + p01 * adj01 + p02 * adj02
    inv = [a / det for a in (adj00, adj11, adj22, adj01, adj02, adj12)]
    scaled = apply_inverse(sz, inv, res)
    for i in range(3):
        residual[pl.ds(i * sz.hi, sz.hi), :] = res[i]
        z[pl.ds(i * sz.hi, sz.hi), :] = scaled[i]
    for i in range(6):
        inverse[pl.ds(i * sz.hi, sz.hi), :] = inv[i]
    for i in range(sz.n_blk // 2):
        z_copies[i] = z[...]


def image_kernel(sz, keep, table, table_in, wc_out, wc_in, z_a, z_b, z, sums, *refs):
    kept, (far, vals, lhs, rhs) = refs[:-4], refs[-4:]
    b = lax.axis_index("blk")

    def tile_at(parity, q):
        return (z_b if parity else z_a)[q]

    for incoming in (False, True):
        edges, wc_ref = (table_in, wc_in) if incoming else (table, wc_out)
        build_far(sz, far, tile_at, b, -1 if incoming else 1)
        for c in range(sz.chunks):
            rows = edge_rotation(sz, edges, c)
            change = gathered_change(sz, edges, far, z, incoming, c, rows)
            if keep:
                put3(sz, kept[int(incoming)], c, change)
            wc = get3(sz, wc_ref, c)
            push = [wc[i] * change[i] for i in range(3)]
            if incoming:
                for i in range(3):
                    store_split(sz, vals, i, c, push[i])
            else:
                back = rotate_back(rows, push)
                for i in range(3):
                    store_split(sz, vals, i, c, -back[i])
        part = scatter(sz, 3, vals, edges, SECOND if incoming else FIRST, lhs, rhs)
        if incoming:
            sums[...] = sums[...] + part
        else:
            sums[...] = part


def second_precond_kernel(sz, mine, other, z, anchor, inverse, w, u, u_copies):
    total = mine[...] + other[...]
    anc = anchor[...]
    image = [total[i * sz.hi : (i + 1) * sz.hi] + anc * comp(sz, z, i) for i in range(3)]
    scaled = apply_inverse(sz, [comp(sz, inverse, i) for i in range(6)], image)
    for i in range(3):
        w[pl.ds(i * sz.hi, sz.hi), :] = image[i]
        u[pl.ds(i * sz.hi, sz.hi), :] = scaled[i]
    for i in range(sz.n_blk // 2):
        u_copies[i] = u[...]


def fold(value):
    rows = value.shape[0]
    out = value[:SUB]
    for i in range(1, rows // SUB):
        out = out + value[i * SUB : (i + 1) * SUB]
    return out


def products_kernel(sz, keep, table, *refs):
    refs = list(refs)
    table_in = refs.pop(0) if keep else None
    wc_out, u_a, u_b, residual, z, w, u, anchor, scal = refs[:9]
    kept, far = refs[9:-1], refs[-1]
    b = lax.axis_index("blk")

    def tile_at(parity, q):
        return (u_b if parity else u_a)[q]

    acc = jnp.zeros((SUB, LANES), F32)
    for incoming in (False, True) if keep else (False,):
        edges = table_in if incoming else table
        build_far(sz, far, tile_at, b, -1 if incoming else 1)
        for c in range(sz.chunks):
            change = gathered_change(sz, edges, far, u, incoming, c, edge_rotation(sz, edges, c))
            if keep:
                put3(sz, kept[int(incoming)], c, change)
            if not incoming:
                wc = get3(sz, wc_out, c)
                for i in range(3):
                    acc = acc + wc[i] * change[i] * change[i]
    share = 1.0 / sz.n_rep
    res, zz, ww, uu = residual[...], z[...], w[...], u[...]
    s1 = fold(res * zz) * share
    s2 = fold(zz * ww) * share
    s3 = fold(ww * uu) * share
    anc = anchor[...]
    s4 = acc + share * fold(anc * (comp(sz, u, 0) * comp(sz, u, 0) + comp(sz, u, 1) * comp(sz, u, 1) + comp(sz, u, 2) * comp(sz, u, 2)))
    block = [jnp.sum(s, axis=0, keepdims=True) for s in (s1, s2, s3, s4)]
    block = jnp.concatenate(block + [jnp.zeros((SUB - 4, LANES), F32)], axis=0)
    for i in range(sz.n_blk * sz.n_rep):
        scal[i] = block


def final_kernel(sz, est, z, u, scal, out):
    along_z, along_u = step_factors(scal, sz.n_blk * sz.n_rep)
    new = est[...] + along_z * z[...] + along_u * u[...]
    for c in range(3):
        for r in range(sz.hi):
            row = c * sz.hi + r
            out[pl.ds(c, 1), pl.ds(r * LANES, LANES)] = new[row : row + 1]


def on_device(measured, rot_vector, confidence, first_local, second_local, edge_counts, start_angles, anchor):
    n_blk, n_rep = lax.axis_size("blk"), lax.axis_size("rep")
    sz = Sizes(n_blk, n_rep, first_local.shape[1], first_local.shape[2], start_angles.shape[1])
    half = n_blk // 2
    tile = (sz.tile_rows, LANES)
    f32 = lambda *shape: jax.ShapeDtypeStruct(shape, F32)
    vmem = pl.BlockSpec(memory_space=pltpu.VMEM)
    wide = sz.pairs * sz.slots
    rows = sz.chunks * SUB
    far_shape = pltpu.VMEM((sz.tile_rows * SUB, LANES), F32)

    def sums_scratch(channels):
        return [
            pltpu.VMEM((channels * 2 * rows, LANES), F32),
            pltpu.VMEM((SPLITS * channels * sz.hi, wide), BF16),
            pltpu.VMEM((LANES, wide), BF16),
        ]

    def call(kernel, name, outs, args, scratch_shapes=(), flops=20_000_000):
        return pl.pallas_call(
            kernel,
            name=name,
            out_shape=outs,
            in_specs=[vmem] * len(args),
            out_specs=[vmem] * len(outs),
            scratch_shapes=list(scratch_shapes),
            cost_estimate=pl.CostEstimate(flops=flops, bytes_accessed=flops // 10, transcendentals=0),
            compiler_params=pltpu.CompilerParams(vmem_limit_bytes=48 * 1024 * 1024),
        )(*args)

    groups = [[core + 2 * i for i in range(half)] for core in range(2)]
    swap = [(i, i ^ 1) for i in range(n_blk)]

    def all_tiles(copies):
        same = lax.all_to_all(copies, "blk", 0, 0, axis_index_groups=groups)
        return same, lax.ppermute(same, "blk", swap)

    def other_half(value):
        if n_rep == 2:
            return lax.ppermute(value, "rep", [(0, 1), (1, 0)])
        return lax.psum(value, "rep") - value

    def all_products(scal):
        return lax.all_to_all(scal, ("blk", "rep"), 0, 0)

    table_shape = f32(CHANNELS * rows, LANES)
    steps = sz.pairs // 2
    (opened,) = call(opening_kernel, "opening", [f32(SUB, LANES)], [], flops=20_000_000_000)
    table, est, est_copies, anchor_rows, *sends = call(
        functools.partial(pack_kernel, sz),
        "pack",
        [table_shape, f32(*tile), f32(half, *tile), f32(sz.hi, LANES)]
        + [f32(2 * sz.edge_rows, LANES)] * (steps - 1)
        + [f32(sz.edge_rows, LANES)],
        [
            measured[:, 0], rot_vector[:, 0], confidence[:, 0], first_local[0], second_local[0], edge_counts.reshape(1, -1),
            start_angles, anchor.reshape(1, -1), opened,
        ],
    )
    recvs = [
        lax.ppermute(sends[m - 1], "blk", [(i, (i + 2 * m) % n_blk) for i in range(n_blk)]) for m in range(1, steps)
    ]
    recvs.append(lax.ppermute(sends[-1], "blk", [(i, (i + sz.pairs) % n_blk) for i in range(1, n_blk, 2)]))
    est_a, est_b = all_tiles(est_copies)

    per_edge = f32(3 * rows, LANES)
    sums_shape = f32(9 * sz.hi, LANES)
    for sweep in range(PASSES):
        last = sweep + 1 == PASSES
        if sweep == 0:
            gap_out, wc_out, sums = call(
                functools.partial(outgoing_misfit_kernel, sz),
                "misfit_outgoing",
                [per_edge, per_edge, sums_shape],
                [table, est_a, est_b, est],
                [far_shape] + sums_scratch(9),
            )
            (relay,) = call(
                functools.partial(relay_kernel, sz), "relay", [f32(steps * sz.edge_rows, LANES)], [table, *recvs]
            )
            relayed = lax.ppermute(relay, "blk", swap)
            table_in, gap_in, wc_in, sums = call(
                functools.partial(incoming_misfit_kernel, sz),
                "misfit_incoming",
                [table_shape, per_edge, per_edge, sums_shape],
                [table, relayed, *recvs[:-1], est_a, est_b, est, sums],
                [far_shape] + sums_scratch(6),
            )
        else:
            wc_out, wc_in, sums, weights, est = call(
                functools.partial(next_misfit_kernel, sz),
                "misfit_next",
                [per_edge, per_edge, sums_shape, f32(sz.pairs, sz.slots), f32(*tile)],
                [table, table_in, gap_out, gap_in, z_out, z_in, u_out, u_in, est, z, u, scal],
                sums_scratch(9),
            )
        residual, inverse, z, z_copies = call(
            functools.partial(precond_kernel, sz),
            "precond",
            [f32(*tile), f32(6 * sz.hi, LANES), f32(*tile), f32(half, *tile)],
            [sums, other_half(sums), est, anchor_rows],
        )
        z_a, z_b = all_tiles(z_copies)
        sums, *kept = call(
            functools.partial(image_kernel, sz, not last),
            "image",
            [f32(*tile)] + ([] if last else [per_edge, per_edge]),
            [table, table_in, wc_out, wc_in, z_a, z_b, z],
            [far_shape] + sums_scratch(3),
        )
        if not last:
            z_out, z_in = kept
        w, u, u_copies = call(
            functools.partial(second_precond_kernel, sz),
            "second_precond",
            [f32(*tile), f32(*tile), f32(half, *tile)],
            [sums, other_half(sums), z, anchor_rows, inverse],
        )
        u_a, u_b = all_tiles(u_copies)
        scal, *kept = call(
            functools.partial(products_kernel, sz, not last),
            "products",
            [f32(n_blk * n_rep, SUB, LANES)] + ([] if last else [per_edge, per_edge]),
            [table] + ([] if last else [table_in]) + [wc_out, u_a, u_b, residual, z, w, u, anchor_rows],
            [far_shape],
        )
        if not last:
            u_out, u_in = kept
        scal = all_products(scal)
    (estimate,) = call(functools.partial(final_kernel, sz), "final", [f32(3, sz.cams)], [est, z, u, scal])
    return (estimate, weights[None])


def solution(mesh):
    return jax.shard_map(
        on_device,
        mesh=mesh,
        in_specs=(
            P(None, "blk", None, "rep"),
            P(None, "blk", None, "rep"),
            P(None, "blk", None, "rep"),
            P("blk", None, "rep"),
            P("blk", None, "rep"),
            P("blk", None, "rep"),
            P(None, "blk"),
            P("blk"),
        ),
        out_specs=(P(None, "blk"), P("blk", None, "rep")),
        check_vma=False,
    )
```

```python
import functools

import jax
import jax.numpy as jnp
from jax import lax
from jax.experimental import pallas as pl
from jax.experimental.pallas import tpu as pltpu
from jax.sharding import PartitionSpec as P

PASSES = 2
SOFTEN = 0.05
LANES = 128
SUB = 8
SPLITS = 2
BLOCK_ENTRIES = ((0, 0), (1, 1), (2, 2), (0, 1), (0, 2), (1, 2))
MEAS, ROT, CONF, FIRST, SECOND = 0, 3, 6, 9, 10
CHANNELS = 11
F32 = jnp.float32
BF16 = jnp.bfloat16


def rotation_entries(v):
    squared = v[0] * v[0] + v[1] * v[1] + v[2] * v[2]
    factor = 2.0 / (1.0 + squared)
    skewed = ((None, -v[2], v[1]), (v[2], None, -v[0]), (-v[1], v[0], None))
    rows = []
    for a in range(3):
        row = []
        for b in range(3):
            if a == b:
                row.append(1.0 + factor * (v[a] * v[a] - squared))
            else:
                row.append(factor * (skewed[a][b] + v[a] * v[b]))
        rows.append(row)
    return rows


def rotate(rows, y):
    return [rows[a][0] * y[0] + rows[a][1] * y[1] + rows[a][2] * y[2] for a in range(3)]


def rotate_back(rows, y):
    return [rows[0][a] * y[0] + rows[1][a] * y[1] + rows[2][a] * y[2] for a in range(3)]


class Sizes:
    def __init__(self, n_blk, n_rep, pairs, slots, cams):
        self.n_blk, self.n_rep = n_blk, n_rep
        self.pairs, self.slots, self.cams = pairs, slots, cams
        self.hi = cams // LANES
        self.tile_rows = 3 * self.hi
        self.chunks = slots // LANES
        self.edge_rows = CHANNELS * self.chunks
        assert pairs == SUB and slots % LANES == 0 and cams % (LANES * SUB) == 0 and n_blk % 2 == 0


def block_at(sz, row, c):
    return pl.ds((row * sz.chunks + c) * SUB, SUB)


def chunk(sz, ref, row, c):
    return ref[block_at(sz, row, c), :]


def gather3(sz, source, index):
    hi = lax.shift_right_logical(index, 7)
    lo = lax.bitwise_and(index, LANES - 1)
    out = [None] * 3
    for r in range(sz.hi):
        mask = hi == r
        for c in range(3):
            got = jnp.take_along_axis(source(c, r), lo, axis=1, mode="promise_in_bounds")
            out[c] = got if r == 0 else jnp.where(mask, got, out[c])
    return out


def far_source(sz, far):
    return lambda c, r: far[pl.ds((c * sz.hi + r) * SUB, SUB), :]


def own_source(sz, own):
    return lambda c, r: jnp.broadcast_to(own[pl.ds(c * sz.hi + r, 1), :], (SUB, LANES))


def build_far(sz, far, tile_at, b, sign):
    for k in range(sz.pairs):
        t = lax.rem(b + (sign * k + sz.n_blk), sz.n_blk)
        far[pl.ds(k, sz.tile_rows, stride=SUB), :] = tile_at(k % 2, lax.div(t, 2))


def store_split(sz, vals, ch, c, value):
    high = value.astype(BF16).astype(F32)
    vals[block_at(sz, 2 * ch, c), :] = high
    vals[block_at(sz, 2 * ch + 1, c), :] = value - high


def scatter(sz, channels, vals, index_ref, index_row):
    lane_iota = lax.broadcasted_iota(jnp.int32, (LANES, LANES), 0).astype(F32).astype(BF16)
    row_iota = lax.broadcasted_iota(jnp.int32, (sz.hi, LANES), 0).astype(F32).astype(BF16)
    one, zero = jnp.ones((), BF16), jnp.zeros((), BF16)
    total = None
    for c in range(sz.chunks):
        index = chunk(sz, index_ref, index_row, c).astype(jnp.int32)
        lows = lax.bitwise_and(index, LANES - 1).astype(F32)
        highs = lax.shift_right_logical(index, 7).astype(F32)
        for pair in range(0, sz.pairs, 2):
            lefts, rights = [], []
            for k in (pair, pair + 1):
                lo = jnp.broadcast_to(lows[k : k + 1], (LANES, LANES)).astype(BF16)
                hi = jnp.broadcast_to(highs[k : k + 1], (sz.hi, LANES)).astype(BF16)
                rights.append(jnp.where(lane_iota == lo, one, zero))
                mask = row_iota == hi
                blocks = []
                for part in range(SPLITS):
                    for ch in range(channels):
                        row = vals[pl.ds(((2 * ch + part) * sz.chunks + c) * SUB + k, 1), :]
                        blocks.append(jnp.where(mask, jnp.broadcast_to(row, (sz.hi, LANES)).astype(BF16), zero))
                lefts.append(jnp.concatenate(blocks, axis=0))
            product = lax.dot_general(
                jnp.concatenate(lefts, axis=1),
                jnp.concatenate(rights, axis=1),
                (((1,), (1,)), ((), ())),
                preferred_element_type=F32,
            )
            total = product if total is None else total + product
    half = channels * sz.hi
    return total[:half] + total[half:]


def opening_kernel(opened):
    opened[...] = jnp.zeros_like(opened)


def pack_kernel(sz, meas, rot, conf, first, second, counts, start, anchor, opened, table, est, est_copies, anchor_out, *sends):
    b = lax.axis_index("blk")
    across = lax.broadcasted_iota(jnp.int32, (sz.pairs, sz.pairs), 0)
    along = lax.broadcasted_iota(jnp.int32, (sz.pairs, sz.pairs), 1)
    spread = jnp.broadcast_to(counts[...], (sz.pairs, sz.pairs))
    limit = jnp.sum(jnp.where(across == along, spread, 0), axis=1, keepdims=True)
    for c in range(sz.chunks):
        lanes = pl.ds(c * LANES, LANES)
        slot = lax.broadcasted_iota(jnp.int32, (sz.pairs, LANES), 1) + c * LANES
        live = slot < limit
        for i in range(3):
            table[block_at(sz, MEAS + i, c), :] = meas[i, :, lanes]
            table[block_at(sz, ROT + i, c), :] = rot[i, :, lanes]
            table[block_at(sz, CONF + i, c), :] = jnp.where(live, conf[i, :, lanes], 0.0)
        table[block_at(sz, FIRST, c), :] = first[:, lanes].astype(F32)
        table[block_at(sz, SECOND, c), :] = second[:, lanes].astype(F32)
    for c in range(3):
        for r in range(sz.hi):
            est[pl.ds(c * sz.hi + r, 1), :] = start[pl.ds(c, 1), pl.ds(r * LANES, LANES)]
    for i in range(sz.n_blk // 2):
        est_copies[i] = est[...]
    for r in range(sz.hi):
        anchor_out[pl.ds(r, 1), :] = anchor[:, pl.ds(r * LANES, LANES)]
    step = 1 - 2 * lax.rem(b, 2)
    count = sz.edge_rows
    for m in range(1, sz.pairs // 2):
        sends[m - 1][pl.ds(0, count), :] = table[pl.ds(2 * m, count, stride=SUB), :]
        sends[m - 1][pl.ds(count, count), :] = table[pl.ds(2 * m + step, count, stride=SUB), :]
    sends[-1][...] = table[pl.ds(sz.pairs - 1, count, stride=SUB), :]


def relay_kernel(sz, table, *refs):
    recvs, relay = refs[:-1], refs[-1]
    even_core = lax.rem(lax.axis_index("blk"), 2) == 0
    count = sz.edge_rows
    steps = sz.pairs // 2
    for j in range(steps):
        if j == 0:
            from_even = table[pl.ds(1, count, stride=SUB), :]
        else:
            from_even = recvs[j - 1][pl.ds(count, count), :]
        if j + 1 < steps:
            from_odd = recvs[j][pl.ds(count, count), :]
        else:
            from_odd = recvs[-1][...]
        relay[pl.ds(j * count, count), :] = jnp.where(even_core, from_even, from_odd)


def step_factors(scal, n):
    total = scal[0]
    for i in range(1, n):
        total = total + scal[i]
    s = [jnp.sum(total[i : i + 1, :], axis=1, keepdims=True) for i in range(4)]
    alpha0 = s[0] / s[1]
    rz1 = alpha0 * alpha0 * s[2] - s[0]
    onward = 1.0 + rz1 / s[0]
    curve = onward * onward * s[1] - 2.0 * onward * alpha0 * s[2] + alpha0 * alpha0 * s[3]
    alpha1 = rz1 / curve
    return alpha0 + alpha1 * onward, -alpha1 * alpha0


def gathered_change(sz, edges, far, own, incoming, c, rows):
    first = chunk(sz, edges, FIRST, c).astype(jnp.int32)
    second = chunk(sz, edges, SECOND, c).astype(jnp.int32)
    if incoming:
        at_first = gather3(sz, far_source(sz, far), first)
        at_second = gather3(sz, own_source(sz, own), second)
    else:
        at_first = gather3(sz, own_source(sz, own), first)
        at_second = gather3(sz, far_source(sz, far), second)
    turned = rotate(rows, at_first)
    return [at_second[i] - turned[i] for i in range(3)]


def edge_rotation(sz, edges, c):
    return rotation_entries([chunk(sz, edges, ROT + i, c) for i in range(3)])


def put3(sz, ref, c, values):
    for i in range(3):
        ref[block_at(sz, i, c), :] = values[i]


def get3(sz, ref, c):
    return [chunk(sz, ref, i, c) for i in range(3)]


def misfit_sums(sz, incoming, misfit_of, edges, wc_ref, weights_ref, sums, vals):
    for c in range(sz.chunks):
        rows = None
        if not incoming:
            rows = edge_rotation(sz, edges, c)
        misfit = misfit_of(c, rows)
        conf = [chunk(sz, edges, CONF + i, c) for i in range(3)]
        energy = conf[0] * misfit[0] * misfit[0] + conf[1] * misfit[1] * misfit[1] + conf[2] * misfit[2] * misfit[2]
        weight = 1.0 / jnp.sqrt(energy + SOFTEN * SOFTEN)
        if weights_ref is not None:
            weights_ref[:, pl.ds(c * LANES, LANES)] = jnp.where(conf[0] > 0.0, weight, 0.0)
        wc = [weight * conf[i] for i in range(3)]
        put3(sz, wc_ref, c, wc)
        push = [wc[i] * misfit[i] for i in range(3)]
        if incoming:
            for i in range(3):
                store_split(sz, vals, i, c, push[i])
                store_split(sz, vals, 3 + i, c, wc[i])
        else:
            back = rotate_back(rows, push)
            for i in range(3):
                store_split(sz, vals, i, c, -back[i])
            for n, (p, q) in enumerate(BLOCK_ENTRIES):
                entry = sum(rows[i][p] * wc[i] * rows[i][q] for i in range(3))
                store_split(sz, vals, 3 + n, c, entry)
    part = scatter(sz, 6 if incoming else 9, vals, edges, SECOND if incoming else FIRST)
    if incoming:
        cut = 6 * sz.hi
        sums[pl.ds(0, cut), :] = sums[pl.ds(0, cut), :] + part
    else:
        sums[...] = part


def first_misfit(sz, incoming, edges, tile_at, own, gap, wc_ref, sums, far, vals):
    build_far(sz, far, tile_at, lax.axis_index("blk"), -1 if incoming else 1)

    def misfit_of(c, rows):
        rows = edge_rotation(sz, edges, c) if rows is None else rows
        change = gathered_change(sz, edges, far, own, incoming, c, rows)
        misfit = [chunk(sz, edges, MEAS + i, c) - change[i] for i in range(3)]
        put3(sz, gap, c, misfit)
        return misfit

    misfit_sums(sz, incoming, misfit_of, edges, wc_ref, None, sums, vals)


def outgoing_misfit_kernel(sz, table, est_a, est_b, own, gap, wc, sums, *scratch):
    tile_at = lambda parity, q: (est_b if parity else est_a)[q]
    first_misfit(sz, False, table, tile_at, own, gap, wc, sums, *scratch)


def incoming_misfit_kernel(sz, table, relayed, *refs):
    steps = sz.pairs // 2
    recvs, (est_a, est_b, own, sums_out, table_in, gap, wc, sums), scratch = refs[: steps - 1], refs[steps - 1 : -2], refs[-2:]
    count = sz.edge_rows
    for k in range(sz.pairs):
        if k == 0:
            block = table[pl.ds(0, count, stride=SUB), :]
        elif k % 2:
            block = relayed[pl.ds((k // 2) * count, count), :]
        else:
            block = recvs[k // 2 - 1][pl.ds(0, count), :]
        table_in[pl.ds(k, count, stride=SUB), :] = block
    sums[...] = sums_out[...]
    tile_at = lambda parity, q: (est_b if parity else est_a)[q]
    first_misfit(sz, True, table_in, tile_at, own, gap, wc, sums, *scratch)


def next_misfit_kernel(
    sz, table, table_in, gap_out, gap_in, z_out, z_in, u_out, u_in, own, z, u, scal,
    wc_out, wc_in, sums, weights, own_new, vals,
):
    along_z, along_u = step_factors(scal, sz.n_blk * sz.n_rep)
    own_new[...] = own[...] + along_z * z[...] + along_u * u[...]
    for incoming in (False, True):
        edges, wc_ref = (table_in, wc_in) if incoming else (table, wc_out)
        old, by_z, by_u = (gap_in, z_in, u_in) if incoming else (gap_out, z_out, u_out)

        def misfit_of(c, rows):
            old3, z3, u3 = get3(sz, old, c), get3(sz, by_z, c), get3(sz, by_u, c)
            return [old3[i] - (along_z * z3[i] + along_u * u3[i]) for i in range(3)]

        misfit_sums(sz, incoming, misfit_of, edges, wc_ref, None if incoming else weights, sums, vals)


def apply_inverse(sz, inv, v):
    a00, a11, a22, a01, a02, a12 = inv
    return [
        a00 * v[0] + a01 * v[1] + a02 * v[2],
        a01 * v[0] + a11 * v[1] + a12 * v[2],
        a02 * v[0] + a12 * v[1] + a22 * v[2],
    ]


def comp(sz, ref, i):
    return ref[pl.ds(i * sz.hi, sz.hi), :]


def precond_kernel(sz, mine, other, est, anchor, residual, inverse, z, z_copies):
    total = mine[...] + other[...]
    part = lambda i: total[i * sz.hi : (i + 1) * sz.hi]
    anc = anchor[...]
    res = [part(i) - anc * comp(sz, est, i) for i in range(3)]
    p00, p11, p22 = [part(3 + i) + anc for i in range(3)]
    p01, p02, p12 = [part(6 + i) for i in range(3)]
    adj00 = p11 * p22 - p12 * p12
    adj01 = p02 * p12 - p01 * p22
    adj02 = p01 * p12 - p02 * p11
    adj11 = p00 * p22 - p02 * p02
    adj12 = p01 * p02 - p00 * p12
    adj22 = p00 * p11 - p01 * p01
    det = p00 * adj00 + p01 * adj01 + p02 * adj02
    inv = [a / det for a in (adj00, adj11, adj22, adj01, adj02, adj12)]
    scaled = apply_inverse(sz, inv, res)
    for i in range(3):
        residual[pl.ds(i * sz.hi, sz.hi), :] = res[i]
        z[pl.ds(i * sz.hi, sz.hi), :] = scaled[i]
    for i in range(6):
        inverse[pl.ds(i * sz.hi, sz.hi), :] = inv[i]
    for i in range(sz.n_blk // 2):
        z_copies[i] = z[...]


def image_kernel(sz, keep, table, table_in, wc_out, wc_in, z_a, z_b, z, sums, *refs):
    kept, (far, vals) = refs[:-2], refs[-2:]
    b = lax.axis_index("blk")

    def tile_at(parity, q):
        return (z_b if parity else z_a)[q]

    for incoming in (False, True):
        edges, wc_ref = (table_in, wc_in) if incoming else (table, wc_out)
        build_far(sz, far, tile_at, b, -1 if incoming else 1)
        for c in range(sz.chunks):
            rows = edge_rotation(sz, edges, c)
            change = gathered_change(sz, edges, far, z, incoming, c, rows)
            if keep:
                put3(sz, kept[int(incoming)], c, change)
            wc = get3(sz, wc_ref, c)
            push = [wc[i] * change[i] for i in range(3)]
            if incoming:
                for i in range(3):
                    store_split(sz, vals, i, c, push[i])
            else:
                back = rotate_back(rows, push)
                for i in range(3):
                    store_split(sz, vals, i, c, -back[i])
        part = scatter(sz, 3, vals, edges, SECOND if incoming else FIRST)
        if incoming:
            sums[...] = sums[...] + part
        else:
            sums[...] = part


def second_precond_kernel(sz, mine, other, z, anchor, inverse, w, u, u_copies):
    total = mine[...] + other[...]
    anc = anchor[...]
    image = [total[i * sz.hi : (i + 1) * sz.hi] + anc * comp(sz, z, i) for i in range(3)]
    scaled = apply_inverse(sz, [comp(sz, inverse, i) for i in range(6)], image)
    for i in range(3):
        w[pl.ds(i * sz.hi, sz.hi), :] = image[i]
        u[pl.ds(i * sz.hi, sz.hi), :] = scaled[i]
    for i in range(sz.n_blk // 2):
        u_copies[i] = u[...]


def fold(value):
    rows = value.shape[0]
    out = value[:SUB]
    for i in range(1, rows // SUB):
        out = out + value[i * SUB : (i + 1) * SUB]
    return out


def products_kernel(sz, keep, table, *refs):
    refs = list(refs)
    table_in = refs.pop(0) if keep else None
    wc_out, u_a, u_b, residual, z, w, u, anchor, scal = refs[:9]
    kept, far = refs[9:-1], refs[-1]
    b = lax.axis_index("blk")

    def tile_at(parity, q):
        return (u_b if parity else u_a)[q]

    acc = jnp.zeros((SUB, LANES), F32)
    for incoming in (False, True) if keep else (False,):
        edges = table_in if incoming else table
        build_far(sz, far, tile_at, b, -1 if incoming else 1)
        for c in range(sz.chunks):
            change = gathered_change(sz, edges, far, u, incoming, c, edge_rotation(sz, edges, c))
            if keep:
                put3(sz, kept[int(incoming)], c, change)
            if not incoming:
                wc = get3(sz, wc_out, c)
                for i in range(3):
                    acc = acc + wc[i] * change[i] * change[i]
    share = 1.0 / sz.n_rep
    res, zz, ww, uu = residual[...], z[...], w[...], u[...]
    s1 = fold(res * zz) * share
    s2 = fold(zz * ww) * share
    s3 = fold(ww * uu) * share
    anc = anchor[...]
    s4 = acc + share * fold(anc * (comp(sz, u, 0) * comp(sz, u, 0) + comp(sz, u, 1) * comp(sz, u, 1) + comp(sz, u, 2) * comp(sz, u, 2)))
    block = [jnp.sum(s, axis=0, keepdims=True) for s in (s1, s2, s3, s4)]
    block = jnp.concatenate(block + [jnp.zeros((SUB - 4, LANES), F32)], axis=0)
    for i in range(sz.n_blk * sz.n_rep):
        scal[i] = block


def final_kernel(sz, est, z, u, scal, out):
    along_z, along_u = step_factors(scal, sz.n_blk * sz.n_rep)
    new = est[...] + along_z * z[...] + along_u * u[...]
    for c in range(3):
        for r in range(sz.hi):
            row = c * sz.hi + r
            out[pl.ds(c, 1), pl.ds(r * LANES, LANES)] = new[row : row + 1]


def on_device(measured, rot_vector, confidence, first_local, second_local, edge_counts, start_angles, anchor):
    n_blk, n_rep = lax.axis_size("blk"), lax.axis_size("rep")
    sz = Sizes(n_blk, n_rep, first_local.shape[1], first_local.shape[2], start_angles.shape[1])
    half = n_blk // 2
    tile = (sz.tile_rows, LANES)
    f32 = lambda *shape: jax.ShapeDtypeStruct(shape, F32)
    vmem = pl.BlockSpec(memory_space=pltpu.VMEM)
    rows = sz.chunks * SUB
    far_shape = pltpu.VMEM((sz.tile_rows * SUB, LANES), F32)

    def sums_scratch(channels):
        return [
            pltpu.VMEM((channels * 2 * rows, LANES), F32),
        ]

    def call(kernel, name, outs, args, scratch_shapes=(), flops=20_000_000):
        return pl.pallas_call(
            kernel,
            name=name,
            out_shape=outs,
            in_specs=[vmem] * len(args),
            out_specs=[vmem] * len(outs),
            scratch_shapes=list(scratch_shapes),
            cost_estimate=pl.CostEstimate(flops=flops, bytes_accessed=flops // 10, transcendentals=0),
            compiler_params=pltpu.CompilerParams(vmem_limit_bytes=48 * 1024 * 1024),
        )(*args)

    groups = [[core + 2 * i for i in range(half)] for core in range(2)]
    swap = [(i, i ^ 1) for i in range(n_blk)]

    def all_tiles(copies):
        same = lax.all_to_all(copies, "blk", 0, 0, axis_index_groups=groups)
        return same, lax.ppermute(same, "blk", swap)

    def other_half(value):
        if n_rep == 2:
            return lax.ppermute(value, "rep", [(0, 1), (1, 0)])
        return lax.psum(value, "rep") - value

    def all_products(scal):
        return lax.all_to_all(scal, ("blk", "rep"), 0, 0)

    table_shape = f32(CHANNELS * rows, LANES)
    steps = sz.pairs // 2
    (opened,) = call(opening_kernel, "opening", [f32(SUB, LANES)], [], flops=20_000_000_000)
    table, est, est_copies, anchor_rows, *sends = call(
        functools.partial(pack_kernel, sz),
        "pack",
        [table_shape, f32(*tile), f32(half, *tile), f32(sz.hi, LANES)]
        + [f32(2 * sz.edge_rows, LANES)] * (steps - 1)
        + [f32(sz.edge_rows, LANES)],
        [
            measured[:, 0], rot_vector[:, 0], confidence[:, 0], first_local[0], second_local[0], edge_counts.reshape(1, -1),
            start_angles, anchor.reshape(1, -1), opened,
        ],
    )
    recvs = [
        lax.ppermute(sends[m - 1], "blk", [(i, (i + 2 * m) % n_blk) for i in range(n_blk)]) for m in range(1, steps)
    ]
    recvs.append(lax.ppermute(sends[-1], "blk", [(i, (i + sz.pairs) % n_blk) for i in range(1, n_blk, 2)]))
    est_a, est_b = all_tiles(est_copies)

    per_edge = f32(3 * rows, LANES)
    sums_shape = f32(9 * sz.hi, LANES)
    for sweep in range(PASSES):
        last = sweep + 1 == PASSES
        if sweep == 0:
            gap_out, wc_out, sums = call(
                functools.partial(outgoing_misfit_kernel, sz),
                "misfit_outgoing",
                [per_edge, per_edge, sums_shape],
                [table, est_a, est_b, est],
                [far_shape] + sums_scratch(9),
            )
            (relay,) = call(
                functools.partial(relay_kernel, sz), "relay", [f32(steps * sz.edge_rows, LANES)], [table, *recvs]
            )
            relayed = lax.ppermute(relay, "blk", swap)
            table_in, gap_in, wc_in, sums = call(
                functools.partial(incoming_misfit_kernel, sz),
                "misfit_incoming",
                [table_shape, per_edge, per_edge, sums_shape],
                [table, relayed, *recvs[:-1], est_a, est_b, est, sums],
                [far_shape] + sums_scratch(6),
            )
        else:
            wc_out, wc_in, sums, weights, est = call(
                functools.partial(next_misfit_kernel, sz),
                "misfit_next",
                [per_edge, per_edge, sums_shape, f32(sz.pairs, sz.slots), f32(*tile)],
                [table, table_in, gap_out, gap_in, z_out, z_in, u_out, u_in, est, z, u, scal],
                sums_scratch(9),
            )
        residual, inverse, z, z_copies = call(
            functools.partial(precond_kernel, sz),
            "precond",
            [f32(*tile), f32(6 * sz.hi, LANES), f32(*tile), f32(half, *tile)],
            [sums, other_half(sums), est, anchor_rows],
        )
        z_a, z_b = all_tiles(z_copies)
        sums, *kept = call(
            functools.partial(image_kernel, sz, not last),
            "image",
            [f32(*tile)] + ([] if last else [per_edge, per_edge]),
            [table, table_in, wc_out, wc_in, z_a, z_b, z],
            [far_shape] + sums_scratch(3),
        )
        if not last:
            z_out, z_in = kept
        w, u, u_copies = call(
            functools.partial(second_precond_kernel, sz),
            "second_precond",
            [f32(*tile), f32(*tile), f32(half, *tile)],
            [sums, other_half(sums), z, anchor_rows, inverse],
        )
        u_a, u_b = all_tiles(u_copies)
        scal, *kept = call(
            functools.partial(products_kernel, sz, not last),
            "products",
            [f32(n_blk * n_rep, SUB, LANES)] + ([] if last else [per_edge, per_edge]),
            [table] + ([] if last else [table_in]) + [wc_out, u_a, u_b, residual, z, w, u, anchor_rows],
            [far_shape],
        )
        if not last:
            u_out, u_in = kept
        scal = all_products(scal)
    (estimate,) = call(functools.partial(final_kernel, sz), "final", [f32(3, sz.cams)], [est, z, u, scal])
    return (estimate, weights[None])


def solution(mesh):
    return jax.shard_map(
        on_device,
        mesh=mesh,
        in_specs=(
            P(None, "blk", None, "rep"),
            P(None, "blk", None, "rep"),
            P(None, "blk", None, "rep"),
            P("blk", None, "rep"),
            P("blk", None, "rep"),
            P("blk", None, "rep"),
            P(None, "blk"),
            P("blk"),
        ),
        out_specs=(P(None, "blk"), P("blk", None, "rep")),
        check_vma=False,
    )
```

```python
import functools

import jax
import jax.numpy as jnp
from jax import lax
from jax.experimental import pallas as pl
from jax.experimental.pallas import tpu as pltpu
from jax.sharding import PartitionSpec as P

PASSES = 2
SOFTEN = 0.05
LANES = 128
SUB = 8
SPLITS = 2
BLOCK_ENTRIES = ((0, 0), (1, 1), (2, 2), (0, 1), (0, 2), (1, 2))
MEAS, ROT, CONF, FIRST, SECOND = 0, 3, 6, 9, 10
CHANNELS = 11
F32 = jnp.float32
BF16 = jnp.bfloat16


def rotation_entries(v):
    squared = v[0] * v[0] + v[1] * v[1] + v[2] * v[2]
    factor = 2.0 / (1.0 + squared)
    skewed = ((None, -v[2], v[1]), (v[2], None, -v[0]), (-v[1], v[0], None))
    rows = []
    for a in range(3):
        row = []
        for b in range(3):
            if a == b:
                row.append(1.0 + factor * (v[a] * v[a] - squared))
            else:
                row.append(factor * (skewed[a][b] + v[a] * v[b]))
        rows.append(row)
    return rows


def rotate(rows, y):
    return [rows[a][0] * y[0] + rows[a][1] * y[1] + rows[a][2] * y[2] for a in range(3)]


def rotate_back(rows, y):
    return [rows[0][a] * y[0] + rows[1][a] * y[1] + rows[2][a] * y[2] for a in range(3)]


class Sizes:
    def __init__(self, n_blk, n_rep, pairs, slots, cams):
        self.n_blk, self.n_rep = n_blk, n_rep
        self.pairs, self.slots, self.cams = pairs, slots, cams
        self.hi = cams // LANES
        self.tile_rows = 3 * self.hi
        self.chunks = slots // LANES
        self.edge_rows = CHANNELS * self.chunks
        assert pairs == SUB and slots % LANES == 0 and cams % (LANES * SUB) == 0 and n_blk % 2 == 0


def block_at(sz, row, c):
    return pl.ds((row * sz.chunks + c) * SUB, SUB)


def chunk(sz, ref, row, c):
    return ref[block_at(sz, row, c), :]


def gather3(sz, source, index):
    hi = lax.shift_right_logical(index, 7)
    lo = lax.bitwise_and(index, LANES - 1)
    out = [None] * 3
    for r in range(sz.hi):
        mask = hi == r
        for c in range(3):
            got = jnp.take_along_axis(source(c, r), lo, axis=1, mode="promise_in_bounds")
            out[c] = got if r == 0 else jnp.where(mask, got, out[c])
    return out


def far_source(sz, far):
    return lambda c, r: far[pl.ds((c * sz.hi + r) * SUB, SUB), :]


def own_source(sz, own):
    return lambda c, r: jnp.broadcast_to(own[pl.ds(c * sz.hi + r, 1), :], (SUB, LANES))


def build_far(sz, far, tile_at, b, sign):
    for k in range(sz.pairs):
        t = lax.rem(b + (sign * k + sz.n_blk), sz.n_blk)
        far[pl.ds(k, sz.tile_rows, stride=SUB), :] = tile_at(k % 2, lax.div(t, 2))


def store_split(sz, vals, ch, c, value):
    high = value.astype(BF16).astype(F32)
    vals[block_at(sz, 2 * ch, c), :] = high
    vals[block_at(sz, 2 * ch + 1, c), :] = value - high


def scatter(sz, channels, vals, index_ref, index_row):
    lane_iota = lax.broadcasted_iota(jnp.int32, (LANES, LANES), 0).astype(F32).astype(BF16)
    row_iota = lax.rem(lax.broadcasted_iota(jnp.int32, (SPLITS * SUB, LANES), 0), SUB).astype(F32).astype(BF16)
    groups = sz.hi // SUB
    one, zero = jnp.ones((), BF16), jnp.zeros((), BF16)
    total = None
    for c in range(sz.chunks):
        index = chunk(sz, index_ref, index_row, c).astype(jnp.int32)
        lows = lax.bitwise_and(index, LANES - 1).astype(F32)
        highs = lax.shift_right_logical(index, 7).astype(F32)
        for pair in range(0, sz.pairs, 2):
            lefts, rights = [], []
            for k in (pair, pair + 1):
                lo = jnp.broadcast_to(lows[k : k + 1], (LANES, LANES)).astype(BF16)
                hi = jnp.broadcast_to(highs[k : k + 1], (SPLITS * SUB, LANES)).astype(BF16)
                rights.append(jnp.where(lane_iota == lo, one, zero))
                masks = [row_iota + float(SUB * g) == hi for g in range(groups)]
                blocks = []
                for ch in range(channels):
                    both = []
                    for part in range(SPLITS):
                        row = vals[pl.ds(((2 * ch + part) * sz.chunks + c) * SUB + k, 1), :]
                        both.append(jnp.broadcast_to(row, (SUB, LANES)))
                    both = jnp.concatenate(both, axis=0).astype(BF16)
                    blocks += [jnp.where(mask, both, zero) for mask in masks]
                lefts.append(jnp.concatenate(blocks, axis=0))
            product = lax.dot_general(
                jnp.concatenate(lefts, axis=1),
                jnp.concatenate(rights, axis=1),
                (((1,), (1,)), ((), ())),
                preferred_element_type=F32,
            )
            total = product if total is None else total + product
    total = total.reshape(channels * groups, SPLITS, SUB, LANES)
    return (total[:, 0] + total[:, 1]).reshape(channels * sz.hi, LANES)


def opening_kernel(opened):
    opened[...] = jnp.zeros_like(opened)


def pack_kernel(sz, meas, rot, conf, first, second, counts, start, anchor, opened, table, est, anchor_out, *sends):
    b = lax.axis_index("blk")
    for c in range(3):
        for r in range(sz.hi):
            est[pl.ds(c * sz.hi + r, 1), :] = start[pl.ds(c, 1), pl.ds(r * LANES, LANES)]
    for r in range(sz.hi):
        anchor_out[pl.ds(r, 1), :] = anchor[:, pl.ds(r * LANES, LANES)]
    across = lax.broadcasted_iota(jnp.int32, (sz.pairs, sz.pairs), 0)
    along = lax.broadcasted_iota(jnp.int32, (sz.pairs, sz.pairs), 1)
    spread = jnp.broadcast_to(counts[...], (sz.pairs, sz.pairs))
    limit = jnp.sum(jnp.where(across == along, spread, 0), axis=1, keepdims=True)
    for c in range(sz.chunks):
        lanes = pl.ds(c * LANES, LANES)
        slot = lax.broadcasted_iota(jnp.int32, (sz.pairs, LANES), 1) + c * LANES
        live = slot < limit
        index = first[:, lanes]
        turned = rotate(rotation_entries([rot[i, :, lanes] for i in range(3)]), gather3(sz, own_source(sz, est), index))
        for i in range(3):
            table[block_at(sz, MEAS + i, c), :] = meas[i, :, lanes] + turned[i]
            table[block_at(sz, ROT + i, c), :] = rot[i, :, lanes]
            table[block_at(sz, CONF + i, c), :] = jnp.where(live, conf[i, :, lanes], 0.0)
        table[block_at(sz, FIRST, c), :] = index.astype(F32)
        table[block_at(sz, SECOND, c), :] = second[:, lanes].astype(F32)
    odd = lax.rem(b, 2)
    count = sz.edge_rows
    for m in range(1, sz.pairs // 2):
        sends[m - 1][pl.ds(0, count), :] = table[pl.ds(2 * m, count, stride=SUB), :]
        sends[m - 1][pl.ds(count, count), :] = table[pl.ds(2 * m + 1 - 2 * odd, count, stride=SUB), :]
    sends[-1][...] = table[pl.ds(sz.pairs - 1, count, stride=SUB), :]

    @pl.when(odd == 0)
    def _():
        sends[-1][pl.ds(0, sz.tile_rows), :] = est[...]


def relay_kernel(sz, table, est, *refs):
    steps = sz.pairs // 2
    edges, tiles, mixed, relay = refs[: steps - 1], refs[steps - 1 : 2 * steps - 2], refs[-2], refs[-1]
    even_core = lax.rem(lax.axis_index("blk"), 2) == 0
    count = sz.edge_rows
    base = steps * count
    for j in range(steps):
        own = table[pl.ds(1, count, stride=SUB), :] if j == 0 else edges[j - 1][pl.ds(count, count), :]
        far = edges[j][pl.ds(count, count), :] if j + 1 < steps else mixed[...]
        relay[pl.ds(j * count, count), :] = jnp.where(even_core, own, far)
        own = est[...] if j == 0 else tiles[j - 1][...]
        far = tiles[j][...] if j + 1 < steps else mixed[pl.ds(0, sz.tile_rows), :]
        relay[pl.ds(base + j * sz.tile_rows, sz.tile_rows), :] = jnp.where(even_core, far, own)


def step_factors(scal, n):
    total = scal[0]
    for i in range(1, n):
        total = total + scal[i]
    s = [jnp.sum(total[i : i + 1, :], axis=1, keepdims=True) for i in range(4)]
    alpha0 = s[0] / s[1]
    rz1 = alpha0 * alpha0 * s[2] - s[0]
    onward = 1.0 + rz1 / s[0]
    curve = onward * onward * s[1] - 2.0 * onward * alpha0 * s[2] + alpha0 * alpha0 * s[3]
    alpha1 = rz1 / curve
    return alpha0 + alpha1 * onward, -alpha1 * alpha0


def near_kernel(sz, table, table_in, own, *near):
    for incoming in range(len(near)):
        edges, channel = (table_in, SECOND) if incoming else (table, FIRST)
        for c in range(sz.chunks):
            index = chunk(sz, edges, channel, c).astype(jnp.int32)
            put3(sz, near[incoming], c, gather3(sz, own_source(sz, own), index))


def gathered_change(sz, edges, far, near, incoming, c, rows):
    index = chunk(sz, edges, FIRST if incoming else SECOND, c).astype(jnp.int32)
    away = gather3(sz, far_source(sz, far), index)
    here = get3(sz, near, c)
    if incoming:
        turned = rotate(rows, away)
        return [here[i] - turned[i] for i in range(3)]
    turned = rotate(rows, here)
    return [away[i] - turned[i] for i in range(3)]


def edge_rotation(sz, edges, c):
    return rotation_entries([chunk(sz, edges, ROT + i, c) for i in range(3)])


def put3(sz, ref, c, values):
    for i in range(3):
        ref[block_at(sz, i, c), :] = values[i]


def get3(sz, ref, c):
    return [chunk(sz, ref, i, c) for i in range(3)]


def misfit_sums(sz, incoming, misfit_of, edges, wc_ref, weights_ref, sums, vals):
    for c in range(sz.chunks):
        rows = None
        if not incoming:
            rows = edge_rotation(sz, edges, c)
        misfit = misfit_of(c, rows)
        conf = [chunk(sz, edges, CONF + i, c) for i in range(3)]
        energy = conf[0] * misfit[0] * misfit[0] + conf[1] * misfit[1] * misfit[1] + conf[2] * misfit[2] * misfit[2]
        weight = 1.0 / jnp.sqrt(energy + SOFTEN * SOFTEN)
        if weights_ref is not None:
            weights_ref[:, pl.ds(c * LANES, LANES)] = jnp.where(conf[0] > 0.0, weight, 0.0)
        wc = [weight * conf[i] for i in range(3)]
        put3(sz, wc_ref, c, wc)
        push = [wc[i] * misfit[i] for i in range(3)]
        if incoming:
            for i in range(3):
                store_split(sz, vals, i, c, push[i])
                store_split(sz, vals, 3 + i, c, wc[i])
        else:
            back = rotate_back(rows, push)
            for i in range(3):
                store_split(sz, vals, i, c, -back[i])
            for n, (p, q) in enumerate(BLOCK_ENTRIES):
                entry = sum(rows[i][p] * wc[i] * rows[i][q] for i in range(3))
                store_split(sz, vals, 3 + n, c, entry)
    part = scatter(sz, 6 if incoming else 9, vals, edges, SECOND if incoming else FIRST)
    if incoming:
        cut = 6 * sz.hi
        sums[pl.ds(0, cut), :] = sums[pl.ds(0, cut), :] + part
    else:
        sums[...] = part


def outgoing_misfit_kernel(sz, table, own, relayed, *refs):
    steps = sz.pairs // 2
    tiles, (gap, wc, sums, far, vals) = refs[: steps - 1], refs[steps - 1 :]
    base = steps * sz.edge_rows
    for k in range(sz.pairs):
        if k == 0:
            block = own[...]
        elif k % 2:
            block = relayed[pl.ds(base + (k // 2) * sz.tile_rows, sz.tile_rows), :]
        else:
            block = tiles[k // 2 - 1][...]
        far[pl.ds(k, sz.tile_rows, stride=SUB), :] = block

    def misfit_of(c, rows):
        away = gather3(sz, far_source(sz, far), chunk(sz, table, SECOND, c).astype(jnp.int32))
        misfit = [chunk(sz, table, MEAS + i, c) - away[i] for i in range(3)]
        put3(sz, gap, c, misfit)
        return misfit

    misfit_sums(sz, False, misfit_of, table, wc, None, sums, vals)


def incoming_misfit_kernel(sz, table, relayed, own, sums_out, *refs):
    steps = sz.pairs // 2
    edges, (table_in, gap, wc, sums, vals) = refs[: steps - 1], refs[steps - 1 :]
    count = sz.edge_rows
    for k in range(sz.pairs):
        if k == 0:
            block = table[pl.ds(0, count, stride=SUB), :]
        elif k % 2:
            block = relayed[pl.ds((k // 2) * count, count), :]
        else:
            block = edges[k // 2 - 1][pl.ds(0, count), :]
        table_in[pl.ds(k, count, stride=SUB), :] = block
    sums[...] = sums_out[...]

    def misfit_of(c, rows):
        here = gather3(sz, own_source(sz, own), chunk(sz, table_in, SECOND, c).astype(jnp.int32))
        misfit = [chunk(sz, table_in, MEAS + i, c) - here[i] for i in range(3)]
        put3(sz, gap, c, misfit)
        return misfit

    misfit_sums(sz, True, misfit_of, table_in, wc, None, sums, vals)


def next_misfit_kernel(
    sz, table, table_in, gap_out, gap_in, z_out, z_in, u_out, u_in, own, z, u, scal,
    wc_out, wc_in, sums, weights, own_new, vals,
):
    along_z, along_u = step_factors(scal, sz.n_blk * sz.n_rep)
    own_new[...] = own[...] + along_z * z[...] + along_u * u[...]
    for incoming in (False, True):
        edges, wc_ref = (table_in, wc_in) if incoming else (table, wc_out)
        old, by_z, by_u = (gap_in, z_in, u_in) if incoming else (gap_out, z_out, u_out)

        def misfit_of(c, rows):
            old3, z3, u3 = get3(sz, old, c), get3(sz, by_z, c), get3(sz, by_u, c)
            return [old3[i] - (along_z * z3[i] + along_u * u3[i]) for i in range(3)]

        misfit_sums(sz, incoming, misfit_of, edges, wc_ref, None if incoming else weights, sums, vals)


def apply_inverse(sz, inv, v):
    a00, a11, a22, a01, a02, a12 = inv
    return [
        a00 * v[0] + a01 * v[1] + a02 * v[2],
        a01 * v[0] + a11 * v[1] + a12 * v[2],
        a02 * v[0] + a12 * v[1] + a22 * v[2],
    ]


def comp(sz, ref, i):
    return ref[pl.ds(i * sz.hi, sz.hi), :]


def precond_kernel(sz, mine, other, est, anchor, residual, inverse, z, z_copies):
    total = mine[...] + other[...]
    part = lambda i: total[i * sz.hi : (i + 1) * sz.hi]
    anc = anchor[...]
    res = [part(i) - anc * comp(sz, est, i) for i in range(3)]
    p00, p11, p22 = [part(3 + i) + anc for i in range(3)]
    p01, p02, p12 = [part(6 + i) for i in range(3)]
    adj00 = p11 * p22 - p12 * p12
    adj01 = p02 * p12 - p01 * p22
    adj02 = p01 * p12 - p02 * p11
    adj11 = p00 * p22 - p02 * p02
    adj12 = p01 * p02 - p00 * p12
    adj22 = p00 * p11 - p01 * p01
    det = p00 * adj00 + p01 * adj01 + p02 * adj02
    inv = [a / det for a in (adj00, adj11, adj22, adj01, adj02, adj12)]
    scaled = apply_inverse(sz, inv, res)
    for i in range(3):
        residual[pl.ds(i * sz.hi, sz.hi), :] = res[i]
        z[pl.ds(i * sz.hi, sz.hi), :] = scaled[i]
    for i in range(6):
        inverse[pl.ds(i * sz.hi, sz.hi), :] = inv[i]
    for i in range(sz.n_blk // 2):
        z_copies[i] = z[...]


def image_kernel(sz, keep, table, table_in, wc_out, wc_in, z_a, z_b, near_out, near_in, sums, *refs):
    kept, (far, vals) = refs[:-2], refs[-2:]
    b = lax.axis_index("blk")

    def tile_at(parity, q):
        return (z_b if parity else z_a)[q]

    for incoming in (False, True):
        edges, wc_ref = (table_in, wc_in) if incoming else (table, wc_out)
        build_far(sz, far, tile_at, b, -1 if incoming else 1)
        for c in range(sz.chunks):
            rows = edge_rotation(sz, edges, c)
            change = gathered_change(sz, edges, far, near_in if incoming else near_out, incoming, c, rows)
            if keep:
                put3(sz, kept[int(incoming)], c, change)
            wc = get3(sz, wc_ref, c)
            push = [wc[i] * change[i] for i in range(3)]
            if incoming:
                for i in range(3):
                    store_split(sz, vals, i, c, push[i])
            else:
                back = rotate_back(rows, push)
                for i in range(3):
                    store_split(sz, vals, i, c, -back[i])
        part = scatter(sz, 3, vals, edges, SECOND if incoming else FIRST)
        if incoming:
            sums[...] = sums[...] + part
        else:
            sums[...] = part


def second_precond_kernel(sz, mine, other, z, anchor, inverse, w, u, u_copies):
    total = mine[...] + other[...]
    anc = anchor[...]
    image = [total[i * sz.hi : (i + 1) * sz.hi] + anc * comp(sz, z, i) for i in range(3)]
    scaled = apply_inverse(sz, [comp(sz, inverse, i) for i in range(6)], image)
    for i in range(3):
        w[pl.ds(i * sz.hi, sz.hi), :] = image[i]
        u[pl.ds(i * sz.hi, sz.hi), :] = scaled[i]
    for i in range(sz.n_blk // 2):
        u_copies[i] = u[...]


def fold(value):
    rows = value.shape[0]
    out = value[:SUB]
    for i in range(1, rows // SUB):
        out = out + value[i * SUB : (i + 1) * SUB]
    return out


def products_kernel(sz, keep, table, *refs):
    refs = list(refs)
    table_in = refs.pop(0) if keep else None
    near_out = refs.pop(0)
    near_in = refs.pop(0) if keep else None
    wc_out, u_a, u_b, residual, z, w, u, anchor, scal = refs[:9]
    kept, far = refs[9:-1], refs[-1]
    b = lax.axis_index("blk")

    def tile_at(parity, q):
        return (u_b if parity else u_a)[q]

    acc = jnp.zeros((SUB, LANES), F32)
    for incoming in (False, True) if keep else (False,):
        edges = table_in if incoming else table
        build_far(sz, far, tile_at, b, -1 if incoming else 1)
        for c in range(sz.chunks):
            near = near_in if incoming else near_out
            change = gathered_change(sz, edges, far, near, incoming, c, edge_rotation(sz, edges, c))
            if keep:
                put3(sz, kept[int(incoming)], c, change)
            if not incoming:
                wc = get3(sz, wc_out, c)
                for i in range(3):
                    acc = acc + wc[i] * change[i] * change[i]
    share = 1.0 / sz.n_rep
    res, zz, ww, uu = residual[...], z[...], w[...], u[...]
    s1 = fold(res * zz) * share
    s2 = fold(zz * ww) * share
    s3 = fold(ww * uu) * share
    anc = anchor[...]
    s4 = acc + share * fold(anc * (comp(sz, u, 0) * comp(sz, u, 0) + comp(sz, u, 1) * comp(sz, u, 1) + comp(sz, u, 2) * comp(sz, u, 2)))
    block = [jnp.sum(s, axis=0, keepdims=True) for s in (s1, s2, s3, s4)]
    block = jnp.concatenate(block + [jnp.zeros((SUB - 4, LANES), F32)], axis=0)
    for i in range(sz.n_blk * sz.n_rep):
        scal[i] = block


def final_kernel(sz, est, z, u, scal, out):
    along_z, along_u = step_factors(scal, sz.n_blk * sz.n_rep)
    new = est[...] + along_z * z[...] + along_u * u[...]
    for c in range(3):
        for r in range(sz.hi):
            row = c * sz.hi + r
            out[pl.ds(c, 1), pl.ds(r * LANES, LANES)] = new[row : row + 1]


def on_device(measured, rot_vector, confidence, first_local, second_local, edge_counts, start_angles, anchor):
    n_blk, n_rep = lax.axis_size("blk"), lax.axis_size("rep")
    sz = Sizes(n_blk, n_rep, first_local.shape[1], first_local.shape[2], start_angles.shape[1])
    half = n_blk // 2
    tile = (sz.tile_rows, LANES)
    f32 = lambda *shape: jax.ShapeDtypeStruct(shape, F32)
    vmem = pl.BlockSpec(memory_space=pltpu.VMEM)
    rows = sz.chunks * SUB
    far_shape = pltpu.VMEM((sz.tile_rows * SUB, LANES), F32)

    def sums_scratch(channels):
        return [
            pltpu.VMEM((channels * 2 * rows, LANES), F32),
        ]

    def call(kernel, name, outs, args, scratch_shapes=(), flops=20_000_000):
        return pl.pallas_call(
            kernel,
            name=name,
            out_shape=outs,
            in_specs=[vmem] * len(args),
            out_specs=[vmem] * len(outs),
            scratch_shapes=list(scratch_shapes),
            cost_estimate=pl.CostEstimate(flops=flops, bytes_accessed=flops // 10, transcendentals=0),
            compiler_params=pltpu.CompilerParams(vmem_limit_bytes=48 * 1024 * 1024),
        )(*args)

    groups = [[core + 2 * i for i in range(half)] for core in range(2)]
    swap = [(i, i ^ 1) for i in range(n_blk)]

    def all_tiles(copies):
        same = lax.all_to_all(copies, "blk", 0, 0, axis_index_groups=groups)
        return same, lax.ppermute(same, "blk", swap)

    def other_half(value):
        if n_rep == 2:
            return lax.ppermute(value, "rep", [(0, 1), (1, 0)])
        return lax.psum(value, "rep") - value

    def all_products(scal):
        return lax.all_to_all(scal, ("blk", "rep"), 0, 0)

    table_shape = f32(CHANNELS * rows, LANES)
    steps = sz.pairs // 2
    (opened,) = call(opening_kernel, "opening", [f32(SUB, LANES)], [], flops=20_000_000_000)
    table, est, anchor_rows, *sends = call(
        functools.partial(pack_kernel, sz),
        "pack",
        [table_shape, f32(*tile), f32(sz.hi, LANES)]
        + [f32(2 * sz.edge_rows, LANES)] * (steps - 1)
        + [f32(sz.edge_rows, LANES)],
        [
            measured[:, 0], rot_vector[:, 0], confidence[:, 0], first_local[0], second_local[0], edge_counts.reshape(1, -1),
            start_angles, anchor.reshape(1, -1), opened,
        ],
    )
    ring = lambda shift, kept: [(i, (i + shift + n_blk) % n_blk) for i in range(n_blk) if i % 2 in kept]
    mixed = lax.ppermute(sends[-1], "blk", ring(-sz.pairs, (0,)) + ring(sz.pairs, (1,)))
    edges = [lax.ppermute(sends[m - 1], "blk", ring(2 * m, (0, 1))) for m in range(1, steps)]
    tiles = [lax.ppermute(est, "blk", ring(-2 * m, (0, 1))) for m in range(1, steps)]

    per_edge = f32(3 * rows, LANES)
    sums_shape = f32(9 * sz.hi, LANES)
    for sweep in range(PASSES):
        last = sweep + 1 == PASSES
        if sweep == 0:
            (relay,) = call(
                functools.partial(relay_kernel, sz),
                "relay",
                [f32(steps * (sz.edge_rows + sz.tile_rows), LANES)],
                [table, est, *edges, *tiles, mixed],
            )
            relayed = lax.ppermute(relay, "blk", swap)
            gap_out, wc_out, sums = call(
                functools.partial(outgoing_misfit_kernel, sz),
                "misfit_outgoing",
                [per_edge, per_edge, sums_shape],
                [table, est, relayed, *tiles],
                [far_shape] + sums_scratch(9),
            )
            table_in, gap_in, wc_in, sums = call(
                functools.partial(incoming_misfit_kernel, sz),
                "misfit_incoming",
                [table_shape, per_edge, per_edge, sums_shape],
                [table, relayed, est, sums, *edges],
                sums_scratch(6),
            )
        else:
            wc_out, wc_in, sums, weights, est = call(
                functools.partial(next_misfit_kernel, sz),
                "misfit_next",
                [per_edge, per_edge, sums_shape, f32(sz.pairs, sz.slots), f32(*tile)],
                [table, table_in, gap_out, gap_in, z_out, z_in, u_out, u_in, est, z, u, scal],
                sums_scratch(9),
            )
        residual, inverse, z, z_copies = call(
            functools.partial(precond_kernel, sz),
            "precond",
            [f32(*tile), f32(6 * sz.hi, LANES), f32(*tile), f32(half, *tile)],
            [sums, other_half(sums), est, anchor_rows],
        )
        z_a, z_b = all_tiles(z_copies)
        near_out, near_in = call(
            functools.partial(near_kernel, sz), "near_z", [per_edge, per_edge], [table, table_in, z]
        )
        sums, *kept = call(
            functools.partial(image_kernel, sz, not last),
            "image",
            [f32(*tile)] + ([] if last else [per_edge, per_edge]),
            [table, table_in, wc_out, wc_in, z_a, z_b, near_out, near_in],
            [far_shape] + sums_scratch(3),
        )
        if not last:
            z_out, z_in = kept
        w, u, u_copies = call(
            functools.partial(second_precond_kernel, sz),
            "second_precond",
            [f32(*tile), f32(*tile), f32(half, *tile)],
            [sums, other_half(sums), z, anchor_rows, inverse],
        )
        u_a, u_b = all_tiles(u_copies)
        near = call(
            functools.partial(near_kernel, sz), "near_u", [per_edge] * (1 if last else 2), [table, table_in, u]
        )
        scal, *kept = call(
            functools.partial(products_kernel, sz, not last),
            "products",
            [f32(n_blk * n_rep, SUB, LANES)] + ([] if last else [per_edge, per_edge]),
            [table] + ([] if last else [table_in]) + [*near, wc_out, u_a, u_b, residual, z, w, u, anchor_rows],
            [far_shape],
        )
        if not last:
            u_out, u_in = kept
        scal = all_products(scal)
    (estimate,) = call(functools.partial(final_kernel, sz), "final", [f32(3, sz.cams)], [est, z, u, scal])
    return (estimate, weights[None])


def solution(mesh):
    return jax.shard_map(
        on_device,
        mesh=mesh,
        in_specs=(
            P(None, "blk", None, "rep"),
            P(None, "blk", None, "rep"),
            P(None, "blk", None, "rep"),
            P("blk", None, "rep"),
            P("blk", None, "rep"),
            P("blk", None, "rep"),
            P(None, "blk"),
            P("blk"),
        ),
        out_specs=(P(None, "blk"), P("blk", None, "rep")),
        check_vma=False,
    )
```

```python
import functools

import jax
import jax.numpy as jnp
from jax import lax
from jax.experimental import pallas as pl
from jax.experimental.pallas import tpu as pltpu
from jax.sharding import PartitionSpec as P

PASSES = 2
SOFTEN = 0.05
LANES = 128
SUB = 8
SPLITS = 2
BLOCK_ENTRIES = ((0, 0), (1, 1), (2, 2), (0, 1), (0, 2), (1, 2))
MEAS, ROT, CONF, FIRST, SECOND = 0, 3, 6, 9, 10
CHANNELS = 11
F32 = jnp.float32
BF16 = jnp.bfloat16


def rotation_entries(v):
    squared = v[0] * v[0] + v[1] * v[1] + v[2] * v[2]
    factor = 2.0 / (1.0 + squared)
    skewed = ((None, -v[2], v[1]), (v[2], None, -v[0]), (-v[1], v[0], None))
    rows = []
    for a in range(3):
        row = []
        for b in range(3):
            if a == b:
                row.append(1.0 + factor * (v[a] * v[a] - squared))
            else:
                row.append(factor * (skewed[a][b] + v[a] * v[b]))
        rows.append(row)
    return rows


def rotate(rows, y):
    return [rows[a][0] * y[0] + rows[a][1] * y[1] + rows[a][2] * y[2] for a in range(3)]


def rotate_back(rows, y):
    return [rows[0][a] * y[0] + rows[1][a] * y[1] + rows[2][a] * y[2] for a in range(3)]


class Sizes:
    def __init__(self, n_blk, n_rep, pairs, slots, cams):
        self.n_blk, self.n_rep = n_blk, n_rep
        self.pairs, self.slots, self.cams = pairs, slots, cams
        self.hi = cams // LANES
        self.tile_rows = 3 * self.hi
        self.chunks = slots // LANES
        self.edge_rows = CHANNELS * self.chunks
        assert pairs == SUB and slots % LANES == 0 and cams % (LANES * SUB) == 0 and n_blk % 2 == 0


def block_at(sz, row, c):
    return pl.ds((row * sz.chunks + c) * SUB, SUB)


def chunk(sz, ref, row, c):
    return ref[block_at(sz, row, c), :]


def gather3(sz, source, index):
    hi = lax.shift_right_logical(index, 7)
    lo = lax.bitwise_and(index, LANES - 1)
    out = [None] * 3
    for r in range(sz.hi):
        mask = hi == r
        for c in range(3):
            got = jnp.take_along_axis(source(c, r), lo, axis=1, mode="promise_in_bounds")
            out[c] = got if r == 0 else jnp.where(mask, got, out[c])
    return out


def far_source(sz, far):
    return lambda c, r: far[pl.ds((c * sz.hi + r) * SUB, SUB), :]


def own_source(sz, own):
    return lambda c, r: jnp.broadcast_to(own[pl.ds(c * sz.hi + r, 1), :], (SUB, LANES))


def build_far(sz, far, tile_at, b, sign):
    for k in range(sz.pairs):
        t = lax.rem(b + (sign * k + sz.n_blk), sz.n_blk)
        far[pl.ds(k, sz.tile_rows, stride=SUB), :] = tile_at(k % 2, lax.div(t, 2))


def store_split(sz, vals, ch, c, value):
    high = value.astype(BF16).astype(F32)
    vals[block_at(sz, 2 * ch, c), :] = high
    vals[block_at(sz, 2 * ch + 1, c), :] = value - high


def scatter(sz, channels, vals, index_ref, index_row):
    lane_iota = lax.broadcasted_iota(jnp.int32, (LANES, LANES), 0).astype(F32).astype(BF16)
    row_iota = lax.rem(lax.broadcasted_iota(jnp.int32, (SPLITS * SUB, LANES), 0), SUB).astype(F32).astype(BF16)
    groups = sz.hi // SUB
    one, zero = jnp.ones((), BF16), jnp.zeros((), BF16)
    total = None
    for c in range(sz.chunks):
        index = chunk(sz, index_ref, index_row, c).astype(jnp.int32)
        lows = lax.bitwise_and(index, LANES - 1).astype(F32)
        highs = lax.shift_right_logical(index, 7).astype(F32)
        for pair in range(0, sz.pairs, 2):
            lefts, rights = [], []
            for k in (pair, pair + 1):
                lo = jnp.broadcast_to(lows[k : k + 1], (LANES, LANES)).astype(BF16)
                hi = jnp.broadcast_to(highs[k : k + 1], (SPLITS * SUB, LANES)).astype(BF16)
                rights.append(jnp.where(lane_iota == lo, one, zero))
                masks = [row_iota + float(SUB * g) == hi for g in range(groups)]
                blocks = []
                for ch in range(channels):
                    both = []
                    for part in range(SPLITS):
                        row = vals[pl.ds(((2 * ch + part) * sz.chunks + c) * SUB + k, 1), :]
                        both.append(jnp.broadcast_to(row, (SUB, LANES)))
                    both = jnp.concatenate(both, axis=0).astype(BF16)
                    blocks += [jnp.where(mask, both, zero) for mask in masks]
                lefts.append(jnp.concatenate(blocks, axis=0))
            product = lax.dot_general(
                jnp.concatenate(lefts, axis=1),
                jnp.concatenate(rights, axis=1),
                (((1,), (1,)), ((), ())),
                preferred_element_type=F32,
            )
            total = product if total is None else total + product
    total = total.reshape(channels * groups, SPLITS, SUB, LANES)
    return (total[:, 0] + total[:, 1]).reshape(channels * sz.hi, LANES)


def opening_kernel(opened):
    opened[...] = jnp.zeros_like(opened)


def pack_kernel(sz, meas, rot, conf, first, second, counts, start, anchor, opened, table, est, anchor_out, swap):
    b = lax.axis_index("blk")
    for c in range(3):
        for r in range(sz.hi):
            est[pl.ds(c * sz.hi + r, 1), :] = start[pl.ds(c, 1), pl.ds(r * LANES, LANES)]
    for r in range(sz.hi):
        anchor_out[pl.ds(r, 1), :] = anchor[:, pl.ds(r * LANES, LANES)]
    across = lax.broadcasted_iota(jnp.int32, (sz.pairs, sz.pairs), 0)
    along = lax.broadcasted_iota(jnp.int32, (sz.pairs, sz.pairs), 1)
    spread = jnp.broadcast_to(counts[...], (sz.pairs, sz.pairs))
    limit = jnp.sum(jnp.where(across == along, spread, 0), axis=1, keepdims=True)
    for c in range(sz.chunks):
        lanes = pl.ds(c * LANES, LANES)
        slot = lax.broadcasted_iota(jnp.int32, (sz.pairs, LANES), 1) + c * LANES
        live = slot < limit
        index = first[:, lanes]
        turned = rotate(rotation_entries([rot[i, :, lanes] for i in range(3)]), gather3(sz, own_source(sz, est), index))
        for i in range(3):
            table[block_at(sz, MEAS + i, c), :] = meas[i, :, lanes] + turned[i]
            table[block_at(sz, ROT + i, c), :] = rot[i, :, lanes]
            table[block_at(sz, CONF + i, c), :] = jnp.where(live, conf[i, :, lanes], 0.0)
        table[block_at(sz, FIRST, c), :] = index.astype(F32)
        table[block_at(sz, SECOND, c), :] = second[:, lanes].astype(F32)
    odd = lax.rem(b, 2)
    count = sz.edge_rows
    for j, (from_odd, from_even) in enumerate(((1, 4), (2, 5), (5, 4), (6, 5))):
        k = from_even + odd * (from_odd - from_even)
        swap[pl.ds(j * count, count), :] = table[pl.ds(k, count, stride=SUB), :]
    swap[pl.ds(4 * count, sz.tile_rows), :] = est[...]


def load_kernel(sz, table, est, sibling, near_edges, far_edges, tiles):
    count = sz.edge_rows
    even = lax.rem(lax.axis_index("blk"), 2) == 0
    own = lambda k: table[pl.ds(k, count, stride=SUB), :]
    other = lambda j: sibling[pl.ds(j * count, count), :]
    for j, (if_even, if_odd) in enumerate(((own(2), other(0)), (own(3), other(1)), (other(0), own(3)), (other(1), own(4)))):
        near_edges[pl.ds(j * count, count), :] = jnp.where(even, if_even, if_odd)
    for j, (if_even, if_odd) in enumerate(((own(6), other(0)), (own(7), other(1)), (other(2), own(7)), (other(3), own(7)))):
        far_edges[pl.ds(j * count, count), :] = jnp.where(even, if_even, if_odd)
    mine, theirs = est[...], sibling[pl.ds(4 * count, sz.tile_rows), :]
    tiles[pl.ds(0, sz.tile_rows), :] = jnp.where(even, mine, theirs)
    tiles[pl.ds(sz.tile_rows, sz.tile_rows), :] = jnp.where(even, theirs, mine)


def relay_kernel(sz, table, near_edges, far_edges, near_tiles, far_tiles, relay):
    count = sz.edge_rows
    even = lax.rem(lax.axis_index("blk"), 2) == 0
    near = lambda j: near_edges[pl.ds(j * count, count), :]
    far = lambda j: far_edges[pl.ds(j * count, count), :]
    first = table[pl.ds(1, count, stride=SUB), :]
    for j, (if_even, if_odd) in enumerate(((first, near(2)), (near(3), near(0)), (near(1), far(2)), (far(3), far(2)), (far(1), far(2)))):
        relay[pl.ds(j * count, count), :] = jnp.where(even, if_even, if_odd)
    relay[pl.ds(5 * count, 2 * sz.tile_rows), :] = near_tiles[...]
    relay[pl.ds(5 * count + 2 * sz.tile_rows, 2 * sz.tile_rows), :] = far_tiles[...]


def step_factors(scal, n):
    total = scal[0]
    for i in range(1, n):
        total = total + scal[i]
    s = [jnp.sum(total[i : i + 1, :], axis=1, keepdims=True) for i in range(4)]
    alpha0 = s[0] / s[1]
    rz1 = alpha0 * alpha0 * s[2] - s[0]
    onward = 1.0 + rz1 / s[0]
    curve = onward * onward * s[1] - 2.0 * onward * alpha0 * s[2] + alpha0 * alpha0 * s[3]
    alpha1 = rz1 / curve
    return alpha0 + alpha1 * onward, -alpha1 * alpha0


def near_kernel(sz, table, table_in, own, *near):
    for incoming in range(len(near)):
        edges, channel = (table_in, SECOND) if incoming else (table, FIRST)
        for c in range(sz.chunks):
            index = chunk(sz, edges, channel, c).astype(jnp.int32)
            put3(sz, near[incoming], c, gather3(sz, own_source(sz, own), index))


def gathered_change(sz, edges, far, near, incoming, c, rows):
    index = chunk(sz, edges, FIRST if incoming else SECOND, c).astype(jnp.int32)
    away = gather3(sz, far_source(sz, far), index)
    here = get3(sz, near, c)
    if incoming:
        turned = rotate(rows, away)
        return [here[i] - turned[i] for i in range(3)]
    turned = rotate(rows, here)
    return [away[i] - turned[i] for i in range(3)]


def edge_rotation(sz, edges, c):
    return rotation_entries([chunk(sz, edges, ROT + i, c) for i in range(3)])


def put3(sz, ref, c, values):
    for i in range(3):
        ref[block_at(sz, i, c), :] = values[i]


def get3(sz, ref, c):
    return [chunk(sz, ref, i, c) for i in range(3)]


def misfit_sums(sz, incoming, misfit_of, edges, wc_ref, weights_ref, sums, vals):
    for c in range(sz.chunks):
        rows = None
        if not incoming:
            rows = edge_rotation(sz, edges, c)
        misfit = misfit_of(c, rows)
        conf = [chunk(sz, edges, CONF + i, c) for i in range(3)]
        energy = conf[0] * misfit[0] * misfit[0] + conf[1] * misfit[1] * misfit[1] + conf[2] * misfit[2] * misfit[2]
        weight = 1.0 / jnp.sqrt(energy + SOFTEN * SOFTEN)
        if weights_ref is not None:
            weights_ref[:, pl.ds(c * LANES, LANES)] = jnp.where(conf[0] > 0.0, weight, 0.0)
        wc = [weight * conf[i] for i in range(3)]
        put3(sz, wc_ref, c, wc)
        push = [wc[i] * misfit[i] for i in range(3)]
        if incoming:
            for i in range(3):
                store_split(sz, vals, i, c, push[i])
                store_split(sz, vals, 3 + i, c, wc[i])
        else:
            back = rotate_back(rows, push)
            for i in range(3):
                store_split(sz, vals, i, c, -back[i])
            for n, (p, q) in enumerate(BLOCK_ENTRIES):
                entry = sum(rows[i][p] * wc[i] * rows[i][q] for i in range(3))
                store_split(sz, vals, 3 + n, c, entry)
    part = scatter(sz, 6 if incoming else 9, vals, edges, SECOND if incoming else FIRST)
    if incoming:
        cut = 6 * sz.hi
        sums[pl.ds(0, cut), :] = sums[pl.ds(0, cut), :] + part
    else:
        sums[...] = part


def outgoing_misfit_kernel(sz, table, own, sibling, relayed, near_tiles, far_tiles, gap, wc, sums, far, vals):
    even = lax.rem(lax.axis_index("blk"), 2) == 0
    tile = sz.tile_rows
    near = lambda j: near_tiles[pl.ds(j * tile, tile), :]
    away = lambda j: far_tiles[pl.ds(j * tile, tile), :]
    passed = lambda j: relayed[pl.ds(5 * sz.edge_rows + j * tile, tile), :]
    beside = sibling[pl.ds(4 * sz.edge_rows, tile), :]
    far[pl.ds(0, tile, stride=SUB), :] = own[...]
    for k, (if_even, if_odd) in enumerate(
        (
            (beside, passed(0)), (near(0), passed(1)), (near(1), near(0)), (passed(0), near(1)),
            (passed(1), passed(2)), (away(0), passed(3)), (away(1), away(0)),
        ),
        1,
    ):
        far[pl.ds(k, tile, stride=SUB), :] = jnp.where(even, if_even, if_odd)

    def misfit_of(c, rows):
        away = gather3(sz, far_source(sz, far), chunk(sz, table, SECOND, c).astype(jnp.int32))
        misfit = [chunk(sz, table, MEAS + i, c) - away[i] for i in range(3)]
        put3(sz, gap, c, misfit)
        return misfit

    misfit_sums(sz, False, misfit_of, table, wc, None, sums, vals)


def incoming_misfit_kernel(sz, table, relayed, own, sums_out, near_edges, far_edges, table_in, gap, wc, sums, vals):
    count = sz.edge_rows
    even = lax.rem(lax.axis_index("blk"), 2) == 0
    near = lambda j: near_edges[pl.ds(j * count, count), :]
    away = lambda j: far_edges[pl.ds(j * count, count), :]
    passed = lambda j: relayed[pl.ds(j * count, count), :]
    table_in[pl.ds(0, count, stride=SUB), :] = table[pl.ds(0, count, stride=SUB), :]
    for k, (if_even, if_odd) in enumerate(
        (
            (near(2), passed(0)), (near(0), passed(1)), (passed(0), passed(2)), (passed(1), near(3)),
            (away(2), near(1)), (away(0), passed(3)), (passed(2), passed(4)),
        ),
        1,
    ):
        table_in[pl.ds(k, count, stride=SUB), :] = jnp.where(even, if_even, if_odd)
    sums[...] = sums_out[...]

    def misfit_of(c, rows):
        here = gather3(sz, own_source(sz, own), chunk(sz, table_in, SECOND, c).astype(jnp.int32))
        misfit = [chunk(sz, table_in, MEAS + i, c) - here[i] for i in range(3)]
        put3(sz, gap, c, misfit)
        return misfit

    misfit_sums(sz, True, misfit_of, table_in, wc, None, sums, vals)


def next_misfit_kernel(
    sz, table, table_in, gap_out, gap_in, z_out, z_in, u_out, u_in, own, z, u, scal,
    wc_out, wc_in, sums, weights, own_new, vals,
):
    along_z, along_u = step_factors(scal, sz.n_blk * sz.n_rep)
    own_new[...] = own[...] + along_z * z[...] + along_u * u[...]
    for incoming in (False, True):
        edges, wc_ref = (table_in, wc_in) if incoming else (table, wc_out)
        old, by_z, by_u = (gap_in, z_in, u_in) if incoming else (gap_out, z_out, u_out)

        def misfit_of(c, rows):
            old3, z3, u3 = get3(sz, old, c), get3(sz, by_z, c), get3(sz, by_u, c)
            return [old3[i] - (along_z * z3[i] + along_u * u3[i]) for i in range(3)]

        misfit_sums(sz, incoming, misfit_of, edges, wc_ref, None if incoming else weights, sums, vals)


def apply_inverse(sz, inv, v):
    a00, a11, a22, a01, a02, a12 = inv
    return [
        a00 * v[0] + a01 * v[1] + a02 * v[2],
        a01 * v[0] + a11 * v[1] + a12 * v[2],
        a02 * v[0] + a12 * v[1] + a22 * v[2],
    ]


def comp(sz, ref, i):
    return ref[pl.ds(i * sz.hi, sz.hi), :]


def precond_kernel(sz, mine, other, est, anchor, residual, inverse, z, z_copies):
    total = mine[...] + other[...]
    part = lambda i: total[i * sz.hi : (i + 1) * sz.hi]
    anc = anchor[...]
    res = [part(i) - anc * comp(sz, est, i) for i in range(3)]
    p00, p11, p22 = [part(3 + i) + anc for i in range(3)]
    p01, p02, p12 = [part(6 + i) for i in range(3)]
    adj00 = p11 * p22 - p12 * p12
    adj01 = p02 * p12 - p01 * p22
    adj02 = p01 * p12 - p02 * p11
    adj11 = p00 * p22 - p02 * p02
    adj12 = p01 * p02 - p00 * p12
    adj22 = p00 * p11 - p01 * p01
    det = p00 * adj00 + p01 * adj01 + p02 * adj02
    inv = [a / det for a in (adj00, adj11, adj22, adj01, adj02, adj12)]
    scaled = apply_inverse(sz, inv, res)
    for i in range(3):
        residual[pl.ds(i * sz.hi, sz.hi), :] = res[i]
        z[pl.ds(i * sz.hi, sz.hi), :] = scaled[i]
    for i in range(6):
        inverse[pl.ds(i * sz.hi, sz.hi), :] = inv[i]
    for i in range(sz.n_blk // 2):
        z_copies[i] = z[...]


def image_kernel(sz, keep, table, table_in, wc_out, wc_in, z_a, z_b, near_out, near_in, sums, *refs):
    kept, (far, vals) = refs[:-2], refs[-2:]
    b = lax.axis_index("blk")

    def tile_at(parity, q):
        return (z_b if parity else z_a)[q]

    for incoming in (False, True):
        edges, wc_ref = (table_in, wc_in) if incoming else (table, wc_out)
        build_far(sz, far, tile_at, b, -1 if incoming else 1)
        for c in range(sz.chunks):
            rows = edge_rotation(sz, edges, c)
            change = gathered_change(sz, edges, far, near_in if incoming else near_out, incoming, c, rows)
            if keep:
                put3(sz, kept[int(incoming)], c, change)
            wc = get3(sz, wc_ref, c)
            push = [wc[i] * change[i] for i in range(3)]
            if incoming:
                for i in range(3):
                    store_split(sz, vals, i, c, push[i])
            else:
                back = rotate_back(rows, push)
                for i in range(3):
                    store_split(sz, vals, i, c, -back[i])
        part = scatter(sz, 3, vals, edges, SECOND if incoming else FIRST)
        if incoming:
            sums[...] = sums[...] + part
        else:
            sums[...] = part


def second_precond_kernel(sz, mine, other, z, anchor, inverse, w, u, u_copies):
    total = mine[...] + other[...]
    anc = anchor[...]
    image = [total[i * sz.hi : (i + 1) * sz.hi] + anc * comp(sz, z, i) for i in range(3)]
    scaled = apply_inverse(sz, [comp(sz, inverse, i) for i in range(6)], image)
    for i in range(3):
        w[pl.ds(i * sz.hi, sz.hi), :] = image[i]
        u[pl.ds(i * sz.hi, sz.hi), :] = scaled[i]
    for i in range(sz.n_blk // 2):
        u_copies[i] = u[...]


def fold(value):
    rows = value.shape[0]
    out = value[:SUB]
    for i in range(1, rows // SUB):
        out = out + value[i * SUB : (i + 1) * SUB]
    return out


def products_kernel(sz, keep, table, *refs):
    refs = list(refs)
    table_in = refs.pop(0) if keep else None
    near_out = refs.pop(0)
    near_in = refs.pop(0) if keep else None
    wc_out, u_a, u_b, residual, z, w, u, anchor, scal = refs[:9]
    kept, far = refs[9:-1], refs[-1]
    b = lax.axis_index("blk")

    def tile_at(parity, q):
        return (u_b if parity else u_a)[q]

    acc = jnp.zeros((SUB, LANES), F32)
    for incoming in (False, True) if keep else (False,):
        edges = table_in if incoming else table
        build_far(sz, far, tile_at, b, -1 if incoming else 1)
        for c in range(sz.chunks):
            near = near_in if incoming else near_out
            change = gathered_change(sz, edges, far, near, incoming, c, edge_rotation(sz, edges, c))
            if keep:
                put3(sz, kept[int(incoming)], c, change)
            if not incoming:
                wc = get3(sz, wc_out, c)
                for i in range(3):
                    acc = acc + wc[i] * change[i] * change[i]
    share = 1.0 / sz.n_rep
    res, zz, ww, uu = residual[...], z[...], w[...], u[...]
    s1 = fold(res * zz) * share
    s2 = fold(zz * ww) * share
    s3 = fold(ww * uu) * share
    anc = anchor[...]
    s4 = acc + share * fold(anc * (comp(sz, u, 0) * comp(sz, u, 0) + comp(sz, u, 1) * comp(sz, u, 1) + comp(sz, u, 2) * comp(sz, u, 2)))
    block = [jnp.sum(s, axis=0, keepdims=True) for s in (s1, s2, s3, s4)]
    block = jnp.concatenate(block + [jnp.zeros((SUB - 4, LANES), F32)], axis=0)
    for i in range(sz.n_blk * sz.n_rep):
        scal[i] = block


def final_kernel(sz, est, z, u, scal, out):
    along_z, along_u = step_factors(scal, sz.n_blk * sz.n_rep)
    new = est[...] + along_z * z[...] + along_u * u[...]
    for c in range(3):
        for r in range(sz.hi):
            row = c * sz.hi + r
            out[pl.ds(c, 1), pl.ds(r * LANES, LANES)] = new[row : row + 1]


def on_device(measured, rot_vector, confidence, first_local, second_local, edge_counts, start_angles, anchor):
    n_blk, n_rep = lax.axis_size("blk"), lax.axis_size("rep")
    sz = Sizes(n_blk, n_rep, first_local.shape[1], first_local.shape[2], start_angles.shape[1])
    half = n_blk // 2
    tile = (sz.tile_rows, LANES)
    f32 = lambda *shape: jax.ShapeDtypeStruct(shape, F32)
    vmem = pl.BlockSpec(memory_space=pltpu.VMEM)
    rows = sz.chunks * SUB
    far_shape = pltpu.VMEM((sz.tile_rows * SUB, LANES), F32)

    def sums_scratch(channels):
        return [
            pltpu.VMEM((channels * 2 * rows, LANES), F32),
        ]

    def call(kernel, name, outs, args, scratch_shapes=(), flops=20_000_000):
        return pl.pallas_call(
            kernel,
            name=name,
            out_shape=outs,
            in_specs=[vmem] * len(args),
            out_specs=[vmem] * len(outs),
            scratch_shapes=list(scratch_shapes),
            cost_estimate=pl.CostEstimate(flops=flops, bytes_accessed=flops // 10, transcendentals=0),
            compiler_params=pltpu.CompilerParams(vmem_limit_bytes=48 * 1024 * 1024),
        )(*args)

    groups = [[core + 2 * i for i in range(half)] for core in range(2)]
    swap = [(i, i ^ 1) for i in range(n_blk)]

    def all_tiles(copies):
        same = lax.all_to_all(copies, "blk", 0, 0, axis_index_groups=groups)
        return same, lax.ppermute(same, "blk", swap)

    def other_half(value):
        if n_rep == 2:
            return lax.ppermute(value, "rep", [(0, 1), (1, 0)])
        return lax.psum(value, "rep") - value

    def all_products(scal):
        return lax.all_to_all(scal, ("blk", "rep"), 0, 0)

    table_shape = f32(CHANNELS * rows, LANES)
    (opened,) = call(opening_kernel, "opening", [f32(SUB, LANES)], [], flops=20_000_000_000)
    table, est, anchor_rows, to_sibling = call(
        functools.partial(pack_kernel, sz),
        "pack",
        [table_shape, f32(*tile), f32(sz.hi, LANES), f32(4 * sz.edge_rows + sz.tile_rows, LANES)],
        [
            measured[:, 0], rot_vector[:, 0], confidence[:, 0], first_local[0], second_local[0], edge_counts.reshape(1, -1),
            start_angles, anchor.reshape(1, -1), opened,
        ],
    )
    sibling = lax.ppermute(to_sibling, "blk", swap)
    edges_shape = f32(4 * sz.edge_rows, LANES)
    *edges, tiles = call(
        functools.partial(load_kernel, sz),
        "load",
        [edges_shape, edges_shape, f32(2 * sz.tile_rows, LANES)],
        [table, est, sibling],
    )
    reach = ((1, 2), (3, 4))
    moves = lambda sign, by: [(i, (i + sign * 2 * by[i % 2] + 2 * n_blk) % n_blk) for i in range(n_blk)]
    edges = [lax.ppermute(value, "blk", moves(1, by)) for value, by in zip(edges, reach)]
    tiles = [lax.ppermute(tiles, "blk", moves(-1, by)) for by in reach]

    per_edge = f32(3 * rows, LANES)
    sums_shape = f32(9 * sz.hi, LANES)
    for sweep in range(PASSES):
        last = sweep + 1 == PASSES
        if sweep == 0:
            (relay,) = call(
                functools.partial(relay_kernel, sz),
                "relay",
                [f32(5 * sz.edge_rows + 4 * sz.tile_rows, LANES)],
                [table, *edges, *tiles],
            )
            relayed = lax.ppermute(relay, "blk", swap)
            gap_out, wc_out, sums = call(
                functools.partial(outgoing_misfit_kernel, sz),
                "misfit_outgoing",
                [per_edge, per_edge, sums_shape],
                [table, est, sibling, relayed, *tiles],
                [far_shape] + sums_scratch(9),
            )
            table_in, gap_in, wc_in, sums = call(
                functools.partial(incoming_misfit_kernel, sz),
                "misfit_incoming",
                [table_shape, per_edge, per_edge, sums_shape],
                [table, relayed, est, sums, *edges],
                sums_scratch(6),
            )
        else:
            wc_out, wc_in, sums, weights, est = call(
                functools.partial(next_misfit_kernel, sz),
                "misfit_next",
                [per_edge, per_edge, sums_shape, f32(sz.pairs, sz.slots), f32(*tile)],
                [table, table_in, gap_out, gap_in, z_out, z_in, u_out, u_in, est, z, u, scal],
                sums_scratch(9),
            )
        residual, inverse, z, z_copies = call(
            functools.partial(precond_kernel, sz),
            "precond",
            [f32(*tile), f32(6 * sz.hi, LANES), f32(*tile), f32(half, *tile)],
            [sums, other_half(sums), est, anchor_rows],
        )
        z_a, z_b = all_tiles(z_copies)
        near_out, near_in = call(
            functools.partial(near_kernel, sz), "near_z", [per_edge, per_edge], [table, table_in, z]
        )
        sums, *kept = call(
            functools.partial(image_kernel, sz, not last),
            "image",
            [f32(*tile)] + ([] if last else [per_edge, per_edge]),
            [table, table_in, wc_out, wc_in, z_a, z_b, near_out, near_in],
            [far_shape] + sums_scratch(3),
        )
        if not last:
            z_out, z_in = kept
        w, u, u_copies = call(
            functools.partial(second_precond_kernel, sz),
            "second_precond",
            [f32(*tile), f32(*tile), f32(half, *tile)],
            [sums, other_half(sums), z, anchor_rows, inverse],
        )
        u_a, u_b = all_tiles(u_copies)
        near = call(
            functools.partial(near_kernel, sz), "near_u", [per_edge] * (1 if last else 2), [table, table_in, u]
        )
        scal, *kept = call(
            functools.partial(products_kernel, sz, not last),
            "products",
            [f32(n_blk * n_rep, SUB, LANES)] + ([] if last else [per_edge, per_edge]),
            [table] + ([] if last else [table_in]) + [*near, wc_out, u_a, u_b, residual, z, w, u, anchor_rows],
            [far_shape],
        )
        if not last:
            u_out, u_in = kept
        scal = all_products(scal)
    (estimate,) = call(functools.partial(final_kernel, sz), "final", [f32(3, sz.cams)], [est, z, u, scal])
    return (estimate, weights[None])


def solution(mesh):
    return jax.shard_map(
        on_device,
        mesh=mesh,
        in_specs=(
            P(None, "blk", None, "rep"),
            P(None, "blk", None, "rep"),
            P(None, "blk", None, "rep"),
            P("blk", None, "rep"),
            P("blk", None, "rep"),
            P("blk", None, "rep"),
            P(None, "blk"),
            P("blk"),
        ),
        out_specs=(P(None, "blk"), P("blk", None, "rep")),
        check_vma=False,
    )
```

```python
import functools

import jax
import jax.numpy as jnp
from jax import lax
from jax.experimental import pallas as pl
from jax.experimental.pallas import tpu as pltpu
from jax.sharding import PartitionSpec as P

PASSES = 2
SOFTEN = 0.05
LANES = 128
SUB = 8
SPLITS = 2
BLOCK_ENTRIES = ((0, 0), (1, 1), (2, 2), (0, 1), (0, 2), (1, 2))
MEAS, ROT, CONF, FIRST, SECOND = 0, 3, 6, 9, 10
CHANNELS = 11
F32 = jnp.float32
BF16 = jnp.bfloat16


def rotation_entries(v):
    squared = v[0] * v[0] + v[1] * v[1] + v[2] * v[2]
    factor = 2.0 / (1.0 + squared)
    skewed = ((None, -v[2], v[1]), (v[2], None, -v[0]), (-v[1], v[0], None))
    rows = []
    for a in range(3):
        row = []
        for b in range(3):
            if a == b:
                row.append(1.0 + factor * (v[a] * v[a] - squared))
            else:
                row.append(factor * (skewed[a][b] + v[a] * v[b]))
        rows.append(row)
    return rows


def rotate(rows, y):
    return [rows[a][0] * y[0] + rows[a][1] * y[1] + rows[a][2] * y[2] for a in range(3)]


def rotate_back(rows, y):
    return [rows[0][a] * y[0] + rows[1][a] * y[1] + rows[2][a] * y[2] for a in range(3)]


class Sizes:
    def __init__(self, n_blk, n_rep, pairs, slots, cams):
        self.n_blk, self.n_rep = n_blk, n_rep
        self.pairs, self.slots, self.cams = pairs, slots, cams
        self.hi = cams // LANES
        self.tile_rows = 3 * self.hi
        self.chunks = slots // LANES
        self.edge_rows = CHANNELS * self.chunks
        assert pairs == SUB and slots % LANES == 0 and cams % (LANES * SUB) == 0 and n_blk % 2 == 0


def block_at(sz, row, c):
    return pl.ds((row * sz.chunks + c) * SUB, SUB)


def chunk(sz, ref, row, c):
    return ref[block_at(sz, row, c), :]


def gather3(sz, source, index):
    hi = lax.shift_right_logical(index, 7)
    lo = lax.bitwise_and(index, LANES - 1)
    out = [None] * 3
    for r in range(sz.hi):
        mask = hi == r
        for c in range(3):
            got = jnp.take_along_axis(source(c, r), lo, axis=1, mode="promise_in_bounds")
            out[c] = got if r == 0 else jnp.where(mask, got, out[c])
    return out


def far_source(sz, far):
    return lambda c, r: far[pl.ds((c * sz.hi + r) * SUB, SUB), :]


def own_source(sz, own):
    return lambda c, r: jnp.broadcast_to(own[pl.ds(c * sz.hi + r, 1), :], (SUB, LANES))


def build_far(sz, far, tile_at, b, sign):
    for k in range(sz.pairs):
        t = lax.rem(b + (sign * k + sz.n_blk), sz.n_blk)
        far[pl.ds(k, sz.tile_rows, stride=SUB), :] = tile_at(k % 2, lax.div(t, 2))


def store_split(sz, vals, ch, c, value):
    high = value.astype(BF16).astype(F32)
    vals[block_at(sz, 2 * ch, c), :] = high
    vals[block_at(sz, 2 * ch + 1, c), :] = value - high


def scatter(sz, channels, vals, index_ref, index_row):
    lane_iota = lax.broadcasted_iota(jnp.int32, (LANES, LANES), 0).astype(F32).astype(BF16)
    row_iota = lax.rem(lax.broadcasted_iota(jnp.int32, (SPLITS * SUB, LANES), 0), SUB).astype(F32).astype(BF16)
    groups = sz.hi // SUB
    one, zero = jnp.ones((), BF16), jnp.zeros((), BF16)
    total = None
    for c in range(sz.chunks):
        index = chunk(sz, index_ref, index_row, c).astype(jnp.int32)
        lows = lax.bitwise_and(index, LANES - 1).astype(F32)
        highs = lax.shift_right_logical(index, 7).astype(F32)
        for pair in range(0, sz.pairs, 2):
            lefts, rights = [], []
            for k in (pair, pair + 1):
                lo = jnp.broadcast_to(lows[k : k + 1], (LANES, LANES)).astype(BF16)
                hi = jnp.broadcast_to(highs[k : k + 1], (SPLITS * SUB, LANES)).astype(BF16)
                rights.append(jnp.where(lane_iota == lo, one, zero))
                masks = [row_iota + float(SUB * g) == hi for g in range(groups)]
                blocks = []
                for ch in range(channels):
                    both = []
                    for part in range(SPLITS):
                        row = vals[pl.ds(((2 * ch + part) * sz.chunks + c) * SUB + k, 1), :]
                        both.append(jnp.broadcast_to(row, (SUB, LANES)))
                    both = jnp.concatenate(both, axis=0).astype(BF16)
                    blocks += [jnp.where(mask, both, zero) for mask in masks]
                lefts.append(jnp.concatenate(blocks, axis=0))
            product = lax.dot_general(
                jnp.concatenate(lefts, axis=1),
                jnp.concatenate(rights, axis=1),
                (((1,), (1,)), ((), ())),
                preferred_element_type=F32,
            )
            total = product if total is None else total + product
    total = total.reshape(channels * groups, SPLITS, SUB, LANES)
    return (total[:, 0] + total[:, 1]).reshape(channels * sz.hi, LANES)


def opening_kernel(opened):
    opened[...] = jnp.zeros_like(opened)


def pack_kernel(sz, meas, rot, conf, first, second, counts, start, anchor, opened, table, est, anchor_out, swap):
    b = lax.axis_index("blk")
    for c in range(3):
        for r in range(sz.hi):
            est[pl.ds(c * sz.hi + r, 1), :] = start[pl.ds(c, 1), pl.ds(r * LANES, LANES)]
    for r in range(sz.hi):
        anchor_out[pl.ds(r, 1), :] = anchor[:, pl.ds(r * LANES, LANES)]
    across = lax.broadcasted_iota(jnp.int32, (sz.pairs, sz.pairs), 0)
    along = lax.broadcasted_iota(jnp.int32, (sz.pairs, sz.pairs), 1)
    spread = jnp.broadcast_to(counts[...], (sz.pairs, sz.pairs))
    limit = jnp.sum(jnp.where(across == along, spread, 0), axis=1, keepdims=True)
    for c in range(sz.chunks):
        lanes = pl.ds(c * LANES, LANES)
        slot = lax.broadcasted_iota(jnp.int32, (sz.pairs, LANES), 1) + c * LANES
        live = slot < limit
        index = first[:, lanes]
        turned = rotate(rotation_entries([rot[i, :, lanes] for i in range(3)]), gather3(sz, own_source(sz, est), index))
        for i in range(3):
            table[block_at(sz, MEAS + i, c), :] = meas[i, :, lanes] + turned[i]
            table[block_at(sz, ROT + i, c), :] = rot[i, :, lanes]
            table[block_at(sz, CONF + i, c), :] = jnp.where(live, conf[i, :, lanes], 0.0)
        table[block_at(sz, FIRST, c), :] = index.astype(F32)
        table[block_at(sz, SECOND, c), :] = second[:, lanes].astype(F32)
    odd = lax.rem(b, 2)
    count = sz.edge_rows
    for j, (from_odd, from_even) in enumerate(((1, 4), (2, 5), (5, 4), (6, 5))):
        k = from_even + odd * (from_odd - from_even)
        swap[pl.ds(j * count, count), :] = table[pl.ds(k, count, stride=SUB), :]
    swap[pl.ds(4 * count, sz.tile_rows), :] = est[...]


def load_kernel(sz, table, est, sibling, near_edges, far_edges, tiles):
    count = sz.edge_rows
    even = lax.rem(lax.axis_index("blk"), 2) == 0
    own = lambda k: table[pl.ds(k, count, stride=SUB), :]
    other = lambda j: sibling[pl.ds(j * count, count), :]
    for j, (if_even, if_odd) in enumerate(((own(2), other(0)), (own(3), other(1)), (other(0), own(3)), (other(1), own(4)))):
        near_edges[pl.ds(j * count, count), :] = jnp.where(even, if_even, if_odd)
    for j, (if_even, if_odd) in enumerate(((own(6), other(0)), (own(7), other(1)), (other(2), own(7)), (other(3), own(7)))):
        far_edges[pl.ds(j * count, count), :] = jnp.where(even, if_even, if_odd)
    mine, theirs = est[...], sibling[pl.ds(4 * count, sz.tile_rows), :]
    tiles[pl.ds(0, sz.tile_rows), :] = jnp.where(even, mine, theirs)
    tiles[pl.ds(sz.tile_rows, sz.tile_rows), :] = jnp.where(even, theirs, mine)


def relay_kernel(sz, table, near_edges, far_edges, after, relay):
    count = sz.edge_rows
    even = lax.rem(lax.axis_index("blk"), 2) == 0
    near = lambda j: near_edges[pl.ds(j * count, count), :]
    far = lambda j: far_edges[pl.ds(j * count, count), :]
    first = table[pl.ds(1, count, stride=SUB), :]
    for j, (if_even, if_odd) in enumerate(((first, near(2)), (near(3), near(0)), (near(1), far(2)), (far(3), far(2)), (far(1), far(2)))):
        relay[pl.ds(j * count, count), :] = jnp.where(even, if_even, if_odd)


def relay_tiles_kernel(sz, near_tiles, far_tiles, relay):
    relay[pl.ds(0, 2 * sz.tile_rows), :] = near_tiles[...]
    relay[pl.ds(2 * sz.tile_rows, 2 * sz.tile_rows), :] = far_tiles[...]


def weights_kernel(sz, rows, out):
    for c in range(sz.chunks):
        out[:, pl.ds(c * LANES, LANES)] = rows[pl.ds(c * SUB, SUB), :]


def step_factors(scal, n):
    total = scal[0]
    for i in range(1, n):
        total = total + scal[i]
    s = [jnp.sum(total[i : i + 1, :], axis=1, keepdims=True) for i in range(4)]
    alpha0 = s[0] / s[1]
    rz1 = alpha0 * alpha0 * s[2] - s[0]
    onward = 1.0 + rz1 / s[0]
    curve = onward * onward * s[1] - 2.0 * onward * alpha0 * s[2] + alpha0 * alpha0 * s[3]
    alpha1 = rz1 / curve
    return alpha0 + alpha1 * onward, -alpha1 * alpha0


def near_kernel(sz, table, table_in, own, *near):
    for incoming in range(len(near)):
        edges, channel = (table_in, SECOND) if incoming else (table, FIRST)
        for c in range(sz.chunks):
            index = chunk(sz, edges, channel, c).astype(jnp.int32)
            put3(sz, near[incoming], c, gather3(sz, own_source(sz, own), index))


def gathered_change(sz, edges, far, near, incoming, c, rows):
    index = chunk(sz, edges, FIRST if incoming else SECOND, c).astype(jnp.int32)
    away = gather3(sz, far_source(sz, far), index)
    here = get3(sz, near, c)
    if incoming:
        turned = rotate(rows, away)
        return [here[i] - turned[i] for i in range(3)]
    turned = rotate(rows, here)
    return [away[i] - turned[i] for i in range(3)]


def edge_rotation(sz, edges, c):
    return rotation_entries([chunk(sz, edges, ROT + i, c) for i in range(3)])


def put3(sz, ref, c, values):
    for i in range(3):
        ref[block_at(sz, i, c), :] = values[i]


def get3(sz, ref, c):
    return [chunk(sz, ref, i, c) for i in range(3)]


def misfit_sums(sz, incoming, misfit_of, edges, wc_ref, weights_ref, sums, vals):
    for c in range(sz.chunks):
        rows = None
        if not incoming:
            rows = edge_rotation(sz, edges, c)
        misfit = misfit_of(c, rows)
        conf = [chunk(sz, edges, CONF + i, c) for i in range(3)]
        energy = conf[0] * misfit[0] * misfit[0] + conf[1] * misfit[1] * misfit[1] + conf[2] * misfit[2] * misfit[2]
        weight = 1.0 / jnp.sqrt(energy + SOFTEN * SOFTEN)
        if weights_ref is not None:
            weights_ref[pl.ds(c * SUB, SUB), :] = jnp.where(conf[0] > 0.0, weight, 0.0)
        wc = [weight * conf[i] for i in range(3)]
        put3(sz, wc_ref, c, wc)
        push = [wc[i] * misfit[i] for i in range(3)]
        if incoming:
            for i in range(3):
                store_split(sz, vals, i, c, push[i])
                store_split(sz, vals, 3 + i, c, wc[i])
        else:
            back = rotate_back(rows, push)
            for i in range(3):
                store_split(sz, vals, i, c, -back[i])
            for n, (p, q) in enumerate(BLOCK_ENTRIES):
                entry = sum(rows[i][p] * wc[i] * rows[i][q] for i in range(3))
                store_split(sz, vals, 3 + n, c, entry)
    part = scatter(sz, 6 if incoming else 9, vals, edges, SECOND if incoming else FIRST)
    if incoming:
        cut = 6 * sz.hi
        sums[pl.ds(0, cut), :] = sums[pl.ds(0, cut), :] + part
    else:
        sums[...] = part


def outgoing_misfit_kernel(sz, table, own, sibling, relayed, near_tiles, far_tiles, gap, wc, sums, far, vals):
    even = lax.rem(lax.axis_index("blk"), 2) == 0
    tile = sz.tile_rows
    near = lambda j: near_tiles[pl.ds(j * tile, tile), :]
    away = lambda j: far_tiles[pl.ds(j * tile, tile), :]
    passed = lambda j: relayed[pl.ds(j * tile, tile), :]
    beside = sibling[pl.ds(4 * sz.edge_rows, tile), :]
    far[pl.ds(0, tile, stride=SUB), :] = own[...]
    for k, (if_even, if_odd) in enumerate(
        (
            (beside, passed(0)), (near(0), passed(1)), (near(1), near(0)), (passed(0), near(1)),
            (passed(1), passed(2)), (away(0), passed(3)), (away(1), away(0)),
        ),
        1,
    ):
        far[pl.ds(k, tile, stride=SUB), :] = jnp.where(even, if_even, if_odd)

    def misfit_of(c, rows):
        away = gather3(sz, far_source(sz, far), chunk(sz, table, SECOND, c).astype(jnp.int32))
        misfit = [chunk(sz, table, MEAS + i, c) - away[i] for i in range(3)]
        put3(sz, gap, c, misfit)
        return misfit

    misfit_sums(sz, False, misfit_of, table, wc, None, sums, vals)


def incoming_misfit_kernel(sz, table, relayed, own, sums_out, near_edges, far_edges, table_in, gap, wc, sums, vals):
    count = sz.edge_rows
    even = lax.rem(lax.axis_index("blk"), 2) == 0
    near = lambda j: near_edges[pl.ds(j * count, count), :]
    away = lambda j: far_edges[pl.ds(j * count, count), :]
    passed = lambda j: relayed[pl.ds(j * count, count), :]
    table_in[pl.ds(0, count, stride=SUB), :] = table[pl.ds(0, count, stride=SUB), :]
    for k, (if_even, if_odd) in enumerate(
        (
            (near(2), passed(0)), (near(0), passed(1)), (passed(0), passed(2)), (passed(1), near(3)),
            (away(2), near(1)), (away(0), passed(3)), (passed(2), passed(4)),
        ),
        1,
    ):
        table_in[pl.ds(k, count, stride=SUB), :] = jnp.where(even, if_even, if_odd)
    sums[...] = sums_out[...]

    def misfit_of(c, rows):
        here = gather3(sz, own_source(sz, own), chunk(sz, table_in, SECOND, c).astype(jnp.int32))
        misfit = [chunk(sz, table_in, MEAS + i, c) - here[i] for i in range(3)]
        put3(sz, gap, c, misfit)
        return misfit

    misfit_sums(sz, True, misfit_of, table_in, wc, None, sums, vals)


def next_misfit_kernel(
    sz, table, table_in, gap_out, gap_in, z_out, z_in, u_out, u_in, own, z, u, scal,
    wc_out, wc_in, sums, weights, own_new, vals,
):
    along_z, along_u = step_factors(scal, sz.n_blk * sz.n_rep)
    own_new[...] = own[...] + along_z * z[...] + along_u * u[...]
    for incoming in (False, True):
        edges, wc_ref = (table_in, wc_in) if incoming else (table, wc_out)
        old, by_z, by_u = (gap_in, z_in, u_in) if incoming else (gap_out, z_out, u_out)

        def misfit_of(c, rows):
            old3, z3, u3 = get3(sz, old, c), get3(sz, by_z, c), get3(sz, by_u, c)
            return [old3[i] - (along_z * z3[i] + along_u * u3[i]) for i in range(3)]

        misfit_sums(sz, incoming, misfit_of, edges, wc_ref, None if incoming else weights, sums, vals)


def apply_inverse(sz, inv, v):
    a00, a11, a22, a01, a02, a12 = inv
    return [
        a00 * v[0] + a01 * v[1] + a02 * v[2],
        a01 * v[0] + a11 * v[1] + a12 * v[2],
        a02 * v[0] + a12 * v[1] + a22 * v[2],
    ]


def comp(sz, ref, i):
    return ref[pl.ds(i * sz.hi, sz.hi), :]


def precond_kernel(sz, mine, other, est, anchor, residual, inverse, z, z_copies):
    total = mine[...] + other[...]
    part = lambda i: total[i * sz.hi : (i + 1) * sz.hi]
    anc = anchor[...]
    res = [part(i) - anc * comp(sz, est, i) for i in range(3)]
    p00, p11, p22 = [part(3 + i) + anc for i in range(3)]
    p01, p02, p12 = [part(6 + i) for i in range(3)]
    adj00 = p11 * p22 - p12 * p12
    adj01 = p02 * p12 - p01 * p22
    adj02 = p01 * p12 - p02 * p11
    adj11 = p00 * p22 - p02 * p02
    adj12 = p01 * p02 - p00 * p12
    adj22 = p00 * p11 - p01 * p01
    det = p00 * adj00 + p01 * adj01 + p02 * adj02
    inv = [a / det for a in (adj00, adj11, adj22, adj01, adj02, adj12)]
    scaled = apply_inverse(sz, inv, res)
    for i in range(3):
        residual[pl.ds(i * sz.hi, sz.hi), :] = res[i]
        z[pl.ds(i * sz.hi, sz.hi), :] = scaled[i]
    for i in range(6):
        inverse[pl.ds(i * sz.hi, sz.hi), :] = inv[i]
    for i in range(sz.n_blk // 2):
        z_copies[i] = z[...]


def image_kernel(sz, keep, table, table_in, wc_out, wc_in, z_a, z_b, near_out, near_in, sums, *refs):
    kept, (far, vals) = refs[:-2], refs[-2:]
    b = lax.axis_index("blk")

    def tile_at(parity, q):
        return (z_b if parity else z_a)[q]

    for incoming in (False, True):
        edges, wc_ref = (table_in, wc_in) if incoming else (table, wc_out)
        build_far(sz, far, tile_at, b, -1 if incoming else 1)
        for c in range(sz.chunks):
            rows = edge_rotation(sz, edges, c)
            change = gathered_change(sz, edges, far, near_in if incoming else near_out, incoming, c, rows)
            if keep:
                put3(sz, kept[int(incoming)], c, change)
            wc = get3(sz, wc_ref, c)
            push = [wc[i] * change[i] for i in range(3)]
            if incoming:
                for i in range(3):
                    store_split(sz, vals, i, c, push[i])
            else:
                back = rotate_back(rows, push)
                for i in range(3):
                    store_split(sz, vals, i, c, -back[i])
        part = scatter(sz, 3, vals, edges, SECOND if incoming else FIRST)
        if incoming:
            sums[...] = sums[...] + part
        else:
            sums[...] = part


def second_precond_kernel(sz, mine, other, z, anchor, inverse, w, u, u_copies):
    total = mine[...] + other[...]
    anc = anchor[...]
    image = [total[i * sz.hi : (i + 1) * sz.hi] + anc * comp(sz, z, i) for i in range(3)]
    scaled = apply_inverse(sz, [comp(sz, inverse, i) for i in range(6)], image)
    for i in range(3):
        w[pl.ds(i * sz.hi, sz.hi), :] = image[i]
        u[pl.ds(i * sz.hi, sz.hi), :] = scaled[i]
    for i in range(sz.n_blk // 2):
        u_copies[i] = u[...]


def fold(value):
    rows = value.shape[0]
    out = value[:SUB]
    for i in range(1, rows // SUB):
        out = out + value[i * SUB : (i + 1) * SUB]
    return out


def products_kernel(sz, keep, table, *refs):
    refs = list(refs)
    table_in = refs.pop(0) if keep else None
    near_out = refs.pop(0)
    near_in = refs.pop(0) if keep else None
    wc_out, u_a, u_b, residual, z, w, u, anchor, scal = refs[:9]
    kept, far = refs[9:-1], refs[-1]
    b = lax.axis_index("blk")

    def tile_at(parity, q):
        return (u_b if parity else u_a)[q]

    acc = jnp.zeros((SUB, LANES), F32)
    for incoming in (False, True) if keep else (False,):
        edges = table_in if incoming else table
        build_far(sz, far, tile_at, b, -1 if incoming else 1)
        for c in range(sz.chunks):
            near = near_in if incoming else near_out
            change = gathered_change(sz, edges, far, near, incoming, c, edge_rotation(sz, edges, c))
            if keep:
                put3(sz, kept[int(incoming)], c, change)
            if not incoming:
                wc = get3(sz, wc_out, c)
                for i in range(3):
                    acc = acc + wc[i] * change[i] * change[i]
    share = 1.0 / sz.n_rep
    res, zz, ww, uu = residual[...], z[...], w[...], u[...]
    s1 = fold(res * zz) * share
    s2 = fold(zz * ww) * share
    s3 = fold(ww * uu) * share
    anc = anchor[...]
    s4 = acc + share * fold(anc * (comp(sz, u, 0) * comp(sz, u, 0) + comp(sz, u, 1) * comp(sz, u, 1) + comp(sz, u, 2) * comp(sz, u, 2)))
    block = [jnp.sum(s, axis=0, keepdims=True) for s in (s1, s2, s3, s4)]
    block = jnp.concatenate(block + [jnp.zeros((SUB - 4, LANES), F32)], axis=0)
    for i in range(sz.n_blk * sz.n_rep):
        scal[i] = block


def final_kernel(sz, est, z, u, scal, out):
    along_z, along_u = step_factors(scal, sz.n_blk * sz.n_rep)
    new = est[...] + along_z * z[...] + along_u * u[...]
    for c in range(3):
        for r in range(sz.hi):
            row = c * sz.hi + r
            out[pl.ds(c, 1), pl.ds(r * LANES, LANES)] = new[row : row + 1]


def on_device(measured, rot_vector, confidence, first_local, second_local, edge_counts, start_angles, anchor):
    n_blk, n_rep = lax.axis_size("blk"), lax.axis_size("rep")
    sz = Sizes(n_blk, n_rep, first_local.shape[1], first_local.shape[2], start_angles.shape[1])
    half = n_blk // 2
    tile = (sz.tile_rows, LANES)
    f32 = lambda *shape: jax.ShapeDtypeStruct(shape, F32)
    vmem = pl.BlockSpec(memory_space=pltpu.VMEM)
    rows = sz.chunks * SUB
    far_shape = pltpu.VMEM((sz.tile_rows * SUB, LANES), F32)

    def sums_scratch(channels):
        return [
            pltpu.VMEM((channels * 2 * rows, LANES), F32),
        ]

    def call(kernel, name, outs, args, scratch_shapes=(), flops=20_000_000):
        return pl.pallas_call(
            kernel,
            name=name,
            out_shape=outs,
            in_specs=[vmem] * len(args),
            out_specs=[vmem] * len(outs),
            scratch_shapes=list(scratch_shapes),
            cost_estimate=pl.CostEstimate(flops=flops, bytes_accessed=flops // 10, transcendentals=0),
            compiler_params=pltpu.CompilerParams(vmem_limit_bytes=48 * 1024 * 1024),
        )(*args)

    groups = [[core + 2 * i for i in range(half)] for core in range(2)]
    swap = [(i, i ^ 1) for i in range(n_blk)]

    def all_tiles(copies):
        same = lax.all_to_all(copies, "blk", 0, 0, axis_index_groups=groups)
        return same, lax.ppermute(same, "blk", swap)

    def other_half(value):
        if n_rep == 2:
            return lax.ppermute(value, "rep", [(0, 1), (1, 0)])
        return lax.psum(value, "rep") - value

    def all_products(scal):
        return lax.all_to_all(scal, ("blk", "rep"), 0, 0)

    table_shape = f32(CHANNELS * rows, LANES)
    (opened,) = call(opening_kernel, "opening", [f32(SUB, LANES)], [], flops=20_000_000_000)
    table, est, anchor_rows, to_sibling = call(
        functools.partial(pack_kernel, sz),
        "pack",
        [table_shape, f32(*tile), f32(sz.hi, LANES), f32(4 * sz.edge_rows + sz.tile_rows, LANES)],
        [
            measured[:, 0], rot_vector[:, 0], confidence[:, 0], first_local[0], second_local[0], edge_counts.reshape(1, -1),
            start_angles, anchor.reshape(1, -1), opened,
        ],
    )
    sibling = lax.ppermute(to_sibling, "blk", swap)
    edges_shape = f32(4 * sz.edge_rows, LANES)
    *edges, tiles = call(
        functools.partial(load_kernel, sz),
        "load",
        [edges_shape, edges_shape, f32(2 * sz.tile_rows, LANES)],
        [table, est, sibling],
    )
    reach = ((1, 2), (3, 4))
    moves = lambda sign, by: [(i, (i + sign * 2 * by[i % 2] + 2 * n_blk) % n_blk) for i in range(n_blk)]
    edges = [lax.ppermute(value, "blk", moves(1, by)) for value, by in zip(edges, reach)]
    tiles = [lax.ppermute(tiles, "blk", moves(-1, by)) for by in reach]

    per_edge = f32(3 * rows, LANES)
    sums_shape = f32(9 * sz.hi, LANES)
    for sweep in range(PASSES):
        last = sweep + 1 == PASSES
        if sweep == 0:
            (relay,) = call(
                functools.partial(relay_tiles_kernel, sz), "relay_tiles", [f32(4 * sz.tile_rows, LANES)], tiles
            )
            relayed_tiles = lax.ppermute(relay, "blk", swap)
            gap_out, wc_out, sums = call(
                functools.partial(outgoing_misfit_kernel, sz),
                "misfit_outgoing",
                [per_edge, per_edge, sums_shape],
                [table, est, sibling, relayed_tiles, *tiles],
                [far_shape] + sums_scratch(9),
            )
            (relay,) = call(
                functools.partial(relay_kernel, sz), "relay_edges", [f32(5 * sz.edge_rows, LANES)], [table, *edges, wc_out]
            )
            relayed = lax.ppermute(relay, "blk", swap)
            table_in, gap_in, wc_in, sums = call(
                functools.partial(incoming_misfit_kernel, sz),
                "misfit_incoming",
                [table_shape, per_edge, per_edge, sums_shape],
                [table, relayed, est, sums, *edges],
                sums_scratch(6),
            )
        else:
            wc_out, wc_in, sums, weights, est = call(
                functools.partial(next_misfit_kernel, sz),
                "misfit_next",
                [per_edge, per_edge, sums_shape, f32(rows, LANES), f32(*tile)],
                [table, table_in, gap_out, gap_in, z_out, z_in, u_out, u_in, est, z, u, scal],
                sums_scratch(9),
            )
        residual, inverse, z, z_copies = call(
            functools.partial(precond_kernel, sz),
            "precond",
            [f32(*tile), f32(6 * sz.hi, LANES), f32(*tile), f32(half, *tile)],
            [sums, other_half(sums), est, anchor_rows],
        )
        z_a, z_b = all_tiles(z_copies)
        near_out, near_in = call(
            functools.partial(near_kernel, sz), "near_z", [per_edge, per_edge], [table, table_in, z]
        )
        sums, *kept = call(
            functools.partial(image_kernel, sz, not last),
            "image",
            [f32(*tile)] + ([] if last else [per_edge, per_edge]),
            [table, table_in, wc_out, wc_in, z_a, z_b, near_out, near_in],
            [far_shape] + sums_scratch(3),
        )
        if not last:
            z_out, z_in = kept
        w, u, u_copies = call(
            functools.partial(second_precond_kernel, sz),
            "second_precond",
            [f32(*tile), f32(*tile), f32(half, *tile)],
            [sums, other_half(sums), z, anchor_rows, inverse],
        )
        u_a, u_b = all_tiles(u_copies)
        near = call(
            functools.partial(near_kernel, sz), "near_u", [per_edge] * (1 if last else 2), [table, table_in, u]
        )
        scal, *kept = call(
            functools.partial(products_kernel, sz, not last),
            "products",
            [f32(n_blk * n_rep, SUB, LANES)] + ([] if last else [per_edge, per_edge]),
            [table] + ([] if last else [table_in]) + [*near, wc_out, u_a, u_b, residual, z, w, u, anchor_rows],
            [far_shape],
        )
        if not last:
            u_out, u_in = kept
        scal = all_products(scal)
    (estimate,) = call(functools.partial(final_kernel, sz), "final", [f32(3, sz.cams)], [est, z, u, scal])
    (weights,) = call(functools.partial(weights_kernel, sz), "weights", [f32(sz.pairs, sz.slots)], [weights])
    return (estimate, weights[None])


def solution(mesh):
    return jax.shard_map(
        on_device,
        mesh=mesh,
        in_specs=(
            P(None, "blk", None, "rep"),
            P(None, "blk", None, "rep"),
            P(None, "blk", None, "rep"),
            P("blk", None, "rep"),
            P("blk", None, "rep"),
            P("blk", None, "rep"),
            P(None, "blk"),
            P("blk"),
        ),
        out_specs=(P(None, "blk"), P("blk", None, "rep")),
        check_vma=False,
    )
```

```python
import functools

import jax
import jax.numpy as jnp
from jax import lax
from jax.experimental import pallas as pl
from jax.experimental.pallas import tpu as pltpu
from jax.sharding import PartitionSpec as P


PASSES = 2
SOFTEN = 0.05
LANES = 128
SUB = 8
SPLITS = 2
BLOCK_ENTRIES = ((0, 0), (1, 1), (2, 2), (0, 1), (0, 2), (1, 2))
MEAS, ROT, CONF, FIRST, SECOND = 0, 3, 6, 9, 10
CHANNELS = 11
F32 = jnp.float32
BF16 = jnp.bfloat16


def rotation_entries(v):
    squared = v[0] * v[0] + v[1] * v[1] + v[2] * v[2]
    factor = 2.0 / (1.0 + squared)
    skewed = ((None, -v[2], v[1]), (v[2], None, -v[0]), (-v[1], v[0], None))
    rows = []
    for a in range(3):
        row = []
        for b in range(3):
            if a == b:
                row.append(1.0 + factor * (v[a] * v[a] - squared))
            else:
                row.append(factor * (skewed[a][b] + v[a] * v[b]))
        rows.append(row)
    return rows


def rotate(rows, y):
    return [rows[a][0] * y[0] + rows[a][1] * y[1] + rows[a][2] * y[2] for a in range(3)]


def rotate_back(rows, y):
    return [rows[0][a] * y[0] + rows[1][a] * y[1] + rows[2][a] * y[2] for a in range(3)]


class Sizes:
    def __init__(self, n_blk, n_rep, pairs, slots, cams):
        self.n_blk, self.n_rep = n_blk, n_rep
        self.pairs, self.slots, self.cams = pairs, slots, cams
        self.hi = cams // LANES
        self.tile_rows = 3 * self.hi
        self.chunks = slots // LANES
        self.edge_rows = CHANNELS * self.chunks
        assert pairs == SUB and slots % LANES == 0 and cams % (LANES * SUB) == 0 and n_blk % 2 == 0


def block_at(sz, row, c):
    return pl.ds((row * sz.chunks + c) * SUB, SUB)


def chunk(sz, ref, row, c):
    return ref[block_at(sz, row, c), :]


def gather3(sz, source, index):
    hi = lax.shift_right_logical(index, 7)
    lo = lax.bitwise_and(index, LANES - 1)
    out = [None] * 3
    for r in range(sz.hi):
        mask = hi == r
        for c in range(3):
            got = jnp.take_along_axis(source(c, r), lo, axis=1, mode="promise_in_bounds")
            out[c] = got if r == 0 else jnp.where(mask, got, out[c])
    return out


def far_source(sz, far):
    return lambda c, r: far[pl.ds((c * sz.hi + r) * SUB, SUB), :]


def own_source(sz, own):
    return lambda c, r: jnp.broadcast_to(own[pl.ds(c * sz.hi + r, 1), :], (SUB, LANES))


def build_far(sz, far, tile_at, b, sign):
    for k in range(sz.pairs):
        t = lax.rem(b + (sign * k + sz.n_blk), sz.n_blk)
        far[pl.ds(k, sz.tile_rows, stride=SUB), :] = tile_at(k % 2, lax.div(t, 2))


def store_split(sz, vals, ch, c, value):
    high = value.astype(BF16).astype(F32)
    vals[block_at(sz, 2 * ch, c), :] = high
    vals[block_at(sz, 2 * ch + 1, c), :] = value - high


def scatter(sz, channels, vals, index_ref, index_row):
    lane_iota = lax.broadcasted_iota(jnp.int32, (LANES, LANES), 0).astype(F32).astype(BF16)
    row_iota = lax.rem(lax.broadcasted_iota(jnp.int32, (SPLITS * SUB, LANES), 0), SUB).astype(F32).astype(BF16)
    groups = sz.hi // SUB
    one, zero = jnp.ones((), BF16), jnp.zeros((), BF16)
    total = None
    for c in range(sz.chunks):
        index = chunk(sz, index_ref, index_row, c).astype(jnp.int32)
        lows = lax.bitwise_and(index, LANES - 1).astype(F32)
        highs = lax.shift_right_logical(index, 7).astype(F32)
        for pair in range(0, sz.pairs, 2):
            lefts, rights = [], []
            for k in (pair, pair + 1):
                lo = jnp.broadcast_to(lows[k : k + 1], (LANES, LANES)).astype(BF16)
                hi = jnp.broadcast_to(highs[k : k + 1], (SPLITS * SUB, LANES)).astype(BF16)
                rights.append(jnp.where(lane_iota == lo, one, zero))
                masks = [row_iota + float(SUB * g) == hi for g in range(groups)]
                blocks = []
                for ch in range(channels):
                    both = []
                    for part in range(SPLITS):
                        row = vals[pl.ds(((2 * ch + part) * sz.chunks + c) * SUB + k, 1), :]
                        both.append(jnp.broadcast_to(row, (SUB, LANES)))
                    both = jnp.concatenate(both, axis=0).astype(BF16)
                    blocks += [jnp.where(mask, both, zero) for mask in masks]
                lefts.append(jnp.concatenate(blocks, axis=0))
            product = lax.dot_general(
                jnp.concatenate(lefts, axis=1),
                jnp.concatenate(rights, axis=1),
                (((1,), (1,)), ((), ())),
                preferred_element_type=F32,
            )
            total = product if total is None else total + product
    total = total.reshape(channels * groups, SPLITS, SUB, LANES)
    return (total[:, 0] + total[:, 1]).reshape(channels * sz.hi, LANES)


def opening_kernel(opened):
    opened[...] = jnp.zeros_like(opened)


def pack_kernel(sz, meas, rot, conf, first, second, counts, start, anchor, opened, table, est, anchor_out, swap):
    b = lax.axis_index("blk")
    for c in range(3):
        for r in range(sz.hi):
            est[pl.ds(c * sz.hi + r, 1), :] = start[pl.ds(c, 1), pl.ds(r * LANES, LANES)]
    for r in range(sz.hi):
        anchor_out[pl.ds(r, 1), :] = anchor[:, pl.ds(r * LANES, LANES)]
    across = lax.broadcasted_iota(jnp.int32, (sz.pairs, sz.pairs), 0)
    along = lax.broadcasted_iota(jnp.int32, (sz.pairs, sz.pairs), 1)
    spread = jnp.broadcast_to(counts[...], (sz.pairs, sz.pairs))
    limit = jnp.sum(jnp.where(across == along, spread, 0), axis=1, keepdims=True)
    for c in range(sz.chunks):
        lanes = pl.ds(c * LANES, LANES)
        slot = lax.broadcasted_iota(jnp.int32, (sz.pairs, LANES), 1) + c * LANES
        live = slot < limit
        index = first[:, lanes]
        turned = rotate(rotation_entries([rot[i, :, lanes] for i in range(3)]), gather3(sz, own_source(sz, est), index))
        for i in range(3):
            table[block_at(sz, MEAS + i, c), :] = meas[i, :, lanes] + turned[i]
            table[block_at(sz, ROT + i, c), :] = rot[i, :, lanes]
            table[block_at(sz, CONF + i, c), :] = jnp.where(live, conf[i, :, lanes], 0.0)
        table[block_at(sz, FIRST, c), :] = index.astype(F32)
        table[block_at(sz, SECOND, c), :] = second[:, lanes].astype(F32)
    odd = lax.rem(b, 2)
    count = sz.edge_rows
    for j, (from_odd, from_even) in enumerate(((1, 4), (2, 5))):
        k = from_even + odd * (from_odd - from_even)
        swap[pl.ds(j * count, count), :] = table[pl.ds(k, count, stride=SUB), :]
    swap[pl.ds(2 * count, sz.tile_rows), :] = est[...]


def load_kernel(sz, table, est, sibling, near_edges, far_edges, last_edges, tiles):
    count = sz.edge_rows
    even = lax.rem(lax.axis_index("blk"), 2) == 0
    own = lambda k: table[pl.ds(k, count, stride=SUB), :]
    other = lambda j: sibling[pl.ds(j * count, count), :]
    for j, (if_even, if_odd) in enumerate(((own(2), other(0)), (own(3), other(1)), (other(0), own(3)), (other(1), own(4)))):
        near_edges[pl.ds(j * count, count), :] = jnp.where(even, if_even, if_odd)
    for j, (if_even, if_odd) in enumerate(((own(6), own(5)), (own(7), own(6)))):
        far_edges[pl.ds(j * count, count), :] = jnp.where(even, if_even, if_odd)
    last_edges[...] = own(7)
    mine, theirs = est[...], sibling[pl.ds(2 * count, sz.tile_rows), :]
    tiles[pl.ds(0, sz.tile_rows), :] = jnp.where(even, mine, theirs)
    tiles[pl.ds(sz.tile_rows, sz.tile_rows), :] = jnp.where(even, theirs, mine)


def relay_kernel(sz, table, near_edges, far_edges, last_edges, after, relay):
    count = sz.edge_rows
    even = lax.rem(lax.axis_index("blk"), 2) == 0
    near = lambda j: near_edges[pl.ds(j * count, count), :]
    far = lambda j: far_edges[pl.ds(j * count, count), :]
    first = table[pl.ds(1, count, stride=SUB), :]
    for j, (if_even, if_odd) in enumerate(((first, near(2)), (near(3), near(0)), (near(1), far(0)), (far(1), last_edges[...]))):
        relay[pl.ds(j * count, count), :] = jnp.where(even, if_even, if_odd)


def relay_tiles_kernel(sz, near_tiles, far_tiles, relay):
    relay[pl.ds(0, 2 * sz.tile_rows), :] = near_tiles[...]
    relay[pl.ds(2 * sz.tile_rows, 2 * sz.tile_rows), :] = far_tiles[...]


def step_factors(scal, n):
    total = scal[0]
    for i in range(1, n):
        total = total + scal[i]
    s = [jnp.sum(total[i : i + 1, :], axis=1, keepdims=True) for i in range(4)]
    alpha0 = s[0] / s[1]
    rz1 = alpha0 * alpha0 * s[2] - s[0]
    onward = 1.0 + rz1 / s[0]
    curve = onward * onward * s[1] - 2.0 * onward * alpha0 * s[2] + alpha0 * alpha0 * s[3]
    alpha1 = rz1 / curve
    return alpha0 + alpha1 * onward, -alpha1 * alpha0


def near_kernel(sz, table, table_in, own, *near):
    for incoming in range(len(near)):
        edges, channel = (table_in, SECOND) if incoming else (table, FIRST)
        for c in range(sz.chunks):
            index = chunk(sz, edges, channel, c).astype(jnp.int32)
            put3(sz, near[incoming], c, gather3(sz, own_source(sz, own), index))


def gathered_change(sz, edges, far, near, incoming, c, rows):
    index = chunk(sz, edges, FIRST if incoming else SECOND, c).astype(jnp.int32)
    away = gather3(sz, far_source(sz, far), index)
    here = get3(sz, near, c)
    if incoming:
        turned = rotate(rows, away)
        return [here[i] - turned[i] for i in range(3)]
    turned = rotate(rows, here)
    return [away[i] - turned[i] for i in range(3)]


def edge_rotation(sz, edges, c):
    return rotation_entries([chunk(sz, edges, ROT + i, c) for i in range(3)])


def put3(sz, ref, c, values):
    for i in range(3):
        ref[block_at(sz, i, c), :] = values[i]


def get3(sz, ref, c):
    return [chunk(sz, ref, i, c) for i in range(3)]


def misfit_sums(sz, incoming, misfit_of, edges, wc_ref, weights_ref, sums, vals):
    for c in range(sz.chunks):
        rows = None
        if not incoming:
            rows = edge_rotation(sz, edges, c)
        misfit = misfit_of(c, rows)
        conf = [chunk(sz, edges, CONF + i, c) for i in range(3)]
        energy = conf[0] * misfit[0] * misfit[0] + conf[1] * misfit[1] * misfit[1] + conf[2] * misfit[2] * misfit[2]
        weight = 1.0 / jnp.sqrt(energy + SOFTEN * SOFTEN)
        if weights_ref is not None:
            weights_ref[:, pl.ds(c * LANES, LANES)] = jnp.where(conf[0] > 0.0, weight, 0.0)
        wc = [weight * conf[i] for i in range(3)]
        put3(sz, wc_ref, c, wc)
        push = [wc[i] * misfit[i] for i in range(3)]
        if incoming:
            for i in range(3):
                store_split(sz, vals, i, c, push[i])
                store_split(sz, vals, 3 + i, c, wc[i])
        else:
            back = rotate_back(rows, push)
            for i in range(3):
                store_split(sz, vals, i, c, -back[i])
            for n, (p, q) in enumerate(BLOCK_ENTRIES):
                entry = sum(rows[i][p] * wc[i] * rows[i][q] for i in range(3))
                store_split(sz, vals, 3 + n, c, entry)
    part = scatter(sz, 6 if incoming else 9, vals, edges, SECOND if incoming else FIRST)
    if incoming:
        cut = 6 * sz.hi
        sums[pl.ds(0, cut), :] = sums[pl.ds(0, cut), :] + part
    else:
        sums[...] = part


def outgoing_misfit_kernel(sz, table, own, sibling, relayed, near_tiles, far_tiles, gap, wc, sums, far, vals):
    even = lax.rem(lax.axis_index("blk"), 2) == 0
    tile = sz.tile_rows
    near = lambda j: near_tiles[pl.ds(j * tile, tile), :]
    away = lambda j: far_tiles[pl.ds(j * tile, tile), :]
    passed = lambda j: relayed[pl.ds(j * tile, tile), :]
    beside = sibling[pl.ds(2 * sz.edge_rows, tile), :]
    far[pl.ds(0, tile, stride=SUB), :] = own[...]
    for k, (if_even, if_odd) in enumerate(
        (
            (beside, passed(0)), (near(0), passed(1)), (near(1), near(0)), (passed(0), near(1)),
            (passed(1), passed(2)), (away(0), passed(3)), (away(1), away(0)),
        ),
        1,
    ):
        far[pl.ds(k, tile, stride=SUB), :] = jnp.where(even, if_even, if_odd)

    def misfit_of(c, rows):
        away = gather3(sz, far_source(sz, far), chunk(sz, table, SECOND, c).astype(jnp.int32))
        misfit = [chunk(sz, table, MEAS + i, c) - away[i] for i in range(3)]
        put3(sz, gap, c, misfit)
        return misfit

    misfit_sums(sz, False, misfit_of, table, wc, None, sums, vals)


def incoming_misfit_kernel(sz, table, relayed, own, sums_out, near_edges, far_edges, table_in, gap, wc, sums, vals):
    count = sz.edge_rows
    even = lax.rem(lax.axis_index("blk"), 2) == 0
    near = lambda j: near_edges[pl.ds(j * count, count), :]
    away = lambda j: far_edges[pl.ds(j * count, count), :]
    passed = lambda j: relayed[pl.ds(j * count, count), :]
    table_in[pl.ds(0, count, stride=SUB), :] = table[pl.ds(0, count, stride=SUB), :]
    for k, (if_even, if_odd) in enumerate(
        (
            (near(2), passed(0)), (near(0), passed(1)), (passed(0), passed(2)), (passed(1), near(3)),
            (passed(2), near(1)), (away(0), away(1)), (passed(3), passed(3)),
        ),
        1,
    ):
        table_in[pl.ds(k, count, stride=SUB), :] = jnp.where(even, if_even, if_odd)
    sums[...] = sums_out[...]

    def misfit_of(c, rows):
        here = gather3(sz, own_source(sz, own), chunk(sz, table_in, SECOND, c).astype(jnp.int32))
        misfit = [chunk(sz, table_in, MEAS + i, c) - here[i] for i in range(3)]
        put3(sz, gap, c, misfit)
        return misfit

    misfit_sums(sz, True, misfit_of, table_in, wc, None, sums, vals)


def next_misfit_kernel(
    sz, table, table_in, gap_out, gap_in, z_out, z_in, u_out, u_in, own, z, u, scal,
    wc_out, wc_in, sums, weights, own_new, vals,
):
    along_z, along_u = step_factors(scal, sz.n_blk * sz.n_rep)
    own_new[...] = own[...] + along_z * z[...] + along_u * u[...]
    for incoming in (False, True):
        edges, wc_ref = (table_in, wc_in) if incoming else (table, wc_out)
        old, by_z, by_u = (gap_in, z_in, u_in) if incoming else (gap_out, z_out, u_out)

        def misfit_of(c, rows):
            old3, z3, u3 = get3(sz, old, c), get3(sz, by_z, c), get3(sz, by_u, c)
            return [old3[i] - (along_z * z3[i] + along_u * u3[i]) for i in range(3)]

        misfit_sums(sz, incoming, misfit_of, edges, wc_ref, None if incoming else weights, sums, vals)


def apply_inverse(inv, v):
    a00, a11, a22, a01, a02, a12 = inv
    return [
        a00 * v[0] + a01 * v[1] + a02 * v[2],
        a01 * v[0] + a11 * v[1] + a12 * v[2],
        a02 * v[0] + a12 * v[1] + a22 * v[2],
    ]


def comp(sz, ref, i):
    return ref[pl.ds(i * sz.hi, sz.hi), :]


def precond_kernel(sz, mine, other, est, anchor, residual, inverse, z, z_copies):
    total = mine[...] + other[...]
    part = lambda i: total[i * sz.hi : (i + 1) * sz.hi]
    anc = anchor[...]
    res = [part(i) - anc * comp(sz, est, i) for i in range(3)]
    p00, p11, p22 = [part(3 + i) + anc for i in range(3)]
    p01, p02, p12 = [part(6 + i) for i in range(3)]
    adj00 = p11 * p22 - p12 * p12
    adj01 = p02 * p12 - p01 * p22
    adj02 = p01 * p12 - p02 * p11
    adj11 = p00 * p22 - p02 * p02
    adj12 = p01 * p02 - p00 * p12
    adj22 = p00 * p11 - p01 * p01
    det = p00 * adj00 + p01 * adj01 + p02 * adj02
    inv = [a / det for a in (adj00, adj11, adj22, adj01, adj02, adj12)]
    scaled = apply_inverse(inv, res)
    for i in range(3):
        residual[pl.ds(i * sz.hi, sz.hi), :] = res[i]
        z[pl.ds(i * sz.hi, sz.hi), :] = scaled[i]
    for i in range(6):
        inverse[pl.ds(i * sz.hi, sz.hi), :] = inv[i]
    for i in range(sz.n_blk // 2):
        z_copies[i] = z[...]


def image_kernel(sz, keep, table, table_in, wc_out, wc_in, z_a, z_b, near_out, near_in, sums, *refs):
    kept, (far, vals) = refs[:-2], refs[-2:]
    b = lax.axis_index("blk")

    def tile_at(parity, q):
        return (z_b if parity else z_a)[q]

    for incoming in (False, True):
        edges, wc_ref = (table_in, wc_in) if incoming else (table, wc_out)
        build_far(sz, far, tile_at, b, -1 if incoming else 1)
        for c in range(sz.chunks):
            rows = edge_rotation(sz, edges, c)
            change = gathered_change(sz, edges, far, near_in if incoming else near_out, incoming, c, rows)
            if keep:
                put3(sz, kept[int(incoming)], c, change)
            wc = get3(sz, wc_ref, c)
            push = [wc[i] * change[i] for i in range(3)]
            if incoming:
                for i in range(3):
                    store_split(sz, vals, i, c, push[i])
            else:
                back = rotate_back(rows, push)
                for i in range(3):
                    store_split(sz, vals, i, c, -back[i])
        part = scatter(sz, 3, vals, edges, SECOND if incoming else FIRST)
        if incoming:
            sums[...] = sums[...] + part
        else:
            sums[...] = part


def second_precond_kernel(sz, mine, other, z, anchor, inverse, w, u, u_copies):
    total = mine[...] + other[...]
    anc = anchor[...]
    image = [total[i * sz.hi : (i + 1) * sz.hi] + anc * comp(sz, z, i) for i in range(3)]
    scaled = apply_inverse([comp(sz, inverse, i) for i in range(6)], image)
    for i in range(3):
        w[pl.ds(i * sz.hi, sz.hi), :] = image[i]
        u[pl.ds(i * sz.hi, sz.hi), :] = scaled[i]
    for i in range(sz.n_blk // 2):
        u_copies[i] = u[...]


def fold(value):
    rows = value.shape[0]
    out = value[:SUB]
    for i in range(1, rows // SUB):
        out = out + value[i * SUB : (i + 1) * SUB]
    return out


def products_kernel(sz, keep, table, *refs):
    refs = list(refs)
    table_in = refs.pop(0) if keep else None
    near_out = refs.pop(0)
    near_in = refs.pop(0) if keep else None
    wc_out, u_a, u_b, residual, z, w, u, anchor, scal = refs[:9]
    kept, far = refs[9:-1], refs[-1]
    b = lax.axis_index("blk")

    def tile_at(parity, q):
        return (u_b if parity else u_a)[q]

    acc = jnp.zeros((SUB, LANES), F32)
    for incoming in (False, True) if keep else (False,):
        edges = table_in if incoming else table
        build_far(sz, far, tile_at, b, -1 if incoming else 1)
        for c in range(sz.chunks):
            near = near_in if incoming else near_out
            change = gathered_change(sz, edges, far, near, incoming, c, edge_rotation(sz, edges, c))
            if keep:
                put3(sz, kept[int(incoming)], c, change)
            if not incoming:
                wc = get3(sz, wc_out, c)
                for i in range(3):
                    acc = acc + wc[i] * change[i] * change[i]
    share = 1.0 / sz.n_rep
    res, zz, ww, uu = residual[...], z[...], w[...], u[...]
    s1 = fold(res * zz) * share
    s2 = fold(zz * ww) * share
    s3 = fold(ww * uu) * share
    anc = anchor[...]
    s4 = acc + share * fold(anc * (comp(sz, u, 0) * comp(sz, u, 0) + comp(sz, u, 1) * comp(sz, u, 1) + comp(sz, u, 2) * comp(sz, u, 2)))
    block = [jnp.sum(s, axis=0, keepdims=True) for s in (s1, s2, s3, s4)]
    block = jnp.concatenate(block + [jnp.zeros((SUB - 4, LANES), F32)], axis=0)
    for i in range(sz.n_blk * sz.n_rep):
        scal[i] = block


def final_kernel(sz, est, z, u, scal, out):
    along_z, along_u = step_factors(scal, sz.n_blk * sz.n_rep)
    new = est[...] + along_z * z[...] + along_u * u[...]
    for c in range(3):
        for r in range(sz.hi):
            row = c * sz.hi + r
            out[pl.ds(c, 1), pl.ds(r * LANES, LANES)] = new[row : row + 1]


def on_device(measured, rot_vector, confidence, first_local, second_local, edge_counts, start_angles, anchor):
    n_blk, n_rep = lax.axis_size("blk"), lax.axis_size("rep")
    sz = Sizes(n_blk, n_rep, first_local.shape[1], first_local.shape[2], start_angles.shape[1])
    half = n_blk // 2
    tile = (sz.tile_rows, LANES)
    f32 = lambda *shape: jax.ShapeDtypeStruct(shape, F32)
    vmem = pl.BlockSpec(memory_space=pltpu.VMEM)
    rows = sz.chunks * SUB
    far_shape = pltpu.VMEM((sz.tile_rows * SUB, LANES), F32)

    def sums_scratch(channels):
        return [
            pltpu.VMEM((channels * 2 * rows, LANES), F32),
        ]

    def call(kernel, outs, args, scratch_shapes=(), flops=20_000_000):
        return pl.pallas_call(
            kernel,
            out_shape=outs,
            in_specs=[vmem] * len(args),
            out_specs=[vmem] * len(outs),
            scratch_shapes=list(scratch_shapes),
            cost_estimate=pl.CostEstimate(flops=flops, bytes_accessed=flops // 10, transcendentals=0),
            compiler_params=pltpu.CompilerParams(vmem_limit_bytes=48 * 1024 * 1024),
        )(*args)

    groups = [[core + 2 * i for i in range(half)] for core in range(2)]
    swap = [(i, i ^ 1) for i in range(n_blk)]

    def all_tiles(copies):
        same = lax.all_to_all(copies, "blk", 0, 0, axis_index_groups=groups)
        return same, lax.ppermute(same, "blk", swap)

    def other_half(value):
        if n_rep == 2:
            return lax.ppermute(value, "rep", [(0, 1), (1, 0)])
        return lax.psum(value, "rep") - value

    def all_products(scal):
        return lax.all_to_all(scal, ("blk", "rep"), 0, 0)

    table_shape = f32(CHANNELS * rows, LANES)
    (opened,) = call(opening_kernel, [f32(SUB, LANES)], [], flops=20_000_000_000)
    table, est, anchor_rows, to_sibling = call(
        functools.partial(pack_kernel, sz),
        [table_shape, f32(*tile), f32(sz.hi, LANES), f32(2 * sz.edge_rows + sz.tile_rows, LANES)],
        [
            measured[:, 0], rot_vector[:, 0], confidence[:, 0], first_local[0], second_local[0], edge_counts.reshape(1, -1),
            start_angles, anchor.reshape(1, -1), opened,
        ],
    )
    sibling = lax.ppermute(to_sibling, "blk", swap)
    *messages, tiles = call(
        functools.partial(load_kernel, sz),
        [f32(n * sz.edge_rows, LANES) for n in (4, 2, 1)] + [f32(2 * sz.tile_rows, LANES)],
        [table, est, sibling],
    )

    def moved(value, sign, even_by, odd_by):
        by = (even_by, odd_by)
        pairs = [(i, (i + sign * 2 * by[i % 2] + 2 * n_blk) % n_blk) for i in range(n_blk) if by[i % 2]]
        return lax.ppermute(value, "blk", pairs)

    *edges, last_edges = [moved(v, 1, *by) for v, by in zip(messages, ((1, 2), (3, 3), (0, 4)))]
    tiles = [moved(tiles, -1, *by) for by in ((1, 2), (3, 4))]

    per_edge = f32(3 * rows, LANES)
    sums_shape = f32(9 * sz.hi, LANES)
    for sweep in range(PASSES):
        last = sweep + 1 == PASSES
        if sweep == 0:
            (relay,) = call(functools.partial(relay_tiles_kernel, sz), [f32(4 * sz.tile_rows, LANES)], tiles)
            relayed_tiles = lax.ppermute(relay, "blk", swap)
            gap_out, wc_out, sums = call(
                functools.partial(outgoing_misfit_kernel, sz),
                [per_edge, per_edge, sums_shape],
                [table, est, sibling, relayed_tiles, *tiles],
                [far_shape] + sums_scratch(9),
            )
            (relay,) = call(
                functools.partial(relay_kernel, sz), [f32(4 * sz.edge_rows, LANES)], [table, *edges, last_edges, wc_out]
            )
            relayed = lax.ppermute(relay, "blk", swap)
            table_in, gap_in, wc_in, sums = call(
                functools.partial(incoming_misfit_kernel, sz),
                [table_shape, per_edge, per_edge, sums_shape],
                [table, relayed, est, sums, *edges],
                sums_scratch(6),
            )
        else:
            wc_out, wc_in, sums, weights, est = call(
                functools.partial(next_misfit_kernel, sz),
                [per_edge, per_edge, sums_shape, f32(sz.pairs, sz.slots), f32(*tile)],
                [table, table_in, gap_out, gap_in, z_out, z_in, u_out, u_in, est, z, u, scal],
                sums_scratch(9),
            )
        residual, inverse, z, z_copies = call(
            functools.partial(precond_kernel, sz),
            [f32(*tile), f32(6 * sz.hi, LANES), f32(*tile), f32(half, *tile)],
            [sums, other_half(sums), est, anchor_rows],
        )
        z_a, z_b = all_tiles(z_copies)
        near_out, near_in = call(functools.partial(near_kernel, sz), [per_edge, per_edge], [table, table_in, z])
        sums, *kept = call(
            functools.partial(image_kernel, sz, not last),
            [f32(*tile)] + ([] if last else [per_edge, per_edge]),
            [table, table_in, wc_out, wc_in, z_a, z_b, near_out, near_in],
            [far_shape] + sums_scratch(3),
        )
        if not last:
            z_out, z_in = kept
        w, u, u_copies = call(
            functools.partial(second_precond_kernel, sz),
            [f32(*tile), f32(*tile), f32(half, *tile)],
            [sums, other_half(sums), z, anchor_rows, inverse],
        )
        u_a, u_b = all_tiles(u_copies)
        near = call(functools.partial(near_kernel, sz), [per_edge] * (1 if last else 2), [table, table_in, u])
        scal, *kept = call(
            functools.partial(products_kernel, sz, not last),
            [f32(n_blk * n_rep, SUB, LANES)] + ([] if last else [per_edge, per_edge]),
            [table] + ([] if last else [table_in]) + [*near, wc_out, u_a, u_b, residual, z, w, u, anchor_rows],
            [far_shape],
        )
        if not last:
            u_out, u_in = kept
        scal = all_products(scal)
    (estimate,) = call(functools.partial(final_kernel, sz), [f32(3, sz.cams)], [est, z, u, scal])
    return (estimate, weights[None])


def solution(mesh):
    return jax.shard_map(
        on_device,
        mesh=mesh,
        in_specs=(
            P(None, "blk", None, "rep"),
            P(None, "blk", None, "rep"),
            P(None, "blk", None, "rep"),
            P("blk", None, "rep"),
            P("blk", None, "rep"),
            P("blk", None, "rep"),
            P(None, "blk"),
            P("blk"),
        ),
        out_specs=(P(None, "blk"), P("blk", None, "rep")),
        check_vma=False,
    )
```

```python
import functools

import jax
import jax.numpy as jnp
from jax import lax
from jax.experimental import pallas as pl
from jax.experimental.pallas import tpu as pltpu
from jax.sharding import PartitionSpec as P


PASSES = 2
SOFTEN = 0.05
LANES = 128
SUB = 8
SPLITS = 2
BLOCK_ENTRIES = ((0, 0), (1, 1), (2, 2), (0, 1), (0, 2), (1, 2))
MEAS, ROT, CONF, FIRST, SECOND = 0, 3, 6, 9, 10
CHANNELS = 11
F32 = jnp.float32
BF16 = jnp.bfloat16


def rotation_entries(v):
    squared = v[0] * v[0] + v[1] * v[1] + v[2] * v[2]
    factor = 2.0 / (1.0 + squared)
    skewed = ((None, -v[2], v[1]), (v[2], None, -v[0]), (-v[1], v[0], None))
    rows = []
    for a in range(3):
        row = []
        for b in range(3):
            if a == b:
                row.append(1.0 + factor * (v[a] * v[a] - squared))
            else:
                row.append(factor * (skewed[a][b] + v[a] * v[b]))
        rows.append(row)
    return rows


def rotate(rows, y):
    return [rows[a][0] * y[0] + rows[a][1] * y[1] + rows[a][2] * y[2] for a in range(3)]


def rotate_back(rows, y):
    return [rows[0][a] * y[0] + rows[1][a] * y[1] + rows[2][a] * y[2] for a in range(3)]


class Sizes:
    def __init__(self, n_blk, n_rep, pairs, slots, cams):
        self.n_blk, self.n_rep = n_blk, n_rep
        self.pairs, self.slots, self.cams = pairs, slots, cams
        self.hi = cams // LANES
        self.tile_rows = 3 * self.hi
        self.chunks = slots // LANES
        self.edge_rows = CHANNELS * self.chunks
        assert pairs == SUB and slots % LANES == 0 and cams % (LANES * SUB) == 0 and n_blk % 2 == 0


def block_at(sz, row, c):
    return pl.ds((row * sz.chunks + c) * SUB, SUB)


def chunk(sz, ref, row, c):
    return ref[block_at(sz, row, c), :]


def gather3(sz, source, index):
    hi = lax.shift_right_logical(index, 7)
    lo = lax.bitwise_and(index, LANES - 1)
    out = [None] * 3
    for r in range(sz.hi):
        mask = hi == r
        for c in range(3):
            got = jnp.take_along_axis(source(c, r), lo, axis=1, mode="promise_in_bounds")
            out[c] = got if r == 0 else jnp.where(mask, got, out[c])
    return out


def far_source(sz, far):
    return lambda c, r: far[pl.ds((c * sz.hi + r) * SUB, SUB), :]


def own_source(sz, own):
    return lambda c, r: jnp.broadcast_to(own[pl.ds(c * sz.hi + r, 1), :], (SUB, LANES))


def build_far(sz, far, tile_at, b, sign):
    for k in range(sz.pairs):
        t = lax.rem(b + (sign * k + sz.n_blk), sz.n_blk)
        far[pl.ds(k, sz.tile_rows, stride=SUB), :] = tile_at(k % 2, lax.div(t, 2))


def store_split(sz, vals, ch, c, value):
    high = value.astype(BF16).astype(F32)
    vals[block_at(sz, 2 * ch, c), :] = high
    vals[block_at(sz, 2 * ch + 1, c), :] = value - high


def scatter(sz, channels, vals, index_ref, index_row):
    lane_iota = lax.broadcasted_iota(jnp.int32, (LANES, LANES), 0).astype(F32).astype(BF16)
    row_iota = lax.rem(lax.broadcasted_iota(jnp.int32, (SPLITS * SUB, LANES), 0), SUB).astype(F32).astype(BF16)
    groups = sz.hi // SUB
    one, zero = jnp.ones((), BF16), jnp.zeros((), BF16)
    total = None
    for c in range(sz.chunks):
        index = chunk(sz, index_ref, index_row, c).astype(jnp.int32)
        lows = lax.bitwise_and(index, LANES - 1).astype(F32)
        highs = lax.shift_right_logical(index, 7).astype(F32)
        for pair in range(0, sz.pairs, 2):
            lefts, rights = [], []
            for k in (pair, pair + 1):
                lo = jnp.broadcast_to(lows[k : k + 1], (LANES, LANES)).astype(BF16)
                hi = jnp.broadcast_to(highs[k : k + 1], (SPLITS * SUB, LANES)).astype(BF16)
                rights.append(jnp.where(lane_iota == lo, one, zero))
                masks = [row_iota + float(SUB * g) == hi for g in range(groups)]
                blocks = []
                for ch in range(channels):
                    both = []
                    for part in range(SPLITS):
                        row = vals[pl.ds(((2 * ch + part) * sz.chunks + c) * SUB + k, 1), :]
                        both.append(jnp.broadcast_to(row, (SUB, LANES)))
                    both = jnp.concatenate(both, axis=0).astype(BF16)
                    blocks += [jnp.where(mask, both, zero) for mask in masks]
                lefts.append(jnp.concatenate(blocks, axis=0))
            product = lax.dot_general(
                jnp.concatenate(lefts, axis=1),
                jnp.concatenate(rights, axis=1),
                (((1,), (1,)), ((), ())),
                preferred_element_type=F32,
            )
            total = product if total is None else total + product
    total = total.reshape(channels * groups, SPLITS, SUB, LANES)
    return (total[:, 0] + total[:, 1]).reshape(channels * sz.hi, LANES)


def opening_kernel(opened):
    opened[...] = jnp.zeros_like(opened)


def pack_kernel(sz, meas, rot, conf, first, second, counts, start, anchor, opened, table, est, anchor_out, *sends):
    b = lax.axis_index("blk")
    for c in range(3):
        for r in range(sz.hi):
            est[pl.ds(c * sz.hi + r, 1), :] = start[pl.ds(c, 1), pl.ds(r * LANES, LANES)]
    for r in range(sz.hi):
        anchor_out[pl.ds(r, 1), :] = anchor[:, pl.ds(r * LANES, LANES)]
    across = lax.broadcasted_iota(jnp.int32, (sz.pairs, sz.pairs), 0)
    along = lax.broadcasted_iota(jnp.int32, (sz.pairs, sz.pairs), 1)
    spread = jnp.broadcast_to(counts[...], (sz.pairs, sz.pairs))
    limit = jnp.sum(jnp.where(across == along, spread, 0), axis=1, keepdims=True)
    for c in range(sz.chunks):
        lanes = pl.ds(c * LANES, LANES)
        slot = lax.broadcasted_iota(jnp.int32, (sz.pairs, LANES), 1) + c * LANES
        live = slot < limit
        index = first[:, lanes]
        turned = rotate(rotation_entries([rot[i, :, lanes] for i in range(3)]), gather3(sz, own_source(sz, est), index))
        for i in range(3):
            table[block_at(sz, MEAS + i, c), :] = meas[i, :, lanes] + turned[i]
            table[block_at(sz, ROT + i, c), :] = rot[i, :, lanes]
            table[block_at(sz, CONF + i, c), :] = jnp.where(live, conf[i, :, lanes], 0.0)
        table[block_at(sz, FIRST, c), :] = index.astype(F32)
        table[block_at(sz, SECOND, c), :] = second[:, lanes].astype(F32)
    odd = lax.rem(b, 2)
    count = sz.edge_rows
    for m in range(1, sz.pairs // 2):
        sends[m - 1][pl.ds(0, count), :] = table[pl.ds(2 * m, count, stride=SUB), :]
        sends[m - 1][pl.ds(count, count), :] = table[pl.ds(2 * m + 1 - 2 * odd, count, stride=SUB), :]
    sends[-1][...] = table[pl.ds(sz.pairs - 1, count, stride=SUB), :]

    @pl.when(odd == 0)
    def _():
        sends[-1][pl.ds(0, sz.tile_rows), :] = est[...]


def relay_kernel(sz, table, est, *refs):
    steps = sz.pairs // 2
    edges, tiles, mixed, relay = refs[: steps - 1], refs[steps - 1 : 2 * steps - 2], refs[-2], refs[-1]
    even_core = lax.rem(lax.axis_index("blk"), 2) == 0
    count = sz.edge_rows
    base = steps * count
    for j in range(steps):
        own = table[pl.ds(1, count, stride=SUB), :] if j == 0 else edges[j - 1][pl.ds(count, count), :]
        far = edges[j][pl.ds(count, count), :] if j + 1 < steps else mixed[...]
        relay[pl.ds(j * count, count), :] = jnp.where(even_core, own, far)
        own = est[...] if j == 0 else tiles[j - 1][...]
        far = tiles[j][...] if j + 1 < steps else mixed[pl.ds(0, sz.tile_rows), :]
        relay[pl.ds(base + j * sz.tile_rows, sz.tile_rows), :] = jnp.where(even_core, far, own)


def step_factors(scal, n):
    total = scal[0]
    for i in range(1, n):
        total = total + scal[i]
    s = [jnp.sum(total[i : i + 1, :], axis=1, keepdims=True) for i in range(4)]
    alpha0 = s[0] / s[1]
    rz1 = alpha0 * alpha0 * s[2] - s[0]
    onward = 1.0 + rz1 / s[0]
    curve = onward * onward * s[1] - 2.0 * onward * alpha0 * s[2] + alpha0 * alpha0 * s[3]
    alpha1 = rz1 / curve
    return alpha0 + alpha1 * onward, -alpha1 * alpha0


def near_kernel(sz, table, table_in, own, *near):
    for incoming in range(len(near)):
        edges, channel = (table_in, SECOND) if incoming else (table, FIRST)
        for c in range(sz.chunks):
            index = chunk(sz, edges, channel, c).astype(jnp.int32)
            put3(sz, near[incoming], c, gather3(sz, own_source(sz, own), index))


def near_and_weights_kernel(sz, table, table_in, own, rows, near_out, near_in, weights):
    for c in range(sz.chunks):
        weights[:, pl.ds(c * LANES, LANES)] = rows[pl.ds(c * SUB, SUB), :]
    near_kernel(sz, table, table_in, own, near_out, near_in)


def gathered_change(sz, edges, far, near, incoming, c, rows):
    index = chunk(sz, edges, FIRST if incoming else SECOND, c).astype(jnp.int32)
    away = gather3(sz, far_source(sz, far), index)
    here = get3(sz, near, c)
    if incoming:
        turned = rotate(rows, away)
        return [here[i] - turned[i] for i in range(3)]
    turned = rotate(rows, here)
    return [away[i] - turned[i] for i in range(3)]


def edge_rotation(sz, edges, c):
    return rotation_entries([chunk(sz, edges, ROT + i, c) for i in range(3)])


def put3(sz, ref, c, values):
    for i in range(3):
        ref[block_at(sz, i, c), :] = values[i]


def get3(sz, ref, c):
    return [chunk(sz, ref, i, c) for i in range(3)]


def misfit_sums(sz, incoming, misfit_of, edges, wc_ref, weights_ref, sums, vals):
    for c in range(sz.chunks):
        rows = None
        if not incoming:
            rows = edge_rotation(sz, edges, c)
        misfit = misfit_of(c, rows)
        conf = [chunk(sz, edges, CONF + i, c) for i in range(3)]
        energy = conf[0] * misfit[0] * misfit[0] + conf[1] * misfit[1] * misfit[1] + conf[2] * misfit[2] * misfit[2]
        weight = 1.0 / jnp.sqrt(energy + SOFTEN * SOFTEN)
        if weights_ref is not None:
            weights_ref[pl.ds(c * SUB, SUB), :] = jnp.where(conf[0] > 0.0, weight, 0.0)
        wc = [weight * conf[i] for i in range(3)]
        put3(sz, wc_ref, c, wc)
        push = [wc[i] * misfit[i] for i in range(3)]
        if incoming:
            for i in range(3):
                store_split(sz, vals, i, c, push[i])
                store_split(sz, vals, 3 + i, c, wc[i])
        else:
            back = rotate_back(rows, push)
            for i in range(3):
                store_split(sz, vals, i, c, -back[i])
            for n, (p, q) in enumerate(BLOCK_ENTRIES):
                entry = sum(rows[i][p] * wc[i] * rows[i][q] for i in range(3))
                store_split(sz, vals, 3 + n, c, entry)
    part = scatter(sz, 6 if incoming else 9, vals, edges, SECOND if incoming else FIRST)
    if incoming:
        cut = 6 * sz.hi
        sums[pl.ds(0, cut), :] = sums[pl.ds(0, cut), :] + part
    else:
        sums[...] = part


def outgoing_misfit_kernel(sz, table, own, relayed, *refs):
    steps = sz.pairs // 2
    tiles, (gap, wc, sums, far, vals) = refs[: steps - 1], refs[steps - 1 :]
    base = steps * sz.edge_rows
    for k in range(sz.pairs):
        if k == 0:
            block = own[...]
        elif k % 2:
            block = relayed[pl.ds(base + (k // 2) * sz.tile_rows, sz.tile_rows), :]
        else:
            block = tiles[k // 2 - 1][...]
        far[pl.ds(k, sz.tile_rows, stride=SUB), :] = block

    def misfit_of(c, rows):
        away = gather3(sz, far_source(sz, far), chunk(sz, table, SECOND, c).astype(jnp.int32))
        misfit = [chunk(sz, table, MEAS + i, c) - away[i] for i in range(3)]
        put3(sz, gap, c, misfit)
        return misfit

    misfit_sums(sz, False, misfit_of, table, wc, None, sums, vals)


def incoming_misfit_kernel(sz, table, relayed, own, sums_out, *refs):
    steps = sz.pairs // 2
    edges, (table_in, gap, wc, sums, vals) = refs[: steps - 1], refs[steps - 1 :]
    count = sz.edge_rows
    for k in range(sz.pairs):
        if k == 0:
            block = table[pl.ds(0, count, stride=SUB), :]
        elif k % 2:
            block = relayed[pl.ds((k // 2) * count, count), :]
        else:
            block = edges[k // 2 - 1][pl.ds(0, count), :]
        table_in[pl.ds(k, count, stride=SUB), :] = block
    sums[...] = sums_out[...]

    def misfit_of(c, rows):
        here = gather3(sz, own_source(sz, own), chunk(sz, table_in, SECOND, c).astype(jnp.int32))
        misfit = [chunk(sz, table_in, MEAS + i, c) - here[i] for i in range(3)]
        put3(sz, gap, c, misfit)
        return misfit

    misfit_sums(sz, True, misfit_of, table_in, wc, None, sums, vals)


def next_misfit_kernel(
    sz, table, table_in, gap_out, gap_in, z_out, z_in, u_out, u_in, own, z, u, scal,
    wc_out, wc_in, sums, weights, own_new, vals,
):
    along_z, along_u = step_factors(scal, sz.n_blk * sz.n_rep)
    own_new[...] = own[...] + along_z * z[...] + along_u * u[...]
    for incoming in (False, True):
        edges, wc_ref = (table_in, wc_in) if incoming else (table, wc_out)
        old, by_z, by_u = (gap_in, z_in, u_in) if incoming else (gap_out, z_out, u_out)

        def misfit_of(c, rows):
            old3, z3, u3 = get3(sz, old, c), get3(sz, by_z, c), get3(sz, by_u, c)
            return [old3[i] - (along_z * z3[i] + along_u * u3[i]) for i in range(3)]

        misfit_sums(sz, incoming, misfit_of, edges, wc_ref, None if incoming else weights, sums, vals)


def apply_inverse(inv, v):
    a00, a11, a22, a01, a02, a12 = inv
    return [
        a00 * v[0] + a01 * v[1] + a02 * v[2],
        a01 * v[0] + a11 * v[1] + a12 * v[2],
        a02 * v[0] + a12 * v[1] + a22 * v[2],
    ]


def comp(sz, ref, i):
    return ref[pl.ds(i * sz.hi, sz.hi), :]


def precond_kernel(sz, mine, other, est, anchor, residual, inverse, z, z_copies):
    total = mine[...] + other[...]
    part = lambda i: total[i * sz.hi : (i + 1) * sz.hi]
    anc = anchor[...]
    res = [part(i) - anc * comp(sz, est, i) for i in range(3)]
    p00, p11, p22 = [part(3 + i) + anc for i in range(3)]
    p01, p02, p12 = [part(6 + i) for i in range(3)]
    adj00 = p11 * p22 - p12 * p12
    adj01 = p02 * p12 - p01 * p22
    adj02 = p01 * p12 - p02 * p11
    adj11 = p00 * p22 - p02 * p02
    adj12 = p01 * p02 - p00 * p12
    adj22 = p00 * p11 - p01 * p01
    det = p00 * adj00 + p01 * adj01 + p02 * adj02
    inv = [a / det for a in (adj00, adj11, adj22, adj01, adj02, adj12)]
    scaled = apply_inverse(inv, res)
    for i in range(3):
        residual[pl.ds(i * sz.hi, sz.hi), :] = res[i]
        z[pl.ds(i * sz.hi, sz.hi), :] = scaled[i]
    for i in range(6):
        inverse[pl.ds(i * sz.hi, sz.hi), :] = inv[i]
    for i in range(sz.n_blk // 2):
        z_copies[i] = z[...]


def image_kernel(sz, keep, table, table_in, wc_out, wc_in, z_a, z_b, near_out, near_in, sums, *refs):
    kept, (far, vals) = refs[:-2], refs[-2:]
    b = lax.axis_index("blk")

    def tile_at(parity, q):
        return (z_b if parity else z_a)[q]

    for incoming in (False, True):
        edges, wc_ref = (table_in, wc_in) if incoming else (table, wc_out)
        build_far(sz, far, tile_at, b, -1 if incoming else 1)
        for c in range(sz.chunks):
            rows = edge_rotation(sz, edges, c)
            change = gathered_change(sz, edges, far, near_in if incoming else near_out, incoming, c, rows)
            if keep:
                put3(sz, kept[int(incoming)], c, change)
            wc = get3(sz, wc_ref, c)
            push = [wc[i] * change[i] for i in range(3)]
            if incoming:
                for i in range(3):
                    store_split(sz, vals, i, c, push[i])
            else:
                back = rotate_back(rows, push)
                for i in range(3):
                    store_split(sz, vals, i, c, -back[i])
        part = scatter(sz, 3, vals, edges, SECOND if incoming else FIRST)
        if incoming:
            sums[...] = sums[...] + part
        else:
            sums[...] = part


def second_precond_kernel(sz, mine, other, z, anchor, inverse, w, u, u_copies):
    total = mine[...] + other[...]
    anc = anchor[...]
    image = [total[i * sz.hi : (i + 1) * sz.hi] + anc * comp(sz, z, i) for i in range(3)]
    scaled = apply_inverse([comp(sz, inverse, i) for i in range(6)], image)
    for i in range(3):
        w[pl.ds(i * sz.hi, sz.hi), :] = image[i]
        u[pl.ds(i * sz.hi, sz.hi), :] = scaled[i]
    for i in range(sz.n_blk // 2):
        u_copies[i] = u[...]


def fold(value):
    rows = value.shape[0]
    out = value[:SUB]
    for i in range(1, rows // SUB):
        out = out + value[i * SUB : (i + 1) * SUB]
    return out


def products_kernel(sz, keep, table, *refs):
    refs = list(refs)
    table_in = refs.pop(0) if keep else None
    near_out = refs.pop(0)
    near_in = refs.pop(0) if keep else None
    wc_out, u_a, u_b, residual, z, w, u, anchor, scal = refs[:9]
    kept, far = refs[9:-1], refs[-1]
    b = lax.axis_index("blk")

    def tile_at(parity, q):
        return (u_b if parity else u_a)[q]

    acc = jnp.zeros((SUB, LANES), F32)
    for incoming in (False, True) if keep else (False,):
        edges = table_in if incoming else table
        build_far(sz, far, tile_at, b, -1 if incoming else 1)
        for c in range(sz.chunks):
            near = near_in if incoming else near_out
            change = gathered_change(sz, edges, far, near, incoming, c, edge_rotation(sz, edges, c))
            if keep:
                put3(sz, kept[int(incoming)], c, change)
            if not incoming:
                wc = get3(sz, wc_out, c)
                for i in range(3):
                    acc = acc + wc[i] * change[i] * change[i]
    share = 1.0 / sz.n_rep
    res, zz, ww, uu = residual[...], z[...], w[...], u[...]
    s1 = fold(res * zz) * share
    s2 = fold(zz * ww) * share
    s3 = fold(ww * uu) * share
    anc = anchor[...]
    s4 = acc + share * fold(anc * (comp(sz, u, 0) * comp(sz, u, 0) + comp(sz, u, 1) * comp(sz, u, 1) + comp(sz, u, 2) * comp(sz, u, 2)))
    block = [jnp.sum(s, axis=0, keepdims=True) for s in (s1, s2, s3, s4)]
    block = jnp.concatenate(block + [jnp.zeros((SUB - 4, LANES), F32)], axis=0)
    for i in range(sz.n_blk * sz.n_rep):
        scal[i] = block


def final_kernel(sz, est, z, u, scal, out):
    along_z, along_u = step_factors(scal, sz.n_blk * sz.n_rep)
    new = est[...] + along_z * z[...] + along_u * u[...]
    for c in range(3):
        for r in range(sz.hi):
            row = c * sz.hi + r
            out[pl.ds(c, 1), pl.ds(r * LANES, LANES)] = new[row : row + 1]


def on_device(measured, rot_vector, confidence, first_local, second_local, edge_counts, start_angles, anchor):
    n_blk, n_rep = lax.axis_size("blk"), lax.axis_size("rep")
    sz = Sizes(n_blk, n_rep, first_local.shape[1], first_local.shape[2], start_angles.shape[1])
    half = n_blk // 2
    tile = (sz.tile_rows, LANES)
    f32 = lambda *shape: jax.ShapeDtypeStruct(shape, F32)
    vmem = pl.BlockSpec(memory_space=pltpu.VMEM)
    rows = sz.chunks * SUB
    far_shape = pltpu.VMEM((sz.tile_rows * SUB, LANES), F32)

    def sums_scratch(channels):
        return [
            pltpu.VMEM((channels * 2 * rows, LANES), F32),
        ]

    def call(kernel, outs, args, scratch_shapes=(), flops=20_000_000):
        return pl.pallas_call(
            kernel,
            out_shape=outs,
            in_specs=[vmem] * len(args),
            out_specs=[vmem] * len(outs),
            scratch_shapes=list(scratch_shapes),
            cost_estimate=pl.CostEstimate(flops=flops, bytes_accessed=flops // 10, transcendentals=0),
            compiler_params=pltpu.CompilerParams(vmem_limit_bytes=48 * 1024 * 1024),
        )(*args)

    groups = [[core + 2 * i for i in range(half)] for core in range(2)]
    swap = [(i, i ^ 1) for i in range(n_blk)]

    def all_tiles(copies):
        same = lax.all_to_all(copies, "blk", 0, 0, axis_index_groups=groups)
        return same, lax.ppermute(same, "blk", swap)

    def other_half(value):
        if n_rep == 2:
            return lax.ppermute(value, "rep", [(0, 1), (1, 0)])
        return lax.psum(value, "rep") - value

    def all_products(scal):
        return lax.all_to_all(scal, ("blk", "rep"), 0, 0)

    table_shape = f32(CHANNELS * rows, LANES)
    steps = sz.pairs // 2
    (opened,) = call(opening_kernel, [f32(SUB, LANES)], [], flops=20_000_000_000)
    table, est, anchor_rows, *sends = call(
        functools.partial(pack_kernel, sz),
        [table_shape, f32(*tile), f32(sz.hi, LANES)]
        + [f32(2 * sz.edge_rows, LANES)] * (steps - 1)
        + [f32(sz.edge_rows, LANES)],
        [
            measured[:, 0], rot_vector[:, 0], confidence[:, 0], first_local[0], second_local[0], edge_counts.reshape(1, -1),
            start_angles, anchor.reshape(1, -1), opened,
        ],
    )
    ring = lambda shift, kept: [(i, (i + shift + n_blk) % n_blk) for i in range(n_blk) if i % 2 in kept]

    def sent(value, pairs):
        return lax.ppermute(value, "blk", pairs)

    mixed = sent(sends[-1], ring(-sz.pairs, (0,)) + ring(sz.pairs, (1,)))
    edges = [sent(sends[m - 1], ring(2 * m, (0, 1))) for m in range(1, steps)]
    tiles = [sent(est, ring(-2 * m, (0, 1))) for m in range(1, steps)]

    per_edge = f32(3 * rows, LANES)
    sums_shape = f32(9 * sz.hi, LANES)
    for sweep in range(PASSES):
        last = sweep + 1 == PASSES
        if sweep == 0:
            (relay,) = call(
                functools.partial(relay_kernel, sz),
                [f32(steps * (sz.edge_rows + sz.tile_rows), LANES)],
                [table, est, *edges, *tiles, mixed],
            )
            relayed = lax.ppermute(relay, "blk", swap)
            gap_out, wc_out, sums = call(
                functools.partial(outgoing_misfit_kernel, sz),
                [per_edge, per_edge, sums_shape],
                [table, est, relayed, *tiles],
                [far_shape] + sums_scratch(9),
            )
            table_in, gap_in, wc_in, sums = call(
                functools.partial(incoming_misfit_kernel, sz),
                [table_shape, per_edge, per_edge, sums_shape],
                [table, relayed, est, sums, *edges],
                sums_scratch(6),
            )
        else:
            wc_out, wc_in, sums, weights, est = call(
                functools.partial(next_misfit_kernel, sz),
                [per_edge, per_edge, sums_shape, f32(rows, LANES), f32(*tile)],
                [table, table_in, gap_out, gap_in, z_out, z_in, u_out, u_in, est, z, u, scal],
                sums_scratch(9),
            )
        residual, inverse, z, z_copies = call(
            functools.partial(precond_kernel, sz),
            [f32(*tile), f32(6 * sz.hi, LANES), f32(*tile), f32(half, *tile)],
            [sums, other_half(sums), est, anchor_rows],
        )
        z_a, z_b = all_tiles(z_copies)
        if last:
            near_out, near_in, weights = call(
                functools.partial(near_and_weights_kernel, sz),
                [per_edge, per_edge, f32(sz.pairs, sz.slots)],
                [table, table_in, z, weights],
            )
        else:
            near_out, near_in = call(functools.partial(near_kernel, sz), [per_edge, per_edge], [table, table_in, z])
        sums, *kept = call(
            functools.partial(image_kernel, sz, not last),
            [f32(*tile)] + ([] if last else [per_edge, per_edge]),
            [table, table_in, wc_out, wc_in, z_a, z_b, near_out, near_in],
            [far_shape] + sums_scratch(3),
        )
        if not last:
            z_out, z_in = kept
        w, u, u_copies = call(
            functools.partial(second_precond_kernel, sz),
            [f32(*tile), f32(*tile), f32(half, *tile)],
            [sums, other_half(sums), z, anchor_rows, inverse],
        )
        u_a, u_b = all_tiles(u_copies)
        near = call(functools.partial(near_kernel, sz), [per_edge] * (1 if last else 2), [table, table_in, u])
        scal, *kept = call(
            functools.partial(products_kernel, sz, not last),
            [f32(n_blk * n_rep, SUB, LANES)] + ([] if last else [per_edge, per_edge]),
            [table] + ([] if last else [table_in]) + [*near, wc_out, u_a, u_b, residual, z, w, u, anchor_rows],
            [far_shape],
        )
        if not last:
            u_out, u_in = kept
        scal = all_products(scal)
    (estimate,) = call(functools.partial(final_kernel, sz), [f32(3, sz.cams)], [est, z, u, scal])
    return (estimate, weights[None])


def solution(mesh):
    return jax.shard_map(
        on_device,
        mesh=mesh,
        in_specs=(
            P(None, "blk", None, "rep"),
            P(None, "blk", None, "rep"),
            P(None, "blk", None, "rep"),
            P("blk", None, "rep"),
            P("blk", None, "rep"),
            P("blk", None, "rep"),
            P(None, "blk"),
            P("blk"),
        ),
        out_specs=(P(None, "blk"), P("blk", None, "rep")),
        check_vma=False,
    )
```
